256 devices in a mesh: gx: 8 (over z), gy: 4 (over x), gz: 8 (over y, core).
Axes of the slice: x: 4, y: 4, z: 8, core: 2. Of those that a mesh axis runs over, the one named last changes fastest.
Arguments:
- patch_logits: bfloat16 [8, 4, 8, 24, 20736], P('gx', 'gy', 'gz'), may hold values from -12 to 312
- patch_start: int32 [8, 4, 8, 3], replicated, may hold values from 0 to 880, as said below
- patch_owner: int32 [8, 4, 8], replicated, may hold values from 0 to 31, as said below
Outputs:
- probs: float32 [64, 128, 3, 1024], P('gx', 'gy', None, 'gz')
The draws below stay inside these ranges and needn't reach their ends.
Inputs may be any that keep to these rules, and one draw needn't show every extreme that they name: `patch_start`: entry [i, j, k, d] is the first cell along dimension d of the patch at lattice position (i, j, k): i * 8 - 8 along x (32 and 128 in place of 8 along y and z), moved by at most 4 cells, then moved inward so that the patch lies inside the volume. `patch_owner`: for every k the entries [:, :, k] are the numbers 0 to 31, each once.
All inputs are finite; a program needn't handle non-finite values.
Results may differ from the reference program's by a relative error of at most 0.0003.
Values may be sent and summed in bfloat16 or wider, within the bound.
A program may use at most 128 MiB of HBM per device.

```python
import jax
import jax.numpy as jnp
from jax import lax

CLASSES = 3
BX = 8
BY = 32
BZ = 128
HALO = 8
JITTER = 4
KX = 8
KY = 4
KZ = 8
NX = 64
NY = 128
NZ = 1024
PX = 24
PY = 48
PZ = 144


def draw_patch_logits(key, part):
    full_shape = (KX, KY, KZ, PX, PY, CLASSES, PZ)
    normal_key, spike_key = jax.random.split(jax.random.fold_in(key, 11))
    values = jnp.clip(2.0 * jax.random.normal(normal_key, full_shape, jnp.float32), -12.0, 12.0)
    return values.reshape(KX, KY, KZ, PX, PY * CLASSES * PZ).astype(jnp.bfloat16)


def draw_patch_start(key, part):
    subkeys = jax.random.split(jax.random.fold_in(key, 23), 3)
    counts = (KX, KY, KZ)
    blocks = (BX, BY, BZ)
    extents = (PX, PY, PZ)
    columns = []
    for dimension in range(3):
        lattice = lax.broadcasted_iota(jnp.int32, (KX, KY, KZ), dimension)
        jitter_cells = jax.random.randint(subkeys[dimension], (KX, KY, KZ), -JITTER, JITTER + 1)
        first_cell = lattice * blocks[dimension] - HALO + jitter_cells
        first_cell = jnp.clip(first_cell, 0, counts[dimension] * blocks[dimension] - extents[dimension])
        columns.append(first_cell)
    return jnp.stack(columns, axis=-1).astype(jnp.int32)


def draw_patch_owner(key, part):
    subkeys = jax.random.split(jax.random.fold_in(key, 37), KZ)

    def shuffled(subkey):
        return jax.random.permutation(subkey, KX * KY)
    orders = jax.vmap(shuffled)(subkeys)
    return jnp.transpose(orders).reshape(KX, KY, KZ).astype(jnp.int32)


def setup_inputs(seed: int = 0) -> dict:
    streams_of = jax.random.split(jax.random.key(seed), 4)
    return {
        "patch_logits": draw_patch_logits(jax.random.fold_in(streams_of[3], 71), 0),
        "patch_start": draw_patch_start(jax.random.fold_in(streams_of[3], 71), 0),
        "patch_owner": draw_patch_owner(jax.random.fold_in(streams_of[3], 71), 0),
    }


def profile(length):
    offsets = jnp.arange(length).astype(jnp.float32)
    centre = (length - 1) / 2.0
    spread = length / 4.0
    return jnp.exp(-((offsets - centre) ** 2) / (2.0 * spread * spread))


def reference(patch_logits, patch_start, patch_owner):
    weight = profile(PX)[:, None, None, None] * profile(PY)[None, :, None, None]
    weight = weight * profile(PZ)[None, None, None, :]
    weight_full = jnp.broadcast_to(weight, (PX, PY, 1, PZ))
    totals = jnp.zeros((NX, NY, CLASSES + 1, NZ), jnp.float32)

    def add_patch(flat_index, totals):
        along_x = flat_index // (KY * KZ)
        along_y = (flat_index // KZ) % KY
        along_z = flat_index % KZ
        patch_code = patch_owner[along_x, along_y, along_z]
        home_x = patch_code // KY
        home_y = patch_code % KY
        corner = patch_start[home_x, home_y, along_z].astype(jnp.int32)
        logits = patch_logits[along_x, along_y, along_z].astype(jnp.float32).reshape(PX, PY, CLASSES, PZ)
        contribution = jnp.concatenate([logits * weight, weight_full], axis=2)
        anchor = (corner[0], corner[1], jnp.int32(0), corner[2])
        current = lax.dynamic_slice(totals, anchor, (PX, PY, CLASSES + 1, PZ))
        return lax.dynamic_update_slice(totals, current + contribution, anchor)

    totals = lax.fori_loop(0, KX * KY * KZ, add_patch, totals)
    scores = totals[:, :, :CLASSES] / totals[:, :, CLASSES:]
    return jax.nn.softmax(scores, axis=2)
```

```python
import functools

import jax
import jax.numpy as jnp
from jax import lax
from jax.experimental import pallas as pl
from jax.experimental.pallas import tpu as pltpu
from jax.sharding import PartitionSpec as P

CLASSES = 3
BX, BY, BZ = 8, 32, 128
PX, PY, PZ = 24, 48, 144
GX, GY, GZ = 8, 4, 8
ROW = CLASSES * PZ
RES = 16
VROWS = PY // RES
PIECE = 1408
SLOTS = 16
F32 = jnp.float32
MESH = pl.DeviceIdType.MESH


def profile(offsets, length):
    inside = (offsets >= 0) & (offsets < length)
    centre = (length - 1) / 2.0
    spread = length / 4.0
    values = jnp.exp(-((offsets.astype(F32) - centre) ** 2) / (2.0 * spread * spread))
    return jnp.where(inside, values, 0.0)


def place():
    return lax.axis_index("gx"), lax.axis_index("gy"), lax.axis_index("gz")


def hop_of(step, lane):
    return (0, 1, 2 - 4 * (lane % 2), -1)[step]


def cut_kernel(owner_ref, start_ref, x_ref, out_ref):
    a, b, k = place()
    code = owner_ref[a, b, k]
    sy = start_ref[code // GY, code % GY, k * 3 + 1]
    lane = lax.broadcasted_iota(jnp.int32, (PX, 128), 1)
    for rho in range(RES):
        slot = lax.rem(sy + rho, RES)
        parts = []
        for v in range(VROWS):
            src = ROW * (rho + RES * v)
            base, rest = src // 128 * 128, src % 128
            width = -(-(rest + ROW) // 128) * 128
            seg = x_ref[:, base : base + width].astype(F32)
            if width < 640:
                seg = jnp.concatenate([seg, jnp.zeros((PX, 640 - width), F32)], axis=1)
            shift = (ROW * v % 128 - rest) % 640
            parts.append(pltpu.roll(seg, shift, 1) if shift else seg)
        r0, r1, r2 = parts
        seam0 = jnp.where(lane < 48, r0[:, 384:512], r1[:, 0:128])
        seam1 = jnp.where(lane < 96, r1[:, 384:512], r2[:, 0:128])
        out_ref[slot, :, 0:384] = r0[:, 0:384].astype(jnp.bfloat16)
        out_ref[slot, :, 384:512] = seam0.astype(jnp.bfloat16)
        out_ref[slot, :, 512:768] = r1[:, 128:384].astype(jnp.bfloat16)
        out_ref[slot, :, 768:896] = seam1.astype(jnp.bfloat16)
        out_ref[slot, :, 896:1408] = r2[:, 128:640].astype(jnp.bfloat16)


def cut(owner, start, x):
    return pl.pallas_call(
        cut_kernel,
        out_shape=jax.ShapeDtypeStruct((RES, PX, PIECE), jnp.bfloat16),
        in_specs=[
            pl.BlockSpec(memory_space=pltpu.SMEM),
            pl.BlockSpec(memory_space=pltpu.SMEM),
            pl.BlockSpec(memory_space=pltpu.VMEM),
        ],
        out_specs=pl.BlockSpec(memory_space=pltpu.VMEM),
    )(owner, start, x)


def greet(partners):
    barrier = pltpu.get_barrier_semaphore()
    for partner in partners:
        pl.semaphore_signal(barrier, inc=1, device_id=partner, device_id_type=MESH)
    pl.semaphore_wait(barrier, len(partners))


def scatter_kernel(x_ref, out_ref, send_sem, recv_sem, local_sem):
    a, b, k = place()
    greet(
        [
            (lax.rem(a + dz + GX, GX), lax.rem(b + db, GY), k)
            for dz in (0, 1, -1, 2, -2)
            for db in range(GY)
            if dz or db
        ]
    )
    copies = []
    for step in (2, 1, 3, 0):
        group = lax.rem(a + step, 4)
        for turn in range(GY):
            if step == 0 and turn == 0:
                continue
            to_b = lax.rem(b + turn, GY)
            if step == 2:
                hop = 2 - 4 * lax.rem(to_b, 2)
            else:
                hop = hop_of(step, 0)
            copy = pltpu.make_async_remote_copy(
                src_ref=x_ref.at[4 * group + to_b],
                dst_ref=out_ref.at[4 * step + b],
                send_sem=send_sem.at[4 * step + turn],
                recv_sem=recv_sem.at[4 * step + turn],
                device_id=(lax.rem(a + hop + GX, GX), to_b, k),
                device_id_type=MESH,
            )
            copy.start()
            copies.append(copy)
    own = pltpu.make_async_copy(x_ref.at[4 * lax.rem(a, 4) + b], out_ref.at[b], local_sem)
    own.start()
    own.wait()
    for copy in copies:
        copy.wait()


def scatter(pieces):
    return pl.pallas_call(
        scatter_kernel,
        out_shape=jax.ShapeDtypeStruct((SLOTS, PX, PIECE), jnp.bfloat16),
        in_specs=[pl.BlockSpec(memory_space=pl.ANY)],
        out_specs=pl.BlockSpec(memory_space=pl.ANY),
        scratch_shapes=[
            pltpu.SemaphoreType.DMA((SLOTS,)),
            pltpu.SemaphoreType.DMA((SLOTS,)),
            pltpu.SemaphoreType.DMA,
        ],
        compiler_params=pltpu.CompilerParams(collective_id=0, has_side_effects=True),
    )(pieces)


def blend_kernel(owner_ref, start_ref, lanes_ref, x_ref, main_ref, rim_ref, sum_ref, acc, edge):
    a, b, k = place()
    acc[...] = jnp.zeros_like(acc)
    edge[...] = jnp.zeros_like(edge)
    residue = 4 * lax.rem(a, 4) + b
    col = lax.broadcasted_iota(jnp.int32, (PX, 256), 1)
    col = jnp.where(col < 192, col, col - 256)
    along_x = profile(lax.broadcasted_iota(jnp.int32, (PX, 256), 0), PX)
    odd = 2 - 4 * lax.rem(b, 2)

    def add_patch(slot, carry):
        step = slot // 4
        hop = jnp.where(step == 2, odd, jnp.where(step == 3, -1, step))
        from_a = lax.rem(a - hop + GX, GX)
        code = owner_ref[from_a, lax.rem(slot, 4), k]
        i, j = code // GY, lax.rem(code, GY)
        sx = start_ref[i, j, k * 3]
        sy = start_ref[i, j, k * 3 + 1]
        shift_z = start_ref[i, j, k * 3 + 2] - k * BZ
        rho = lax.rem(residue - sy + 8 * RES, RES)
        first_y = (sy + rho) // RES
        along_z = profile(col - shift_z, PZ)
        for v in range(VROWS):
            along_y = profile(jnp.full((PX, 256), rho + RES * v, jnp.int32), PY)
            weight = along_x * along_y * along_z
            rolled = []
            for c in range(CLASSES):
                m = CLASSES * v + c
                base = 128 * m if m < 8 else 1152
                turn = lax.rem(shift_z - (PZ * m - base) + 512, 256)
                seg = x_ref[slot, :, base : base + 256].astype(F32)
                rolled.append(pltpu.roll(seg, turn, 1))
            for d in range(2):
                value = (rolled[d + 1] - rolled[0]) * weight
                rows = pl.ds(sx, PX)
                acc[2 * (first_y + v) + d, rows, :] += value[:, 0:128]
                edge[2 * (first_y + v) + d, rows, :] += value[:, 128:256]
        return carry

    lax.fori_loop(0, SLOTS, add_patch, 0)

    for row in range(8):
        for d in range(2):
            for block in range(8):
                main_ref[block, row // 2, row % 2, d] = acc[2 * row + d, 8 * block : 8 * block + 8, :]
    lane = lax.broadcasted_iota(jnp.int32, (64, 128), 1)
    for d in range(2):
        up = jnp.zeros((64, 128), F32)
        low = jnp.zeros((64, 128), F32)
        for row in range(8):
            value = edge[2 * row + d]
            mine = lane // 16 == row
            turned = pltpu.roll(value, 16 * row, 1) if row else value
            up = jnp.where(mine, turned, up)
            turned = pltpu.roll(value, (16 * row + 16) % 128, 1) if row < 7 else value
            low = jnp.where(mine, turned, low)
        rim_ref[0, d] = up
        rim_ref[1, d] = low

    row = lax.broadcasted_iota(jnp.int32, (BX * BY, GX * GY * GZ), 0)
    plane = profile(a * BX + lax.rem(row, BX) - lanes_ref[0:1, :], PX)
    plane = plane * profile(b * BY + row // BX - lanes_ref[1:2, :], PY)
    row = lax.broadcasted_iota(jnp.int32, (BZ, GX * GY * GZ), 0)
    depth = profile(k * BZ + row - lanes_ref[2:3, :], PZ)
    sum_ref[...] = lax.dot_general(
        plane, depth, (((1,), (1,)), ((), ())), precision=lax.Precision.HIGHEST, preferred_element_type=F32
    )


def blend(owner, start, lanes, pieces):
    return pl.pallas_call(
        blend_kernel,
        out_shape=(
            jax.ShapeDtypeStruct((8, 4, 2, 2, 8, 128), F32),
            jax.ShapeDtypeStruct((2, 2, 64, 128), F32),
            jax.ShapeDtypeStruct((BX * BY, BZ), F32),
        ),
        in_specs=[
            pl.BlockSpec(memory_space=pltpu.SMEM),
            pl.BlockSpec(memory_space=pltpu.SMEM),
            pl.BlockSpec(memory_space=pltpu.VMEM),
            pl.BlockSpec(memory_space=pltpu.VMEM),
        ],
        out_specs=(pl.BlockSpec(memory_space=pltpu.VMEM),) * 3,
        scratch_shapes=[pltpu.VMEM((16, 64, 128), F32), pltpu.VMEM((16, 64, 128), F32)],
    )(owner, start, lanes, pieces)


def gather_kernel(main_ref, rim_ref, sum_ref, out_ref, total, rims, parts, send_sem, recv_sem, rim_send, rim_recv):
    a, b, k = place()
    above, below = lax.rem(k + 1, GZ), lax.rem(k + GZ - 1, GZ)
    others = [(dz, db) for dz in (4, 3, 5, 2, 6, 1, 7, 0) for db in range(GY) if dz or db]
    partners = [(lax.rem(a + dz, GX), lax.rem(b + db, GY), k) for dz, db in others]
    greet([(a, b, above), (a, b, below)] + partners)
    rim_copies = []
    for side, to_k in ((0, above), (1, below)):
        copy = pltpu.make_async_remote_copy(
            src_ref=rim_ref.at[side],
            dst_ref=rims.at[side],
            send_sem=rim_send.at[side],
            recv_sem=rim_recv.at[side],
            device_id=(a, b, to_k),
            device_id_type=MESH,
        )
        copy.start()
        rim_copies.append(copy)
    for copy in rim_copies:
        copy.wait()
    lane = lax.broadcasted_iota(jnp.int32, (8, 128), 1)
    for block in range(8):
        for d in range(2):
            up = rims[0, d, 8 * block : 8 * block + 8, :]
            low = rims[1, d, 8 * block : 8 * block + 8, :]
            for row in range(8):
                shifted = jnp.where(lane < 16, pltpu.roll(up, (128 - 16 * row) % 128, 1), 0.0)
                shifted = shifted + jnp.where(lane >= 112, pltpu.roll(low, 112 - 16 * row, 1), 0.0)
                total[block, row // 2, row % 2, d] = main_ref[block, row // 2, row % 2, d] + shifted
    copies = []
    for at, ((dz, db), partner) in enumerate(zip(others, partners)):
        copy = pltpu.make_async_remote_copy(
            src_ref=total.at[partner[0], partner[1]],
            dst_ref=parts.at[a, b],
            send_sem=send_sem.at[at],
            recv_sem=recv_sem.at[at],
            device_id=partner,
            device_id_type=MESH,
        )
        copy.start()
        copies.append(copy)
    parts[a, b] = total[a, b]
    for copy in copies:
        copy.wait()
    for residue in range(RES):
        for h in range(2):
            y = RES * h + residue
            d1 = parts[residue // 4, residue % 4, h, 0] + parts[residue // 4 + 4, residue % 4, h, 0]
            d2 = parts[residue // 4, residue % 4, h, 1] + parts[residue // 4 + 4, residue % 4, h, 1]
            norm = sum_ref[8 * y : 8 * y + 8, :]
            d1, d2 = d1 / norm, d2 / norm
            top = jnp.maximum(jnp.maximum(d1, d2), 0.0)
            e0, e1, e2 = jnp.exp(-top), jnp.exp(d1 - top), jnp.exp(d2 - top)
            scale = 1.0 / (e0 + e1 + e2)
            out_ref[y, 0] = e0 * scale
            out_ref[y, 1] = e1 * scale
            out_ref[y, 2] = e2 * scale


def gather(main, rim, weight_sum):
    return pl.pallas_call(
        gather_kernel,
        out_shape=jax.ShapeDtypeStruct((BY, CLASSES, BX, BZ), F32),
        in_specs=[pl.BlockSpec(memory_space=pltpu.VMEM)] * 3,
        out_specs=pl.BlockSpec(memory_space=pltpu.VMEM),
        scratch_shapes=[
            pltpu.VMEM((8, 4, 2, 2, 8, 128), F32),
            pltpu.VMEM((2, 2, 64, 128), F32),
            pltpu.VMEM((8, 4, 2, 2, 8, 128), F32),
            pltpu.SemaphoreType.DMA((31,)),
            pltpu.SemaphoreType.DMA((31,)),
            pltpu.SemaphoreType.DMA((2,)),
            pltpu.SemaphoreType.DMA((2,)),
        ],
        compiler_params=pltpu.CompilerParams(collective_id=1, has_side_effects=True),
    )(main, rim, weight_sum)


def per_device(patch_logits, patch_start, patch_owner):
    start = patch_start.reshape(GX, GY, GZ * 3)
    lanes = patch_start.reshape(GX * GY * GZ, 3).T
    pieces = cut(patch_owner, start, patch_logits.reshape(PX, PY * ROW))
    pieces = scatter(pieces)
    main, rim, weight_sum = blend(patch_owner, start, lanes, pieces)
    probs = gather(main, rim, weight_sum)
    return jnp.transpose(probs, (2, 0, 1, 3))


def solution(mesh):
    return jax.shard_map(
        per_device,
        mesh=mesh,
        in_specs=(P("gx", "gy", "gz", None, None), P(), P()),
        out_specs=P("gx", "gy", None, "gz"),
        check_vma=False,
    )
```

```python
import jax
import jax.numpy as jnp
from jax import lax
from jax.experimental import pallas as pl
from jax.experimental.pallas import tpu as pltpu
from jax.sharding import PartitionSpec as P

CLASSES = 3
BX, BY, BZ = 8, 32, 128
PX, PY, PZ = 24, 48, 144
GX, GY, GZ = 8, 4, 8
ROW = CLASSES * PZ
RES = 16
VROWS = PY // RES
GROUPS = PX // 8
TILES = 31
LAST = PY * ROW // 128 - 1
MARGIN = 40
OWNERS = GX * GY
F32 = jnp.float32
BF16 = jnp.bfloat16
MESH = pl.DeviceIdType.MESH


def profile(offsets, length):
    inside = (offsets >= 0) & (offsets < length)
    centre = (length - 1) / 2.0
    spread = length / 4.0
    values = jnp.exp(-((offsets.astype(F32) - centre) ** 2) / (2.0 * spread * spread))
    return jnp.where(inside, values, 0.0)


def iota(dim):
    return lax.broadcasted_iota(jnp.int32, (8, 128), dim)


def wrap(index, size):
    return lax.rem(index + size, size)


def hop_of(step, to_b):
    return (0, 1, 2 - 4 * lax.rem(to_b, 2), -1)[step]


def blend_kernel(
    owner_ref, start_ref, x_ref, out_ref,
    patch, send, recv, table, sums, value, acc, rim, rims, total, parts,
    in_sem, send_sem, recv_sem, rim_send, rim_recv, part_send, part_recv,
):
    a, b, k = lax.axis_index("gx"), lax.axis_index("gy"), lax.axis_index("gz")
    above, below = wrap(k + 1, GZ), wrap(k - 1, GZ)
    barrier = pltpu.get_barrier_semaphore()
    for dz in range(GX):
        for db in range(GY):
            if dz or db:
                to = (wrap(a + dz, GX), wrap(b + db, GY), k)
                pl.semaphore_signal(barrier, inc=1, device_id=to, device_id_type=MESH)
    for to_k in (above, below):
        pl.semaphore_signal(barrier, inc=1, device_id=(a, b, to_k), device_id_type=MESH)
    load = pltpu.make_async_copy(x_ref, patch, in_sem)
    load.start()

    lane, sub = iota(1), iota(0)

    def start_of(code, at_k, dim):
        return start_ref[code // GY, dim, lax.rem(code, GY), at_k]

    zero = jnp.zeros((8, 128), F32)
    for s in range(4):
        for d in range(2):
            for t in range(2):
                for v in range(VROWS):
                    for row in (*range(0, MARGIN, 8), *range(MARGIN + PX, PX + 2 * MARGIN, 8)):
                        value[s, v, d, t, row : row + 8, :] = zero
                for row in range(0, PX + 2 * MARGIN, 8):
                    value[s, VROWS, d, t, row : row + 8, :] = zero
    for offset in range(3 * PX):
        table[offset] = profile(jnp.full((8, 128), offset - PX, jnp.int32), PX)

    my_sy = start_of(owner_ref[a, b, k], k, 1)
    load.wait()

    def cut(residue, store):
        rho = lax.rem(residue - my_sy + 8 * RES, RES)
        for g in range(GROUPS):
            held = [[], [], []]
            for v in range(VROWS):
                into = ROW * v % 128
                delta = ROW * rho + ROW * RES * v - into
                first = (delta + 127) // 128
                turn = first * 128 - delta
                count = -(-(into + ROW) // 128)
                turned = []
                for t in range(-1, count):
                    at = first + t
                    if t == -1:
                        at = jnp.maximum(at, 0)
                    if t == count - 1:
                        at = jnp.minimum(at, LAST)
                    tile = patch[g, at]
                    turned.append(pltpu.roll(tile.astype(F32), turn, 1))
                held[v] = [jnp.where(lane < turn, turned[t], turned[t + 1]) for t in range(count)]
            r0, r1, r2 = held
            tiles = r0[:3] + [jnp.where(lane < 48, r0[3], r1[0])] + r1[1:3]
            tiles = tiles + [jnp.where(lane < 96, r1[3], r2[0])] + r2[1:4]
            for t in range(10):
                store(GROUPS * t + g, tiles[t].astype(BF16))
            tail = r2[4] if g == 0 else pltpu.roll(r2[4], 16 * g, 1)
            tails = tail if g == 0 else jnp.where(lane < 16 * g, tails, tail)
        store(TILES - 1, tails.astype(BF16))

    def piece_copy(step, turn):
        to_b = wrap(b + turn, GY)
        return pltpu.make_async_remote_copy(
            src_ref=send.at[4 * step + turn],
            dst_ref=recv.at[4 * step + b],
            send_sem=send_sem.at[4 * step + turn],
            recv_sem=recv_sem.at[4 * step + b],
            device_id=(wrap(a + hop_of(step, to_b), GX), to_b, k),
            device_id_type=MESH,
        )

    def piece_arrival(step, from_b):
        return pltpu.make_async_remote_copy(
            src_ref=send.at[4 * step],
            dst_ref=recv.at[4 * step + from_b],
            send_sem=send_sem.at[4 * step],
            recv_sem=recv_sem.at[4 * step + from_b],
            device_id=(a, b, above),
            device_id_type=MESH,
        )

    for step in (2, 1, 3, 0):

        def cut_one(turn, carry, step=step):
            residue = 4 * lax.rem(a + step, 4) + wrap(b + turn, GY)

            def store(tile, what):
                send[4 * step + turn, tile] = what

            cut(residue, store)
            return carry

        lax.fori_loop(1 if step == 0 else 0, GY, cut_one, 0)
        if step == 2:
            pl.semaphore_wait(barrier, OWNERS + 1)
        for turn in range(1 if step == 0 else 0, GY):
            piece_copy(step, turn).start()

    def store_own(tile, what):
        recv[b, tile] = what

    cut(4 * lax.rem(a, 4) + b, store_own)

    def add_weight(index, carry):
        i, j, at_k = a - 2 + index // 9, b - 1 + lax.rem(index // 3, 3), k - 1 + lax.rem(index, 3)
        valid = (i >= 0) & (i < GX) & (j >= 0) & (j < GY) & (at_k >= 0) & (at_k < GZ)
        i, j, at_k = jnp.clip(i, 0, GX - 1), jnp.clip(j, 0, GY - 1), jnp.clip(at_k, 0, GZ - 1)
        along_z = profile(BZ * k + lane - start_ref[i, 2, j, at_k], PZ)
        along_z = along_z * jnp.where(valid, 1.0, 0.0)
        y = BY * b + sub - start_ref[i, 1, j, at_k]
        planes = [profile(y + 8 * g, PY) * along_z for g in range(4)]
        base = jnp.clip(BX * a - start_ref[i, 0, j, at_k] + PX, 0, 2 * PX)
        new = []
        for x in range(BX):
            along_x = table[base + x]
            new += [carry[4 * x + g] + along_x * planes[g] for g in range(4)]
        return tuple(new)

    weights = lax.fori_loop(0, 45, add_weight, (zero,) * 32)
    for at in range(32):
        sums[at] = weights[at]

    residue = 4 * lax.rem(a, 4) + b
    along_x = [profile(sub + 8 * g, PX) for g in range(GROUPS)]
    columns = (lane, jnp.where(lane < 64, lane + 128, lane - 128))

    def corner(step, from_b):
        from_a = wrap(a - hop_of(step, b), GX)
        code = owner_ref[from_a, from_b, k]
        sy = start_of(code, k, 1)
        rho = lax.rem(residue - sy + 8 * RES, RES)
        return start_of(code, k, 0), (sy + rho) // RES, rho, start_of(code, k, 2) - BZ * k

    for group, step in enumerate((0, 1, 3, 2)):

        def weigh(from_b, carry, step=step):
            if step == 0:

                @pl.when(from_b != b)
                def _():
                    piece_arrival(step, from_b).wait_recv()

            else:
                piece_arrival(step, from_b).wait_recv()
            _, _, rho, shift_z = corner(step, from_b)
            along_z = [profile(c - shift_z, PZ) for c in columns]
            for v in range(VROWS):
                along_y = profile(jnp.full((8, 128), RES * v, jnp.int32) + rho, PY)
                turns, swaps = [], []
                for c in range(CLASSES):
                    m = CLASSES * v + c
                    turn = lax.rem(shift_z - 16 * (m % 8) + 512, 256)
                    low = lax.rem(turn, 128)
                    turns.append(low)
                    high = turn // 128
                    swaps.append((jnp.where(lane < low, 1, 0) + high) == 1)
                for g in range(GROUPS):
                    rolled = []
                    for c in range(CLASSES):
                        m = CLASSES * v + c
                        column = m if m < 8 else 9
                        first = recv[4 * step + from_b, GROUPS * column + g].astype(F32)
                        if column == 9:
                            second = recv[4 * step + from_b, TILES - 1].astype(F32)
                            second = pltpu.roll(second, 128 - 16 * g, 1) if g else second
                        else:
                            second = recv[4 * step + from_b, GROUPS * (column + 1) + g].astype(F32)
                        first, second = pltpu.roll(first, turns[c], 1), pltpu.roll(second, turns[c], 1)
                        rolled.append((jnp.where(swaps[c], second, first), jnp.where(swaps[c], first, second)))
                    along_xy = along_x[g] * along_y
                    rows = slice(MARGIN + 8 * g, MARGIN + 8 * g + 8)
                    for t in range(2):
                        weight = along_xy * along_z[t]
                        for d in range(2):
                            value[from_b, v, d, t, rows, :] = (rolled[d + 1][t] - rolled[0][t]) * weight
            return carry

        lax.fori_loop(0, GY, weigh, 0)
        corners = [corner(step, from_b) for from_b in range(GY)]
        for t in (1, 0):

            def place(y, carry, t=t, group=group, corners=corners):
                places = []
                for sx, first_y, _, _ in corners:
                    v = y - first_y
                    places.append((jnp.where((v >= 0) & (v < VROWS), v, VROWS), MARGIN - sx))
                for d in range(2):
                    for block in range(GX):
                        rows = slice(8 * block, 8 * block + 8)
                        got = None if group == 0 else acc[y, d, t, rows, :]
                        for s, (v, row) in enumerate(places):
                            more = value[s, v, d, t, pl.ds(row + 8 * block, 8), :]
                            got = more if got is None else got + more
                        acc[y, d, t, rows, :] = got
                return carry

            lax.fori_loop(0, 8, place, 0)
            if group == 3 and t == 1:
                for d in range(2):
                    for block in range(GX):
                        rows = slice(8 * block, 8 * block + 8)
                        up, low = zero, zero
                        for y in range(8):
                            turned = acc[y, d, 1, rows, :]
                            turned = pltpu.roll(turned, 16 * y, 1) if y else turned
                            up = jnp.where(lane // 16 == y, turned, up)
                            low = jnp.where(lane // 16 == (y + 7) % 8, turned, low)
                        rim[0, d, rows, :] = up
                        rim[1, d, rows, :] = low
                rim_copies = []
                for side, to_k in ((0, above), (1, below)):
                    copy = pltpu.make_async_remote_copy(
                        src_ref=rim.at[side],
                        dst_ref=rims.at[side],
                        send_sem=rim_send.at[side],
                        recv_sem=rim_recv.at[side],
                        device_id=(a, b, to_k),
                        device_id_type=MESH,
                    )
                    copy.start()
                    rim_copies.append(copy)
    for copy in rim_copies:
        copy.wait()

    def whom(index):
        far = index // GY
        dz = 4 + ((far + 1) // 2) * (1 - 2 * lax.rem(far, 2))
        return wrap(a + dz, GX), wrap(b + lax.rem(index + 1, GY), GY)

    def part_copy(index):
        to_a, to_b = whom(index)
        return pltpu.make_async_remote_copy(
            src_ref=total.at[pl.ds(pl.multiple_of(32 * (GY * to_a + to_b), 32), 32)],
            dst_ref=parts.at[pl.ds(pl.multiple_of(32 * (GY * a + b), 32), 32)],
            send_sem=part_send.at[index],
            recv_sem=part_recv.at[index],
            device_id=(to_a, to_b, k),
            device_id_type=MESH,
        )

    def finish_owner(to_a, to_b, store):
        rows = pl.ds(pl.multiple_of(8 * to_a, 8), 8)
        for h in range(2):
            y = 2 * to_b + h
            for d in range(2):
                up = pltpu.roll(rims[0, d, rows, :], lax.rem(128 - 16 * y, 128), 1)
                low = pltpu.roll(rims[1, d, rows, :], lax.rem(256 - 16 * y, 128), 1)
                more = jnp.where(lane < 16, up, jnp.where(lane >= 112, low, 0.0))
                store(16 * h + 8 * d, acc[y, d, 0, rows, :] + more)

    def send_part(index, carry):
        to_a, to_b = whom(index)

        def store(row, what):
            total[pl.ds(pl.multiple_of(32 * (GY * to_a + to_b) + row, 8), 8), :] = what

        finish_owner(to_a, to_b, store)

        @pl.when(index > 0)
        def _():
            part_copy(index - 1).start()

        return carry

    lax.fori_loop(0, OWNERS - 1, send_part, 0)

    def store_mine(row, what):
        parts[pl.ds(pl.multiple_of(32 * (GY * a + b) + row, 8), 8), :] = what

    finish_owner(a, b, store_mine)
    part_copy(OWNERS - 2).start()

    for step in range(4):
        for turn in range(1 if step == 0 else 0, GY):
            piece_copy(step, turn).wait_send()

    def await_part(index, carry):
        part_copy(index).wait()
        return carry

    lax.fori_loop(0, OWNERS - 1, await_part, 0)

    for x in range(BX):
        for h in range(2):
            for g in range(2):
                halves = []
                for d in range(2):
                    row = 8 * g * 32 + 16 * h + 8 * d + x
                    one = parts[pl.ds(row, 8, stride=32), :]
                    halves.append(one + parts[pl.ds(row + 512, 8, stride=32), :])
                norm = sums[4 * x + 2 * h + g]
                d1, d2 = halves[0] / norm, halves[1] / norm
                top = jnp.maximum(jnp.maximum(d1, d2), 0.0)
                e0, e1, e2 = jnp.exp(-top), jnp.exp(d1 - top), jnp.exp(d2 - top)
                scale = 1.0 / (e0 + e1 + e2)
                rows = slice(16 * h + 8 * g, 16 * h + 8 * g + 8)
                out_ref[x, 0, rows, :] = e0 * scale
                out_ref[x, 1, rows, :] = e1 * scale
                out_ref[x, 2, rows, :] = e2 * scale


def per_device(patch_logits, patch_start, patch_owner):
    tiles = patch_logits.reshape(GROUPS, 8, LAST + 1, 128)
    probs = pl.pallas_call(
        blend_kernel,
        out_shape=jax.ShapeDtypeStruct((BX, CLASSES, BY, BZ), F32),
        in_specs=[
            pl.BlockSpec(memory_space=pltpu.SMEM),
            pl.BlockSpec(memory_space=pltpu.SMEM),
            pl.BlockSpec(memory_space=pl.ANY),
        ],
        out_specs=pl.BlockSpec(memory_space=pltpu.VMEM),
        scratch_shapes=[
            pltpu.VMEM((GROUPS, LAST + 1, 8, 128), BF16),
            pltpu.VMEM((16, TILES, 8, 128), BF16),
            pltpu.VMEM((16, TILES, 8, 128), BF16),
            pltpu.VMEM((3 * PX, 8, 128), F32),
            pltpu.VMEM((32, 8, 128), F32),
            pltpu.VMEM((4, VROWS + 1, 2, 2, PX + 2 * MARGIN, 128), F32),
            pltpu.VMEM((8, 2, 2, 64, 128), F32),
            pltpu.VMEM((2, 2, 64, 128), F32),
            pltpu.VMEM((2, 2, 64, 128), F32),
            pltpu.VMEM((32 * OWNERS, 128), F32),
            pltpu.VMEM((32 * OWNERS, 128), F32),
            pltpu.SemaphoreType.DMA,
            pltpu.SemaphoreType.DMA((16,)),
            pltpu.SemaphoreType.DMA((16,)),
            pltpu.SemaphoreType.DMA((2,)),
            pltpu.SemaphoreType.DMA((2,)),
            pltpu.SemaphoreType.DMA((OWNERS,)),
            pltpu.SemaphoreType.DMA((OWNERS,)),
        ],
        compiler_params=pltpu.CompilerParams(collective_id=0, has_side_effects=True),
    )(patch_owner, jnp.transpose(patch_start, (0, 3, 1, 2)), jnp.transpose(tiles, (0, 2, 1, 3)))
    return jnp.transpose(probs, (0, 2, 1, 3))


def solution(mesh):
    return jax.shard_map(
        per_device,
        mesh=mesh,
        in_specs=(P("gx", "gy", "gz", None, None), P(), P()),
        out_specs=P("gx", "gy", None, "gz"),
        check_vma=False,
    )
```

```python
import jax
import jax.numpy as jnp
from jax import lax
from jax.experimental import pallas as pl
from jax.experimental.pallas import tpu as pltpu
from jax.sharding import PartitionSpec as P

CLASSES = 3
BX, BY, BZ = 8, 32, 128
PX, PY, PZ = 24, 48, 144
GX, GY, GZ = 8, 4, 8
ROW = CLASSES * PZ
RES = 16
VROWS = PY // RES
GROUPS = PX // 8
TILES = (21, 11)
LAST = PY * ROW // 128 - 1
MARGIN = 40
OWNERS = GX * GY
F32 = jnp.float32
BF16 = jnp.bfloat16
MESH = pl.DeviceIdType.MESH


def profile(offsets, length):
    inside = (offsets >= 0) & (offsets < length)
    centre = (length - 1) / 2.0
    spread = length / 4.0
    values = jnp.exp(-((offsets.astype(F32) - centre) ** 2) / (2.0 * spread * spread))
    return jnp.where(inside, values, 0.0)


def iota(dim):
    return lax.broadcasted_iota(jnp.int32, (8, 128), dim)


def wrap(index, size):
    return lax.rem(index + size, size)


def hop_of(step, to_b):
    return (0, 1, 2 - 4 * lax.rem(to_b, 2), -1)[step]


def blend_kernel(
    owner_ref, start_ref, x_ref, out_ref,
    patch, send0, send1, recv0, recv1, table, sums, kept, value, acc, rim, rims, total, parts,
    in_sem, send_sem, recv_sem, rim_send, rim_recv, part_send, part_recv,
):
    a, b, k = lax.axis_index("gx"), lax.axis_index("gy"), lax.axis_index("gz")
    above, below = wrap(k + 1, GZ), wrap(k - 1, GZ)
    send, recv = (send0, send1), (recv0, recv1)
    near = [
        (wrap(a + dz, GX), wrap(b + db, GY), k) for dz in (0, 1, -1, 2, -2) for db in range(GY) if dz or db
    ] + [(a, b, above), (a, b, below)]
    barrier = pltpu.get_barrier_semaphore()
    for to in near:
        pl.semaphore_signal(barrier, inc=1, device_id=to, device_id_type=MESH)
    load = pltpu.make_async_copy(x_ref, patch, in_sem)
    load.start()

    lane, sub = iota(1), iota(0)
    zero = jnp.zeros((8, 128), F32)

    def start_of(code, at_k, dim):
        return start_ref[code // GY, dim, lax.rem(code, GY), at_k]

    my_sy = start_of(owner_ref[a, b, k], k, 1)
    load.wait()

    def cut(residue, store):
        rho = lax.rem(residue - my_sy + 8 * RES, RES)
        for half, (skip, length) in enumerate(((0, 2 * PZ), (2 * PZ, PZ))):
            for g in range(GROUPS):
                tiles = {}
                for v in range(VROWS):
                    into = length * v
                    delta = ROW * rho + (ROW * RES * v + skip - into)
                    first = (delta + 127) // 128
                    turn = first * 128 - delta
                    low, high = into // 128, (into + length - 1) // 128
                    turned = []
                    for t in range(low - 1, high + 1):
                        at = first + t
                        if t < 0:
                            at = jnp.maximum(at, 0)
                        if half == 1 and v == VROWS - 1 and t == high:
                            at = jnp.minimum(at, LAST)
                        turned.append(pltpu.roll(patch[g, at].astype(F32), turn, 1))
                    for t in range(low, high + 1):
                        tile = jnp.where(lane < turn, turned[t - low], turned[t - low + 1])
                        tiles[t] = jnp.where(lane < into % 128, tiles[t], tile) if t in tiles else tile
                for t in range(7 if half == 0 else 3):
                    store(half, GROUPS * t + g, tiles[t].astype(BF16))
                if half == 1:
                    if g == 0:
                        tail = tiles[3]
                    elif g == 1:
                        store(1, 9, jnp.where(lane < 48, tail, pltpu.roll(tiles[3], 48, 1)).astype(BF16))
                    else:
                        store(1, 10, tiles[3].astype(BF16))

    def piece_copy(half, step, turn):
        to_b = wrap(b + turn, GY)
        return pltpu.make_async_remote_copy(
            src_ref=send[half].at[4 * step + turn],
            dst_ref=recv[half].at[4 * step + b],
            send_sem=send_sem.at[half, 4 * step + turn],
            recv_sem=recv_sem.at[half, 4 * step + b],
            device_id=(wrap(a + hop_of(step, to_b), GX), to_b, k),
            device_id_type=MESH,
        )

    def piece_arrival(half, step, from_b):
        return pltpu.make_async_remote_copy(
            src_ref=send[half].at[4 * step],
            dst_ref=recv[half].at[4 * step + from_b],
            send_sem=send_sem.at[half, 4 * step],
            recv_sem=recv_sem.at[half, 4 * step + from_b],
            device_id=(a, b, above),
            device_id_type=MESH,
        )

    turns_of = ((2, range(GY)), (1, range(GY)), (3, range(GY)), (0, range(1, GY)))
    for step, turns in turns_of:

        def cut_one(turn, carry, step=step):
            residue = 4 * lax.rem(a + step, 4) + wrap(b + turn, GY)

            def store(half, tile, what):
                send[half][4 * step + turn, tile] = what

            cut(residue, store)
            return carry

        lax.fori_loop(turns.start, GY, cut_one, 0)
        if step == 2:
            pl.semaphore_wait(barrier, len(near))
        for turn in turns:
            piece_copy(0, step, turn).start()
    for step, turns in turns_of:
        for turn in turns:
            piece_copy(1, step, turn).start()

    def store_own(half, tile, what):
        recv[half][b, tile] = what

    cut(4 * lax.rem(a, 4) + b, store_own)

    for s in range(4):
        for t in range(2):
            for v in range(VROWS):
                for row in (*range(0, MARGIN, 8), *range(MARGIN + PX, PX + 2 * MARGIN, 8)):
                    value[s, v, t, row : row + 8, :] = zero
            for row in range(0, PX + 2 * MARGIN, 8):
                value[s, VROWS, t, row : row + 8, :] = zero
    for offset in range(3 * PX):
        table[offset] = profile(jnp.full((8, 128), offset - PX, jnp.int32), PX)

    def add_weight(index, carry):
        i, j, at_k = a - 2 + index // 9, b - 1 + lax.rem(index // 3, 3), k - 1 + lax.rem(index, 3)
        valid = (i >= 0) & (i < GX) & (j >= 0) & (j < GY) & (at_k >= 0) & (at_k < GZ)
        i, j, at_k = jnp.clip(i, 0, GX - 1), jnp.clip(j, 0, GY - 1), jnp.clip(at_k, 0, GZ - 1)
        along_z = profile(BZ * k + lane - start_ref[i, 2, j, at_k], PZ)
        along_z = along_z * jnp.where(valid, 1.0, 0.0)
        y = BY * b + sub - start_ref[i, 1, j, at_k]
        planes = [profile(y + 8 * g, PY) * along_z for g in range(4)]
        base = jnp.clip(BX * a - start_ref[i, 0, j, at_k] + PX, 0, 2 * PX)
        new = []
        for x in range(BX):
            along_x = table[base + x]
            new += [carry[4 * x + g] + along_x * planes[g] for g in range(4)]
        return tuple(new)

    weights = lax.fori_loop(0, 45, add_weight, (zero,) * 32)
    for at in range(32):
        sums[at] = weights[at]

    residue = 4 * lax.rem(a, 4) + b
    along_x = [profile(sub + 8 * g, PX) for g in range(GROUPS)]
    columns = (lane, jnp.where(lane < 64, lane + 128, lane - 128))

    def corner(step, from_b):
        from_a = wrap(a - hop_of(step, b), GX)
        code = owner_ref[from_a, from_b, k]
        sy = start_of(code, k, 1)
        rho = lax.rem(residue - sy + 8 * RES, RES)
        return start_of(code, k, 0), (sy + rho) // RES, rho, start_of(code, k, 2) - BZ * k

    def aligned(first, second, shift, lead):
        turn = lax.rem(shift - lead + 512, 256)
        low = lax.rem(turn, 128)
        swap = (jnp.where(lane < low, 1, 0) + turn // 128) == 1
        first, second = pltpu.roll(first.astype(F32), low, 1), pltpu.roll(second.astype(F32), low, 1)
        return jnp.where(swap, second, first), jnp.where(swap, first, second)

    def weigh_group(half, step):
        def weigh(from_b, carry):
            slot = 4 * step + from_b
            if step == 0:

                @pl.when(from_b != b)
                def _():
                    piece_arrival(half, step, from_b).wait_recv()

            else:
                piece_arrival(half, step, from_b).wait_recv()
            _, _, rho, shift = corner(step, from_b)
            along_z = [profile(c - shift, PZ) for c in columns]
            for v in range(VROWS):
                along_y = profile(jnp.full((8, 128), RES * v, jnp.int32) + rho, PY)
                for g in range(GROUPS):
                    if half == 0:
                        pair = []
                        for m in (2 * v, 2 * v + 1):
                            ends = recv0[slot, GROUPS * m + g], recv0[slot, GROUPS * m + GROUPS + g]
                            pair.append(aligned(*ends, shift, 16 * m))
                        base, upper = pair
                        for t in range(2):
                            kept[slot, v, t, g] = base[t]
                    else:
                        first = recv1[slot, GROUPS * v + g].astype(F32)
                        if v < VROWS - 1:
                            second = recv1[slot, GROUPS * v + GROUPS + g].astype(F32)
                        else:
                            second = recv1[slot, 9 + g // 2].astype(F32)
                            second = pltpu.roll(second, 80, 1) if g == 1 else second
                        upper = aligned(first, second, shift, 16 * v)
                        base = [kept[slot, v, t, g] for t in range(2)]
                    along_xy = along_x[g] * along_y
                    rows = slice(MARGIN + 8 * g, MARGIN + 8 * g + 8)
                    for t in range(2):
                        value[from_b, v, t, rows, :] = (upper[t] - base[t]) * (along_xy * along_z[t])
            return carry

        lax.fori_loop(0, GY, weigh, 0)

    def place_group(half, step, t, first):
        corners = [corner(step, from_b) for from_b in range(GY)]

        def place(y, carry):
            places = []
            for sx, first_y, _, _ in corners:
                v = y - first_y
                places.append((jnp.where((v >= 0) & (v < VROWS), v, VROWS), MARGIN - sx))
            for block in range(GX):
                rows = slice(8 * block, 8 * block + 8)
                got = None if first else acc[half, y, t, rows, :]
                for s, (v, row) in enumerate(places):
                    more = value[s, v, t, pl.ds(row + 8 * block, 8), :]
                    got = more if got is None else got + more
                acc[half, y, t, rows, :] = got
            return carry

        lax.fori_loop(0, 8, place, 0)

    def rim_copies(half):
        return [
            pltpu.make_async_remote_copy(
                src_ref=rim.at[half, side],
                dst_ref=rims.at[half, side],
                send_sem=rim_send.at[half, side],
                recv_sem=rim_recv.at[half, side],
                device_id=(a, b, to_k),
                device_id_type=MESH,
            )
            for side, to_k in ((0, above), (1, below))
        ]

    def send_rims(half):
        for block in range(GX):
            rows = slice(8 * block, 8 * block + 8)
            up, low = zero, zero
            for y in range(8):
                turned = acc[half, y, 1, rows, :]
                turned = pltpu.roll(turned, 16 * y, 1) if y else turned
                up = jnp.where(lane // 16 == y, turned, up)
                low = jnp.where(lane // 16 == (y + 7) % 8, turned, low)
            rim[half, 0, rows, :] = up
            rim[half, 1, rows, :] = low
        for copy in rim_copies(half):
            copy.start()

    def whom(index):
        far = index // GY
        dz = 4 + ((far + 1) // 2) * (1 - 2 * lax.rem(far, 2))
        return wrap(a + dz, GX), wrap(b + lax.rem(index + 1, GY), GY)

    def part_copy(half, index):
        to_a, to_b = whom(index)
        return pltpu.make_async_remote_copy(
            src_ref=total.at[half, pl.ds(pl.multiple_of(16 * (GY * to_a + to_b), 16), 16)],
            dst_ref=parts.at[half, pl.ds(pl.multiple_of(16 * (GY * a + b), 16), 16)],
            send_sem=part_send.at[half, index],
            recv_sem=part_recv.at[half, index],
            device_id=(to_a, to_b, k),
            device_id_type=MESH,
        )

    def finish_owner(half, to_a, to_b, into, slot):
        rows = pl.ds(pl.multiple_of(8 * to_a, 8), 8)
        for h in range(2):
            y = 2 * to_b + h
            back = lax.rem(128 - 16 * y, 128)
            up = pltpu.roll(rims[half, 0, rows, :], back, 1)
            low = pltpu.roll(rims[half, 1, rows, :], back, 1)
            more = jnp.where(lane < 16, up, jnp.where(lane >= 112, low, 0.0))
            into[half, pl.ds(pl.multiple_of(16 * slot + 8 * h, 8), 8), :] = acc[half, y, 0, rows, :] + more

    def send_parts(half):
        for copy in rim_copies(half):
            copy.wait()

        def send_part(index, carry):
            to_a, to_b = whom(index)
            finish_owner(half, to_a, to_b, total, GY * to_a + to_b)

            @pl.when(index > 0)
            def _():
                part_copy(half, index - 1).start()

            return carry

        lax.fori_loop(0, OWNERS - 1, send_part, 0)
        finish_owner(half, a, b, parts, GY * a + b)
        part_copy(half, OWNERS - 2).start()

    def blend_group(half, step, first):
        weigh_group(half, step)
        for t in range(2):
            place_group(half, step, t, first)

    def blend_last(half, step):
        weigh_group(half, step)
        place_group(half, step, 1, False)
        send_rims(half)
        place_group(half, step, 0, False)

    blend_group(0, 0, True)
    blend_group(0, 1, False)
    blend_group(0, 3, False)
    blend_last(0, 2)
    blend_group(1, 0, True)
    send_parts(0)
    blend_group(1, 1, False)
    blend_group(1, 3, False)
    blend_last(1, 2)
    send_parts(1)

    for half in range(2):
        for step, turns in turns_of:
            for turn in turns:
                piece_copy(half, step, turn).wait_send()

        def await_part(index, carry, half=half):
            part_copy(half, index).wait()
            return carry

        lax.fori_loop(0, OWNERS - 1, await_part, 0)

    for x in range(BX):
        for h in range(2):
            for g in range(2):
                row = 8 * g * 16 + 8 * h + x
                norm = sums[4 * x + 2 * h + g]
                d1, d2 = [
                    (parts[half, pl.ds(row, 8, stride=16), :] + parts[half, pl.ds(row + 256, 8, stride=16), :]) / norm
                    for half in range(2)
                ]
                top = jnp.maximum(jnp.maximum(d1, d2), 0.0)
                e0, e1, e2 = jnp.exp(-top), jnp.exp(d1 - top), jnp.exp(d2 - top)
                scale = 1.0 / (e0 + e1 + e2)
                rows = slice(16 * h + 8 * g, 16 * h + 8 * g + 8)
                out_ref[x, 0, rows, :] = e0 * scale
                out_ref[x, 1, rows, :] = e1 * scale
                out_ref[x, 2, rows, :] = e2 * scale


def per_device(patch_logits, patch_start, patch_owner):
    tiles = patch_logits.reshape(GROUPS, 8, LAST + 1, 128)
    probs = pl.pallas_call(
        blend_kernel,
        out_shape=jax.ShapeDtypeStruct((BX, CLASSES, BY, BZ), F32),
        in_specs=[
            pl.BlockSpec(memory_space=pltpu.SMEM),
            pl.BlockSpec(memory_space=pltpu.SMEM),
            pl.BlockSpec(memory_space=pltpu.HBM),
        ],
        out_specs=pl.BlockSpec(memory_space=pltpu.VMEM),
        scratch_shapes=[
            pltpu.VMEM((GROUPS, LAST + 1, 8, 128), BF16),
            pltpu.VMEM((16, TILES[0], 8, 128), BF16),
            pltpu.VMEM((16, TILES[1], 8, 128), BF16),
            pltpu.VMEM((16, TILES[0], 8, 128), BF16),
            pltpu.VMEM((16, TILES[1], 8, 128), BF16),
            pltpu.VMEM((3 * PX, 8, 128), F32),
            pltpu.VMEM((32, 8, 128), F32),
            pltpu.VMEM((16, VROWS, 2, GROUPS, 8, 128), F32),
            pltpu.VMEM((4, VROWS + 1, 2, PX + 2 * MARGIN, 128), F32),
            pltpu.VMEM((2, 8, 2, 64, 128), F32),
            pltpu.VMEM((2, 2, 64, 128), F32),
            pltpu.VMEM((2, 2, 64, 128), F32),
            pltpu.VMEM((2, 16 * OWNERS, 128), F32),
            pltpu.VMEM((2, 16 * OWNERS, 128), F32),
            pltpu.SemaphoreType.DMA,
            pltpu.SemaphoreType.DMA((2, 16)),
            pltpu.SemaphoreType.DMA((2, 16)),
            pltpu.SemaphoreType.DMA((2, 2)),
            pltpu.SemaphoreType.DMA((2, 2)),
            pltpu.SemaphoreType.DMA((2, OWNERS)),
            pltpu.SemaphoreType.DMA((2, OWNERS)),
        ],
        compiler_params=pltpu.CompilerParams(collective_id=0, has_side_effects=True, vmem_limit_bytes=62000000),
    )(patch_owner, jnp.transpose(patch_start, (0, 3, 1, 2)), jnp.transpose(tiles, (0, 2, 1, 3)))
    return jnp.transpose(probs, (0, 2, 1, 3))


def solution(mesh):
    return jax.shard_map(
        per_device,
        mesh=mesh,
        in_specs=(P("gx", "gy", "gz", None, None), P(), P()),
        out_specs=P("gx", "gy", None, "gz"),
        check_vma=False,
    )
```

```python
import jax
import jax.numpy as jnp
from jax import lax
from jax.experimental import pallas as pl
from jax.experimental.pallas import tpu as pltpu
from jax.sharding import PartitionSpec as P

CLASSES = 3
BX, BY, BZ = 8, 32, 128
PX, PY, PZ = 24, 48, 144
GX, GY, GZ = 8, 4, 8
ROW = CLASSES * PZ
RES = 16
VROWS = PY // RES
GROUPS = PX // 8
TILES = (21, 11)
LAST = PY * ROW // 128 - 1
MARGIN = 5
SPAN = 13
OWNERS = GX * GY
F32 = jnp.float32
BF16 = jnp.bfloat16
MESH = pl.DeviceIdType.MESH


def profile(offsets, length):
    inside = (offsets >= 0) & (offsets < length)
    centre = (length - 1) / 2.0
    spread = length / 4.0
    values = jnp.exp(-((offsets.astype(F32) - centre) ** 2) / (2.0 * spread * spread))
    return jnp.where(inside, values, 0.0)


def iota(dim):
    return lax.broadcasted_iota(jnp.int32, (8, 128), dim)


def wrap(index, size):
    return lax.rem(index + size, size)


def hop_of(step, to_b):
    return (0, 1, 2 - 4 * lax.rem(to_b, 2), -1)[step]


def blend_kernel(
    owner_hbm, start_hbm, x_ref, out_ref,
    owner_ref, start_ref, patch, send0, send1, recv0, recv1, table, sums, kept, value, acc, rim, rims, total, parts,
    in_sem, owner_sem, start_sem, send_sem, recv_sem, rim_send, rim_recv, part_send, part_recv,
):
    a, b, k = lax.axis_index("gx"), lax.axis_index("gy"), lax.axis_index("gz")
    above, below = wrap(k + 1, GZ), wrap(k - 1, GZ)
    send, recv = (send0, send1), (recv0, recv1)
    near = [
        (wrap(a + dz, GX), wrap(b + db, GY), k) for dz in (0, 1, -1, 2, -2) for db in range(GY) if dz or db
    ] + [(a, b, above), (a, b, below)]
    barrier = pltpu.get_barrier_semaphore()
    for to in near:
        pl.semaphore_signal(barrier, inc=1, device_id=to, device_id_type=MESH)
    load = pltpu.make_async_copy(x_ref, patch, in_sem)
    load.start()
    indices = [
        pltpu.make_async_copy(owner_hbm, owner_ref, owner_sem),
        pltpu.make_async_copy(start_hbm, start_ref, start_sem),
    ]
    for copy in indices:
        copy.start()

    lane, sub = iota(1), iota(0)
    zero = jnp.zeros((8, 128), F32)

    def start_of(code, at_k, dim):
        return start_ref[code // GY, dim, lax.rem(code, GY), at_k]

    for copy in indices:
        copy.wait()
    my_sy = start_of(owner_ref[a, b, k], k, 1)
    load.wait()

    def cut(residue, store):
        rho = lax.rem(residue - my_sy + 8 * RES, RES)
        for half, (skip, length) in enumerate(((0, 2 * PZ), (2 * PZ, PZ))):
            for g in range(GROUPS):
                tiles = {}
                for v in range(VROWS):
                    into = length * v
                    delta = ROW * rho + (ROW * RES * v + skip - into)
                    first = (delta + 127) // 128
                    turn = first * 128 - delta
                    low, high = into // 128, (into + length - 1) // 128
                    turned = []
                    for t in range(low - 1, high + 1):
                        at = first + t
                        if t < 0:
                            at = jnp.maximum(at, 0)
                        if half == 1 and v == VROWS - 1 and t == high:
                            at = jnp.minimum(at, LAST)
                        turned.append(pltpu.roll(patch[g, at].astype(F32), turn, 1))
                    for t in range(low, high + 1):
                        tile = jnp.where(lane < turn, turned[t - low], turned[t - low + 1])
                        tiles[t] = jnp.where(lane < into % 128, tiles[t], tile) if t in tiles else tile
                for t in range(7 if half == 0 else 3):
                    store(half, GROUPS * t + g, tiles[t].astype(BF16))
                if half == 1:
                    if g == 0:
                        tail = tiles[3]
                    elif g == 1:
                        store(1, 9, jnp.where(lane < 48, tail, pltpu.roll(tiles[3], 48, 1)).astype(BF16))
                    else:
                        store(1, 10, tiles[3].astype(BF16))

    def piece_copy(half, step, turn):
        to_b = wrap(b + turn, GY)
        return pltpu.make_async_remote_copy(
            src_ref=send[half].at[4 * step + turn],
            dst_ref=recv[half].at[4 * step + b],
            send_sem=send_sem.at[half, 4 * step + turn],
            recv_sem=recv_sem.at[half, 4 * step + b],
            device_id=(wrap(a + hop_of(step, to_b), GX), to_b, k),
            device_id_type=MESH,
        )

    def piece_arrival(half, step, from_b):
        return pltpu.make_async_remote_copy(
            src_ref=send[half].at[4 * step],
            dst_ref=recv[half].at[4 * step + from_b],
            send_sem=send_sem.at[half, 4 * step],
            recv_sem=recv_sem.at[half, 4 * step + from_b],
            device_id=(a, b, above),
            device_id_type=MESH,
        )

    turns_of = ((2, range(GY)), (1, range(GY)), (3, range(GY)), (0, range(1, GY)))
    for step, turns in turns_of:

        def cut_one(turn, carry, step=step):
            residue = 4 * lax.rem(a + step, 4) + wrap(b + turn, GY)

            def store(half, tile, what):
                send[half][4 * step + turn, tile] = what

            cut(residue, store)
            return carry

        lax.fori_loop(turns.start, GY, cut_one, 0)
        if step == 2:
            pl.semaphore_wait(barrier, len(near))
        for turn in turns:
            piece_copy(0, step, turn).start()
    for step, turns in turns_of:
        for turn in turns:
            piece_copy(1, step, turn).start()

    def store_own(half, tile, what):
        recv[half][b, tile] = what

    cut(4 * lax.rem(a, 4) + b, store_own)

    for s in range(4):
        for t in range(2):
            for v in range(VROWS + 1):
                for at in range(SPAN):
                    if v == VROWS or not MARGIN <= at < MARGIN + GROUPS + 1:
                        value[s, v, t, at] = zero
    for offset in range(3 * PX):
        table[offset] = profile(jnp.full((8, 128), offset - PX, jnp.int32), PX)

    def add_weight(index, carry):
        i, j, at_k = a - 2 + index // 9, b - 1 + lax.rem(index // 3, 3), k - 1 + lax.rem(index, 3)
        valid = (i >= 0) & (i < GX) & (j >= 0) & (j < GY) & (at_k >= 0) & (at_k < GZ)
        i, j, at_k = jnp.clip(i, 0, GX - 1), jnp.clip(j, 0, GY - 1), jnp.clip(at_k, 0, GZ - 1)
        along_z = profile(BZ * k + lane - start_ref[i, 2, j, at_k], PZ)
        along_z = along_z * jnp.where(valid, 1.0, 0.0)
        y = BY * b + sub - start_ref[i, 1, j, at_k]
        planes = [profile(y + 8 * g, PY) * along_z for g in range(4)]
        base = jnp.clip(BX * a - start_ref[i, 0, j, at_k] + PX, 0, 2 * PX)
        new = []
        for x in range(BX):
            along_x = table[base + x]
            new += [carry[4 * x + g] + along_x * planes[g] for g in range(4)]
        return tuple(new)

    weights = lax.fori_loop(0, 45, add_weight, (zero,) * 32)
    for at in range(32):
        sums[at] = weights[at]

    residue = 4 * lax.rem(a, 4) + b
    along_x = [profile(sub + 8 * g, PX) for g in range(GROUPS)]
    columns = (lane, jnp.where(lane < 64, lane + 128, lane - 128))

    def corner(step, from_b):
        from_a = wrap(a - hop_of(step, b), GX)
        code = owner_ref[from_a, from_b, k]
        sy = start_of(code, k, 1)
        rho = lax.rem(residue - sy + 8 * RES, RES)
        return start_of(code, k, 0), (sy + rho) // RES, rho, start_of(code, k, 2) - BZ * k

    def aligned(first, second, shift, lead):
        turn = lax.rem(shift - lead + 512, 256)
        low = lax.rem(turn, 128)
        swap = (jnp.where(lane < low, 1, 0) + turn // 128) == 1
        first, second = pltpu.roll(first.astype(F32), low, 1), pltpu.roll(second.astype(F32), low, 1)
        return jnp.where(swap, second, first), jnp.where(swap, first, second)

    def weigh_group(half, step):
        def weigh(from_b, carry):
            slot = 4 * step + from_b
            if step == 0:

                @pl.when(from_b != b)
                def _():
                    piece_arrival(half, step, from_b).wait_recv()

            else:
                piece_arrival(half, step, from_b).wait_recv()
            sx, _, rho, shift = corner(step, from_b)
            turn_x = lax.rem(sx, 8)
            along_z = [profile(c - shift, PZ) for c in columns]
            for v in range(VROWS):
                along_y = profile(jnp.full((8, 128), RES * v, jnp.int32) + rho, PY)
                turned = [[], []]
                for g in range(GROUPS):
                    if half == 0:
                        pair = []
                        for m in (2 * v, 2 * v + 1):
                            ends = recv0[slot, GROUPS * m + g], recv0[slot, GROUPS * m + GROUPS + g]
                            pair.append(aligned(*ends, shift, 16 * m))
                        base, upper = pair
                        for t in range(2):
                            kept[slot, v, t, g] = base[t]
                    else:
                        first = recv1[slot, GROUPS * v + g].astype(F32)
                        if v < VROWS - 1:
                            second = recv1[slot, GROUPS * v + GROUPS + g].astype(F32)
                        else:
                            second = recv1[slot, 9 + g // 2].astype(F32)
                            second = pltpu.roll(second, 80, 1) if g == 1 else second
                        upper = aligned(first, second, shift, 16 * v)
                        base = [kept[slot, v, t, g] for t in range(2)]
                    along_xy = along_x[g] * along_y
                    for t in range(2):
                        product = (upper[t] - base[t]) * (along_xy * along_z[t])
                        turned[t].append(pltpu.roll(product, turn_x, 0))
                for t in range(2):
                    ends = [zero] + turned[t] + [zero]
                    for g in range(GROUPS + 1):
                        value[from_b, v, t, MARGIN + g] = jnp.where(sub < turn_x, ends[g], ends[g + 1])
            return carry

        lax.fori_loop(0, GY, weigh, 0)

    def place_group(half, step, t, first):
        corners = [corner(step, from_b) for from_b in range(GY)]

        def place(y, carry):
            places = []
            for sx, first_y, _, _ in corners:
                v = y - first_y
                places.append((jnp.where((v >= 0) & (v < VROWS), v, VROWS), MARGIN - sx // 8))
            for block in range(GX):
                rows = slice(8 * block, 8 * block + 8)
                got = None if first else acc[half, y, t, rows, :]
                for s, (v, at) in enumerate(places):
                    more = value[s, v, t, at + block]
                    got = more if got is None else got + more
                acc[half, y, t, rows, :] = got
            return carry

        lax.fori_loop(0, 8, place, 0)

    def rim_copies(half):
        return [
            pltpu.make_async_remote_copy(
                src_ref=rim.at[half, side],
                dst_ref=rims.at[half, side],
                send_sem=rim_send.at[half, side],
                recv_sem=rim_recv.at[half, side],
                device_id=(a, b, to_k),
                device_id_type=MESH,
            )
            for side, to_k in ((0, above), (1, below))
        ]

    def send_rims(half):
        for block in range(GX):
            rows = slice(8 * block, 8 * block + 8)
            up, low = zero, zero
            for y in range(8):
                turned = acc[half, y, 1, rows, :]
                turned = pltpu.roll(turned, 16 * y, 1) if y else turned
                up = jnp.where(lane // 16 == y, turned, up)
                low = jnp.where(lane // 16 == (y + 7) % 8, turned, low)
            rim[half, 0, rows, :] = up
            rim[half, 1, rows, :] = low
        for copy in rim_copies(half):
            copy.start()

    def whom(index):
        far = index // GY
        dz = 4 + ((far + 1) // 2) * (1 - 2 * lax.rem(far, 2))
        return wrap(a + dz, GX), wrap(b + lax.rem(index + 1, GY), GY)

    def part_copy(half, index):
        to_a, to_b = whom(index)
        return pltpu.make_async_remote_copy(
            src_ref=total.at[half, pl.ds(pl.multiple_of(16 * (GY * to_a + to_b), 16), 16)],
            dst_ref=parts.at[half, pl.ds(pl.multiple_of(16 * (GY * a + b), 16), 16)],
            send_sem=part_send.at[half, index],
            recv_sem=part_recv.at[half, index],
            device_id=(to_a, to_b, k),
            device_id_type=MESH,
        )

    def finish_block(half, block, store):
        rows = pl.ds(pl.multiple_of(8 * block, 8), 8)
        up, low = rims[half, 0, rows, :], rims[half, 1, rows, :]
        for y in range(8):
            back = (128 - 16 * y) % 128
            ends = (pltpu.roll(up, back, 1), pltpu.roll(low, back, 1)) if y else (up, low)
            more = jnp.where(lane < 16, ends[0], jnp.where(lane >= 112, ends[1], 0.0))
            store(y, acc[half, y, 0, rows, :] + more)

    def send_parts(half):
        for copy in rim_copies(half):
            copy.wait()

        def send_block(far, carry):
            block, _ = whom(GY * far)

            def store(y, what):
                total[half, pl.ds(pl.multiple_of(64 * block + 8 * y, 8), 8), :] = what

            finish_block(half, block, store)

            @pl.when(far > 0)
            def _():
                for turn in range(GY):
                    part_copy(half, GY * far - GY + turn).start()

            return carry

        lax.fori_loop(0, GX, send_block, 0)
        for turn in range(GY - 1):
            part_copy(half, OWNERS - GY + turn).start()
        mine = pl.ds(pl.multiple_of(16 * (GY * a + b), 16), 16)
        parts[half, mine, :] = total[half, mine, :]

    def blend_group(half, step, first):
        weigh_group(half, step)
        for t in range(2):
            place_group(half, step, t, first)

    def blend_last(half, step):
        weigh_group(half, step)
        place_group(half, step, 1, False)
        send_rims(half)
        place_group(half, step, 0, False)

    blend_group(0, 0, True)
    blend_group(0, 1, False)
    blend_group(0, 3, False)
    blend_last(0, 2)
    blend_group(1, 0, True)
    send_parts(0)
    blend_group(1, 1, False)
    blend_group(1, 3, False)
    blend_last(1, 2)
    send_parts(1)

    for half in range(2):
        for step, turns in turns_of:
            for turn in turns:
                piece_copy(half, step, turn).wait_send()

        def await_part(index, carry, half=half):
            part_copy(half, index).wait()
            return carry

        lax.fori_loop(0, OWNERS - 1, await_part, 0)

    for x in range(BX):
        for h in range(2):
            for g in range(2):
                row = 8 * g * 16 + 8 * h + x
                norm = sums[4 * x + 2 * h + g]
                d1, d2 = [
                    (parts[half, pl.ds(row, 8, stride=16), :] + parts[half, pl.ds(row + 256, 8, stride=16), :]) / norm
                    for half in range(2)
                ]
                top = jnp.maximum(jnp.maximum(d1, d2), 0.0)
                e0, e1, e2 = jnp.exp(-top), jnp.exp(d1 - top), jnp.exp(d2 - top)
                scale = 1.0 / (e0 + e1 + e2)
                rows = slice(16 * h + 8 * g, 16 * h + 8 * g + 8)
                out_ref[x, 0, rows, :] = e0 * scale
                out_ref[x, 1, rows, :] = e1 * scale
                out_ref[x, 2, rows, :] = e2 * scale


def per_device(patch_logits, patch_start, patch_owner):
    tiles = patch_logits.reshape(GROUPS, 8, LAST + 1, 128)
    probs = pl.pallas_call(
        blend_kernel,
        out_shape=jax.ShapeDtypeStruct((BX, CLASSES, BY, BZ), F32),
        in_specs=[
            pl.BlockSpec(memory_space=pl.ANY),
            pl.BlockSpec(memory_space=pl.ANY),
            pl.BlockSpec(memory_space=pl.ANY),
        ],
        out_specs=pl.BlockSpec(memory_space=pltpu.VMEM),
        scratch_shapes=[
            pltpu.SMEM((GX, GY, GZ), jnp.int32),
            pltpu.SMEM((GX, 3, GY, GZ), jnp.int32),
            pltpu.VMEM((GROUPS, LAST + 1, 8, 128), BF16),
            pltpu.VMEM((16, TILES[0], 8, 128), BF16),
            pltpu.VMEM((16, TILES[1], 8, 128), BF16),
            pltpu.VMEM((16, TILES[0], 8, 128), BF16),
            pltpu.VMEM((16, TILES[1], 8, 128), BF16),
            pltpu.VMEM((3 * PX, 8, 128), F32),
            pltpu.VMEM((32, 8, 128), F32),
            pltpu.VMEM((16, VROWS, 2, GROUPS, 8, 128), F32),
            pltpu.VMEM((4, VROWS + 1, 2, SPAN, 8, 128), F32),
            pltpu.VMEM((2, 8, 2, 64, 128), F32),
            pltpu.VMEM((2, 2, 64, 128), F32),
            pltpu.VMEM((2, 2, 64, 128), F32),
            pltpu.VMEM((2, 16 * OWNERS, 128), F32),
            pltpu.VMEM((2, 16 * OWNERS, 128), F32),
            pltpu.SemaphoreType.DMA,
            pltpu.SemaphoreType.DMA,
            pltpu.SemaphoreType.DMA,
            pltpu.SemaphoreType.DMA((2, 16)),
            pltpu.SemaphoreType.DMA((2, 16)),
            pltpu.SemaphoreType.DMA((2, 2)),
            pltpu.SemaphoreType.DMA((2, 2)),
            pltpu.SemaphoreType.DMA((2, OWNERS)),
            pltpu.SemaphoreType.DMA((2, OWNERS)),
        ],
        compiler_params=pltpu.CompilerParams(collective_id=0, has_side_effects=True, vmem_limit_bytes=62000000),
    )(patch_owner, jnp.transpose(patch_start, (0, 3, 1, 2)), jnp.transpose(tiles, (0, 2, 1, 3)))
    return jnp.transpose(probs, (0, 2, 1, 3))


def solution(mesh):
    return jax.shard_map(
        per_device,
        mesh=mesh,
        in_specs=(P("gx", "gy", "gz", None, None), P(), P()),
        out_specs=P("gx", "gy", None, "gz"),
        check_vma=False,
    )
```

```python
import jax
import jax.numpy as jnp
from jax import lax
from jax.experimental import pallas as pl
from jax.experimental.pallas import tpu as pltpu
from jax.sharding import PartitionSpec as P

CLASSES = 3
BX, BY, BZ = 8, 32, 128
PX, PY, PZ = 24, 48, 144
GX, GY, GZ = 8, 4, 8
ROW = CLASSES * PZ
RES = 16
VROWS = PY // RES
GROUPS = PX // 8
TILES = (21, 11)
LAST = PY * ROW // 128 - 1
MARGIN = 5
SPAN = 13
OWNERS = GX * GY
F32 = jnp.float32
BF16 = jnp.bfloat16
MESH = pl.DeviceIdType.MESH


def profile(offsets, length):
    inside = (offsets >= 0) & (offsets < length)
    centre = (length - 1) / 2.0
    spread = length / 4.0
    values = jnp.exp(-((offsets.astype(F32) - centre) ** 2) / (2.0 * spread * spread))
    return jnp.where(inside, values, 0.0)


def iota(dim):
    return lax.broadcasted_iota(jnp.int32, (8, 128), dim)


def wrap(index, size):
    return lax.rem(index + size, size)


def hop_of(step, to_b):
    return (0, 1, 2 - 4 * lax.rem(to_b, 2), -1)[step]


def blend_kernel(
    owner_hbm, start_hbm, x_ref, out_ref,
    owner_ref, start_ref, patch, send0, send1, recv0, recv1, table, sums, kept, value, acc, rim, rims, total, parts,
    in_sem, owner_sem, start_sem, send_sem, recv_sem, rim_send, rim_recv, part_send, part_recv,
):
    a, b, k = lax.axis_index("gx"), lax.axis_index("gy"), lax.axis_index("gz")
    above, below = wrap(k + 1, GZ), wrap(k - 1, GZ)
    send, recv = (send0, send1), (recv0, recv1)
    near = [
        (wrap(a + dz, GX), wrap(b + db, GY), k) for dz in (0, 1, -1, 2, -2) for db in range(GY) if dz or db
    ] + [(a, b, above), (a, b, below)]
    barrier = pltpu.get_barrier_semaphore()
    for to in near:
        pl.semaphore_signal(barrier, inc=1, device_id=to, device_id_type=MESH)
    load = pltpu.make_async_copy(x_ref, patch, in_sem)
    load.start()
    indices = [
        pltpu.make_async_copy(owner_hbm, owner_ref, owner_sem),
        pltpu.make_async_copy(start_hbm, start_ref, start_sem),
    ]
    for copy in indices:
        copy.start()

    lane, sub = iota(1), iota(0)
    zero = jnp.zeros((8, 128), F32)

    def start_of(code, at_k, dim):
        return start_ref[code // GY, dim, lax.rem(code, GY), at_k]

    for copy in indices:
        copy.wait()
    my_sy = start_of(owner_ref[a, b, k], k, 1)
    load.wait()

    def cut(residue, store):
        rho = lax.rem(residue - my_sy + 8 * RES, RES)
        for half, (skip, length) in enumerate(((0, 2 * PZ), (2 * PZ, PZ))):
            for g in range(GROUPS):
                tiles = {}
                for v in range(VROWS):
                    into = length * v
                    delta = ROW * rho + (ROW * RES * v + skip - into)
                    first = (delta + 127) // 128
                    turn = first * 128 - delta
                    low, high = into // 128, (into + length - 1) // 128
                    turned = []
                    for t in range(low - 1, high + 1):
                        at = first + t
                        if t < 0:
                            at = jnp.maximum(at, 0)
                        if half == 1 and v == VROWS - 1 and t == high:
                            at = jnp.minimum(at, LAST)
                        turned.append(pltpu.roll(patch[g, at].astype(F32), turn, 1))
                    for t in range(low, high + 1):
                        tile = jnp.where(lane < turn, turned[t - low], turned[t - low + 1])
                        tiles[t] = jnp.where(lane < into % 128, tiles[t], tile) if t in tiles else tile
                for t in range(7 if half == 0 else 3):
                    store(half, GROUPS * t + g, tiles[t].astype(BF16))
                if half == 1:
                    if g == 0:
                        tail = tiles[3]
                    elif g == 1:
                        store(1, 9, jnp.where(lane < 48, tail, pltpu.roll(tiles[3], 48, 1)).astype(BF16))
                    else:
                        store(1, 10, tiles[3].astype(BF16))

    def piece_copy(half, step, turn):
        to_b = wrap(b + turn, GY)
        return pltpu.make_async_remote_copy(
            src_ref=send[half].at[4 * step + turn],
            dst_ref=recv[half].at[4 * step + b],
            send_sem=send_sem.at[half, 4 * step + turn],
            recv_sem=recv_sem.at[half, 4 * step + b],
            device_id=(wrap(a + hop_of(step, to_b), GX), to_b, k),
            device_id_type=MESH,
        )

    def piece_arrival(half, step, from_b):
        return pltpu.make_async_remote_copy(
            src_ref=send[half].at[4 * step],
            dst_ref=recv[half].at[4 * step + from_b],
            send_sem=send_sem.at[half, 4 * step],
            recv_sem=recv_sem.at[half, 4 * step + from_b],
            device_id=(a, b, above),
            device_id_type=MESH,
        )

    turns_of = ((2, range(GY)), (1, range(GY)), (3, range(GY)), (0, range(1, GY)))
    for step, turns in turns_of:

        def cut_one(turn, carry, step=step):
            residue = 4 * lax.rem(a + step, 4) + wrap(b + turn, GY)

            def store(half, tile, what):
                send[half][4 * step + turn, tile] = what

            cut(residue, store)
            return carry

        lax.fori_loop(turns.start, GY, cut_one, 0)
        if step == 2:
            pl.semaphore_wait(barrier, len(near))
        for turn in turns:
            piece_copy(0, step, turn).start()
    for step, turns in turns_of:
        for turn in turns:
            piece_copy(1, step, turn).start()

    def store_own(half, tile, what):
        recv[half][b, tile] = what

    cut(4 * lax.rem(a, 4) + b, store_own)

    for s in range(4):
        for t in range(2):
            for v in range(VROWS + 1):
                for at in range(SPAN):
                    if v == VROWS or not MARGIN <= at < MARGIN + GROUPS + 1:
                        value[s, v, t, at] = zero
    for offset in range(3 * PX):
        table[offset] = profile(jnp.full((8, 128), offset - PX, jnp.int32), PX)

    def add_weight(index, carry):
        i, j, at_k = a - 2 + index // 9, b - 1 + lax.rem(index // 3, 3), k - 1 + lax.rem(index, 3)
        valid = (i >= 0) & (i < GX) & (j >= 0) & (j < GY) & (at_k >= 0) & (at_k < GZ)
        i, j, at_k = jnp.clip(i, 0, GX - 1), jnp.clip(j, 0, GY - 1), jnp.clip(at_k, 0, GZ - 1)
        along_z = profile(BZ * k + lane - start_ref[i, 2, j, at_k], PZ)
        along_z = along_z * jnp.where(valid, 1.0, 0.0)
        y = BY * b + sub - start_ref[i, 1, j, at_k]
        planes = [profile(y + 8 * g, PY) * along_z for g in range(4)]
        base = jnp.clip(BX * a - start_ref[i, 0, j, at_k] + PX, 0, 2 * PX)
        new = []
        for x in range(BX):
            along_x = table[base + x]
            new += [carry[4 * x + g] + along_x * planes[g] for g in range(4)]
        return tuple(new)

    weights = lax.fori_loop(0, 45, add_weight, (zero,) * 32)
    for at in range(32):
        sums[at] = weights[at]

    residue = 4 * lax.rem(a, 4) + b
    along_x = [profile(sub + 8 * g, PX) for g in range(GROUPS)]
    columns = (lane, jnp.where(lane < 64, lane + 128, lane - 128))

    def corner(step, from_b):
        from_a = wrap(a - hop_of(step, b), GX)
        code = owner_ref[from_a, from_b, k]
        sy = start_of(code, k, 1)
        rho = lax.rem(residue - sy + 8 * RES, RES)
        return start_of(code, k, 0), (sy + rho) // RES, rho, start_of(code, k, 2) - BZ * k

    def aligned(first, second, shift, lead):
        turn = lax.rem(shift - lead + 512, 256)
        low = lax.rem(turn, 128)
        swap = (jnp.where(lane < low, 1, 0) + turn // 128) == 1
        first, second = pltpu.roll(first.astype(F32), low, 1), pltpu.roll(second.astype(F32), low, 1)
        return jnp.where(swap, second, first), jnp.where(swap, first, second)

    def weigh_group(half, step):
        def weigh(from_b, carry):
            slot = 4 * step + from_b
            if step == 0:

                @pl.when(from_b != b)
                def _():
                    piece_arrival(half, step, from_b).wait_recv()

            else:
                piece_arrival(half, step, from_b).wait_recv()
            sx, _, rho, shift = corner(step, from_b)
            turn_x = lax.rem(sx, 8)
            along_z = [profile(c - shift, PZ) for c in columns]
            for v in range(VROWS):
                along_y = profile(jnp.full((8, 128), RES * v, jnp.int32) + rho, PY)
                turned, bases = [[], []], []
                for g in range(GROUPS):
                    if half == 0:
                        pair = []
                        for m in (2 * v, 2 * v + 1):
                            ends = recv0[slot, GROUPS * m + g], recv0[slot, GROUPS * m + GROUPS + g]
                            pair.append(aligned(*ends, shift, 16 * m))
                        base, upper = pair
                        bases.append(base)
                    else:
                        first = recv1[slot, GROUPS * v + g].astype(F32)
                        if v < VROWS - 1:
                            second = recv1[slot, GROUPS * v + GROUPS + g].astype(F32)
                        else:
                            second = recv1[slot, 9 + g // 2].astype(F32)
                            second = pltpu.roll(second, 80, 1) if g == 1 else second
                        upper = aligned(first, second, shift, 16 * v)
                        base = [kept[slot, v, t, g] for t in range(2)]
                    along_xy = along_x[g] * along_y
                    for t in range(2):
                        product = (upper[t] - base[t]) * (along_xy * along_z[t])
                        turned[t].append(pltpu.roll(product, turn_x, 0))
                for g, base in enumerate(bases):
                    for t in range(2):
                        kept[slot, v, t, g] = base[t]
                for t in range(2):
                    ends = [zero] + turned[t] + [zero]
                    for g in range(GROUPS + 1):
                        value[from_b, v, t, MARGIN + g] = jnp.where(sub < turn_x, ends[g], ends[g + 1])
            return carry

        lax.fori_loop(0, GY, weigh, 0)

    def place_group(half, step, lane_tiles, first):
        corners = [corner(step, from_b) for from_b in range(GY)]

        def place(y, carry):
            places = []
            for sx, first_y, _, _ in corners:
                v = y - first_y
                places.append((jnp.where((v >= 0) & (v < VROWS), v, VROWS), MARGIN - sx // 8))
            sums_of = {}
            for t in lane_tiles:
                for block in range(GX):
                    one, two, three, four = [value[s, v, t, at + block] for s, (v, at) in enumerate(places)]
                    got = (one + two) + (three + four)
                    if not first:
                        got = got + acc[half, y, t, 8 * block : 8 * block + 8, :]
                    sums_of[t, block] = got
            for (t, block), got in sums_of.items():
                acc[half, y, t, 8 * block : 8 * block + 8, :] = got
            return carry

        lax.fori_loop(0, 8, place, 0)

    def rim_copies(half):
        return [
            pltpu.make_async_remote_copy(
                src_ref=rim.at[half, side],
                dst_ref=rims.at[half, side],
                send_sem=rim_send.at[half, side],
                recv_sem=rim_recv.at[half, side],
                device_id=(a, b, to_k),
                device_id_type=MESH,
            )
            for side, to_k in ((0, above), (1, below))
        ]

    def send_rims(half):
        for block in range(GX):
            rows = slice(8 * block, 8 * block + 8)
            up, low = zero, zero
            for y in range(8):
                turned = acc[half, y, 1, rows, :]
                turned = pltpu.roll(turned, 16 * y, 1) if y else turned
                up = jnp.where(lane // 16 == y, turned, up)
                low = jnp.where(lane // 16 == (y + 7) % 8, turned, low)
            rim[half, 0, rows, :] = up
            rim[half, 1, rows, :] = low
        for copy in rim_copies(half):
            copy.start()

    def whom(index):
        far = index // GY
        dz = 4 + ((far + 1) // 2) * (1 - 2 * lax.rem(far, 2))
        return wrap(a + dz, GX), wrap(b + lax.rem(index + 1, GY), GY)

    def part_copy(half, index):
        to_a, to_b = whom(index)
        return pltpu.make_async_remote_copy(
            src_ref=total.at[half, pl.ds(pl.multiple_of(16 * (GY * to_a + to_b), 16), 16)],
            dst_ref=parts.at[half, pl.ds(pl.multiple_of(16 * (GY * a + b), 16), 16)],
            send_sem=part_send.at[half, index],
            recv_sem=part_recv.at[half, index],
            device_id=(to_a, to_b, k),
            device_id_type=MESH,
        )

    def finish_block(half, block):
        rows = pl.ds(pl.multiple_of(8 * block, 8), 8)
        up, low = rims[half, 0, rows, :], rims[half, 1, rows, :]
        cells = []
        for y in range(8):
            back = (128 - 16 * y) % 128
            ends = (pltpu.roll(up, back, 1), pltpu.roll(low, back, 1)) if y else (up, low)
            more = jnp.where(lane < 16, ends[0], jnp.where(lane >= 112, ends[1], 0.0))
            cells.append(acc[half, y, 0, rows, :] + more)
        for y, what in enumerate(cells):
            total[half, pl.ds(pl.multiple_of(64 * block + 8 * y, 8), 8), :] = what

    def send_parts(half):
        for copy in rim_copies(half):
            copy.wait()

        def send_block(far, carry):
            block, _ = whom(GY * far)
            finish_block(half, block)

            @pl.when(far > 0)
            def _():
                for turn in range(GY):
                    part_copy(half, GY * far - GY + turn).start()

            return carry

        lax.fori_loop(0, GX, send_block, 0)
        for turn in range(GY - 1):
            part_copy(half, OWNERS - GY + turn).start()
        mine = pl.ds(pl.multiple_of(16 * (GY * a + b), 16), 16)
        parts[half, mine, :] = total[half, mine, :]

    def blend_group(half, step, first):
        weigh_group(half, step)
        place_group(half, step, (0, 1), first)

    def blend_last(half, step):
        weigh_group(half, step)
        place_group(half, step, (1,), False)
        send_rims(half)
        place_group(half, step, (0,), False)

    blend_group(0, 0, True)
    blend_group(0, 1, False)
    blend_group(0, 3, False)
    blend_last(0, 2)
    blend_group(1, 0, True)
    send_parts(0)
    blend_group(1, 1, False)
    blend_group(1, 3, False)
    blend_last(1, 2)
    send_parts(1)

    for half in range(2):
        for step, turns in turns_of:
            for turn in turns:
                piece_copy(half, step, turn).wait_send()

        def await_part(index, carry, half=half):
            part_copy(half, index).wait()
            return carry

        lax.fori_loop(0, OWNERS - 1, await_part, 0)

    for x in range(BX):
        for h in range(2):
            for g in range(2):
                row = 8 * g * 16 + 8 * h + x
                norm = sums[4 * x + 2 * h + g]
                d1, d2 = [
                    (parts[half, pl.ds(row, 8, stride=16), :] + parts[half, pl.ds(row + 256, 8, stride=16), :]) / norm
                    for half in range(2)
                ]
                top = jnp.maximum(jnp.maximum(d1, d2), 0.0)
                e0, e1, e2 = jnp.exp(-top), jnp.exp(d1 - top), jnp.exp(d2 - top)
                scale = 1.0 / (e0 + e1 + e2)
                rows = slice(16 * h + 8 * g, 16 * h + 8 * g + 8)
                out_ref[x, 0, rows, :] = e0 * scale
                out_ref[x, 1, rows, :] = e1 * scale
                out_ref[x, 2, rows, :] = e2 * scale


def per_device(patch_logits, patch_start, patch_owner):
    tiles = patch_logits.reshape(GROUPS, 8, LAST + 1, 128)
    probs = pl.pallas_call(
        blend_kernel,
        out_shape=jax.ShapeDtypeStruct((BX, CLASSES, BY, BZ), F32),
        in_specs=[
            pl.BlockSpec(memory_space=pl.ANY),
            pl.BlockSpec(memory_space=pl.ANY),
            pl.BlockSpec(memory_space=pl.ANY),
        ],
        out_specs=pl.BlockSpec(memory_space=pltpu.VMEM),
        scratch_shapes=[
            pltpu.SMEM((GX, GY, GZ), jnp.int32),
            pltpu.SMEM((GX, 3, GY, GZ), jnp.int32),
            pltpu.VMEM((GROUPS, LAST + 1, 8, 128), BF16),
            pltpu.VMEM((16, TILES[0], 8, 128), BF16),
            pltpu.VMEM((16, TILES[1], 8, 128), BF16),
            pltpu.VMEM((16, TILES[0], 8, 128), BF16),
            pltpu.VMEM((16, TILES[1], 8, 128), BF16),
            pltpu.VMEM((3 * PX, 8, 128), F32),
            pltpu.VMEM((32, 8, 128), F32),
            pltpu.VMEM((16, VROWS, 2, GROUPS, 8, 128), F32),
            pltpu.VMEM((4, VROWS + 1, 2, SPAN, 8, 128), F32),
            pltpu.VMEM((2, 8, 2, 64, 128), F32),
            pltpu.VMEM((2, 2, 64, 128), F32),
            pltpu.VMEM((2, 2, 64, 128), F32),
            pltpu.VMEM((2, 16 * OWNERS, 128), F32),
            pltpu.VMEM((2, 16 * OWNERS, 128), F32),
            pltpu.SemaphoreType.DMA,
            pltpu.SemaphoreType.DMA,
            pltpu.SemaphoreType.DMA,
            pltpu.SemaphoreType.DMA((2, 16)),
            pltpu.SemaphoreType.DMA((2, 16)),
            pltpu.SemaphoreType.DMA((2, 2)),
            pltpu.SemaphoreType.DMA((2, 2)),
            pltpu.SemaphoreType.DMA((2, OWNERS)),
            pltpu.SemaphoreType.DMA((2, OWNERS)),
        ],
        compiler_params=pltpu.CompilerParams(collective_id=0, has_side_effects=True, vmem_limit_bytes=62000000),
    )(patch_owner, jnp.transpose(patch_start, (0, 3, 1, 2)), jnp.transpose(tiles, (0, 2, 1, 3)))
    return jnp.transpose(probs, (0, 2, 1, 3))


def solution(mesh):
    return jax.shard_map(
        per_device,
        mesh=mesh,
        in_specs=(P("gx", "gy", "gz", None, None), P(), P()),
        out_specs=P("gx", "gy", None, "gz"),
        check_vma=False,
    )
```

```python
import jax
import jax.numpy as jnp
from jax import lax
from jax.experimental import pallas as pl
from jax.experimental.pallas import tpu as pltpu
from jax.sharding import PartitionSpec as P

CLASSES = 3
BX, BY, BZ = 8, 32, 128
PX, PY, PZ = 24, 48, 144
GX, GY, GZ = 8, 4, 8
ROW = CLASSES * PZ
RES = 16
VROWS = PY // RES
GROUPS = PX // 8
TILES = (21, 11)
LAST = PY * ROW // 128 - 1
MARGIN = 5
SPAN = 13
OWNERS = GX * GY
F32 = jnp.float32
BF16 = jnp.bfloat16
MESH = pl.DeviceIdType.MESH


def profile(offsets, length):
    inside = (offsets >= 0) & (offsets < length)
    centre = (length - 1) / 2.0
    spread = length / 4.0
    values = jnp.exp(-((offsets.astype(F32) - centre) ** 2) / (2.0 * spread * spread))
    return jnp.where(inside, values, 0.0)


def iota(dim):
    return lax.broadcasted_iota(jnp.int32, (8, 128), dim)


def wrap(index, size):
    return index & (size - 1)


def halved(index, times):
    return lax.shift_right_logical(index, jnp.int32(times))


def hop_of(step, to_b):
    return (0, 1, 2 - 4 * (to_b & 1), -1)[step]


def blend_kernel(
    owner_hbm, start_hbm, x_ref, out_ref,
    owner_ref, start_ref, patch, send0, send1, recv0, recv1, table, sums, kept, value, acc, rim, rims, total, parts,
    in_sem, owner_sem, start_sem, send_sem, recv_sem, rim_send, rim_recv, part_send, part_recv,
):
    a, b, k = lax.axis_index("gx"), lax.axis_index("gy"), lax.axis_index("gz")
    above, below = wrap(k + 1, GZ), wrap(k - 1, GZ)
    send, recv = (send0, send1), (recv0, recv1)
    near = [
        (wrap(a + dz, GX), wrap(b + db, GY), k) for dz in (0, 1, -1, 2, -2) for db in range(GY) if dz or db
    ] + [(a, b, above), (a, b, below)]
    barrier = pltpu.get_barrier_semaphore()
    for to in near:
        pl.semaphore_signal(barrier, inc=1, device_id=to, device_id_type=MESH)
    load = pltpu.make_async_copy(x_ref, patch, in_sem)
    load.start()
    indices = [
        pltpu.make_async_copy(owner_hbm, owner_ref, owner_sem),
        pltpu.make_async_copy(start_hbm, start_ref, start_sem),
    ]
    for copy in indices:
        copy.start()

    lane, sub = iota(1), iota(0)
    zero = jnp.zeros((8, 128), F32)

    def start_of(code, at_k, dim):
        return start_ref[halved(code, 2), dim, code & (GY - 1), at_k]

    for copy in indices:
        copy.wait()
    my_sy = start_of(owner_ref[a, b, k], k, 1)
    load.wait()

    def cut(residue, store):
        rho = (residue - my_sy) & (RES - 1)
        tails = []
        for g in range(GROUPS):
            done = []
            for half, (skip, length) in enumerate(((0, 2 * PZ), (2 * PZ, PZ))):
                tiles = {}
                for v in range(VROWS):
                    into = length * v
                    delta = ROW * rho + (ROW * RES * v + skip - into)
                    first = halved(delta + 127, 7)
                    turn = first * 128 - delta
                    low, high = into // 128, (into + length - 1) // 128
                    turned = []
                    for t in range(low - 1, high + 1):
                        at = first + t
                        if t < 0:
                            at = jnp.maximum(at, 0)
                        if half == 1 and v == VROWS - 1 and t == high:
                            at = jnp.minimum(at, LAST)
                        turned.append(pltpu.roll(patch[g, at].astype(F32), turn, 1))
                    for t in range(low, high + 1):
                        tile = jnp.where(lane < turn, turned[t - low], turned[t - low + 1])
                        tiles[t] = jnp.where(lane < into % 128, tiles[t], tile) if t in tiles else tile
                done.append(tiles)
            for t in range(7):
                store(0, GROUPS * t + g, done[0][t].astype(BF16))
            for t in range(3):
                store(1, GROUPS * t + g, done[1][t].astype(BF16))
            tails.append(done[1][3])
        store(1, 9, jnp.where(lane < 48, tails[0], pltpu.roll(tails[1], 48, 1)).astype(BF16))
        store(1, 10, tails[2].astype(BF16))

    def piece_copy(half, step, turn):
        to_b = wrap(b + turn, GY)
        return pltpu.make_async_remote_copy(
            src_ref=send[half].at[4 * step + turn],
            dst_ref=recv[half].at[4 * step + b],
            send_sem=send_sem.at[half, 4 * step + turn],
            recv_sem=recv_sem.at[half, 4 * step + b],
            device_id=(wrap(a + hop_of(step, to_b), GX), to_b, k),
            device_id_type=MESH,
        )

    def piece_arrival(half, step, from_b):
        return pltpu.make_async_remote_copy(
            src_ref=send[half].at[4 * step],
            dst_ref=recv[half].at[4 * step + from_b],
            send_sem=send_sem.at[half, 4 * step],
            recv_sem=recv_sem.at[half, 4 * step + from_b],
            device_id=(a, b, above),
            device_id_type=MESH,
        )

    turns_of = ((2, range(GY)), (1, range(GY)), (3, range(GY)), (0, range(1, GY)))
    for step, turns in turns_of:

        def cut_one(turn, carry, step=step):
            residue = 4 * wrap(a + step, 4) + wrap(b + turn, GY)

            def store(half, tile, what):
                send[half][4 * step + turn, tile] = what

            cut(residue, store)
            return carry

        lax.fori_loop(turns.start, GY, cut_one, 0)
        if step == 2:
            pl.semaphore_wait(barrier, len(near))
        for turn in turns:
            piece_copy(0, step, turn).start()
    for step, turns in turns_of:
        for turn in turns:
            piece_copy(1, step, turn).start()

    def store_own(half, tile, what):
        recv[half][b, tile] = what

    cut(4 * wrap(a, 4) + b, store_own)

    for s in range(4):
        for t in range(2):
            for v in range(VROWS + 1):
                for at in range(SPAN):
                    if v == VROWS or not MARGIN <= at < MARGIN + GROUPS + 1:
                        value[s, v, t, at] = zero
    for offset in range(3 * PX):
        table[offset] = profile(jnp.full((8, 128), offset - PX, jnp.int32), PX)

    def add_weight(index, carry):
        i, j, at_k = a - 2 + lax.div(index, 9), b - 1 + lax.rem(lax.div(index, 3), 3), k - 1 + lax.rem(index, 3)
        valid = (i >= 0) & (i < GX) & (j >= 0) & (j < GY) & (at_k >= 0) & (at_k < GZ)
        i, j, at_k = jnp.clip(i, 0, GX - 1), jnp.clip(j, 0, GY - 1), jnp.clip(at_k, 0, GZ - 1)
        along_z = profile(BZ * k + lane - start_ref[i, 2, j, at_k], PZ)
        along_z = along_z * jnp.where(valid, 1.0, 0.0)
        y = BY * b + sub - start_ref[i, 1, j, at_k]
        planes = [profile(y + 8 * g, PY) * along_z for g in range(4)]
        base = jnp.clip(BX * a - start_ref[i, 0, j, at_k] + PX, 0, 2 * PX)
        new = []
        for x in range(BX):
            along_x = table[base + x]
            new += [carry[4 * x + g] + along_x * planes[g] for g in range(4)]
        return tuple(new)

    weights = lax.fori_loop(0, 45, add_weight, (zero,) * 32)
    for at in range(32):
        sums[at] = weights[at]

    residue = 4 * wrap(a, 4) + b
    along_x = [profile(sub + 8 * g, PX) for g in range(GROUPS)]
    columns = (lane, jnp.where(lane < 64, lane + 128, lane - 128))

    def corner(step, from_b):
        from_a = wrap(a - hop_of(step, b), GX)
        code = owner_ref[from_a, from_b, k]
        sy = start_of(code, k, 1)
        rho = (residue - sy) & (RES - 1)
        return start_of(code, k, 0), halved(sy + rho, 4), rho, start_of(code, k, 2) - BZ * k

    def aligned(first, second, shift, lead):
        turn = (shift - lead) & 255
        low = turn & 127
        swap = (jnp.where(lane < low, 1, 0) + halved(turn, 7)) == 1
        first, second = pltpu.roll(first.astype(F32), low, 1), pltpu.roll(second.astype(F32), low, 1)
        return jnp.where(swap, second, first), jnp.where(swap, first, second)

    def weigh_group(half, step):
        def weigh(from_b, carry):
            slot = 4 * step + from_b
            if step == 0:

                @pl.when(from_b != b)
                def _():
                    piece_arrival(half, step, from_b).wait_recv()

            else:
                piece_arrival(half, step, from_b).wait_recv()
            sx, _, rho, shift = corner(step, from_b)
            turn_x = sx & 7
            along_z = [profile(c - shift, PZ) for c in columns]
            held = {}
            for v in range(VROWS):
                for g in range(GROUPS):
                    if half == 0:
                        for m in (2 * v, 2 * v + 1):
                            held[m, g] = recv0[slot, GROUPS * m + g], recv0[slot, GROUPS * m + GROUPS + g]
                    else:
                        tail = 9 + g // 2 if v == VROWS - 1 else GROUPS * v + GROUPS + g
                        held[v, g] = recv1[slot, GROUPS * v + g], recv1[slot, tail]
                        held[v, g, 0] = [kept[slot, v, t, g] for t in range(2)]
            for v in range(VROWS):
                along_y = profile(jnp.full((8, 128), RES * v, jnp.int32) + rho, PY)
                turned = [[], []]
                for g in range(GROUPS):
                    if half == 0:
                        base, upper = [aligned(*held[m, g], shift, 16 * m) for m in (2 * v, 2 * v + 1)]
                        for t in range(2):
                            kept[slot, v, t, g] = base[t]
                    else:
                        first, second = held[v, g]
                        if v == VROWS - 1 and g == 1:
                            second = pltpu.roll(second.astype(F32), 80, 1)
                        upper = aligned(first, second, shift, 16 * v)
                        base = held[v, g, 0]
                    along_xy = along_x[g] * along_y
                    for t in range(2):
                        product = (upper[t] - base[t]) * (along_xy * along_z[t])
                        turned[t].append(pltpu.roll(product, turn_x, 0))
                for t in range(2):
                    ends = [zero] + turned[t] + [zero]
                    for g in range(GROUPS + 1):
                        value[from_b, v, t, MARGIN + g] = jnp.where(sub < turn_x, ends[g], ends[g + 1])
            return carry

        lax.fori_loop(0, GY, weigh, 0)

    def place_group(half, step, lane_tiles, first):
        corners = [corner(step, from_b) for from_b in range(GY)]

        def place(y, carry):
            places = []
            for sx, first_y, _, _ in corners:
                v = y - first_y
                places.append((jnp.where((v >= 0) & (v < VROWS), v, VROWS), MARGIN - halved(sx, 3)))
            loaded = [{t: value[s, v, t, pl.ds(at, GX)] for t in lane_tiles} for s, (v, at) in enumerate(places)]
            sums_of = {}
            for t in lane_tiles:
                for block in range(GX):
                    one, two, three, four = [tiles[t][block] for tiles in loaded]
                    got = (one + two) + (three + four)
                    if not first:
                        got = got + acc[half, y, t, 8 * block : 8 * block + 8, :]
                    sums_of[t, block] = got
            for (t, block), got in sums_of.items():
                acc[half, y, t, 8 * block : 8 * block + 8, :] = got
            return carry

        lax.fori_loop(0, 8, place, 0)

    def rim_copies(half):
        return [
            pltpu.make_async_remote_copy(
                src_ref=rim.at[half, side],
                dst_ref=rims.at[half, side],
                send_sem=rim_send.at[half, side],
                recv_sem=rim_recv.at[half, side],
                device_id=(a, b, to_k),
                device_id_type=MESH,
            )
            for side, to_k in ((0, above), (1, below))
        ]

    def send_rims(half):
        for block in range(GX):
            rows = slice(8 * block, 8 * block + 8)
            up, low = zero, zero
            for y in range(8):
                turned = acc[half, y, 1, rows, :]
                turned = pltpu.roll(turned, 16 * y, 1) if y else turned
                up = jnp.where(lane // 16 == y, turned, up)
                low = jnp.where(lane // 16 == (y + 7) % 8, turned, low)
            rim[half, 0, rows, :] = up
            rim[half, 1, rows, :] = low
        for copy in rim_copies(half):
            copy.start()

    def whom(index):
        far = halved(index, 2)
        dz = 4 + halved(far + 1, 1) * (1 - 2 * (far & 1))
        return wrap(a + dz, GX), wrap(b + index + 1, GY)

    def part_copy(half, index):
        to_a, to_b = whom(index)
        return pltpu.make_async_remote_copy(
            src_ref=total.at[half, pl.ds(pl.multiple_of(16 * (GY * to_a + to_b), 16), 16)],
            dst_ref=parts.at[half, pl.ds(pl.multiple_of(16 * (GY * a + b), 16), 16)],
            send_sem=part_send.at[half, index],
            recv_sem=part_recv.at[half, index],
            device_id=(to_a, to_b, k),
            device_id_type=MESH,
        )

    def finish_block(half, block):
        rows = pl.ds(pl.multiple_of(8 * block, 8), 8)
        up, low = rims[half, 0, rows, :], rims[half, 1, rows, :]
        cells = []
        for y in range(8):
            back = (128 - 16 * y) % 128
            ends = (pltpu.roll(up, back, 1), pltpu.roll(low, back, 1)) if y else (up, low)
            more = jnp.where(lane < 16, ends[0], jnp.where(lane >= 112, ends[1], 0.0))
            cells.append(acc[half, y, 0, rows, :] + more)
        for y, what in enumerate(cells):
            total[half, pl.ds(pl.multiple_of(64 * block + 8 * y, 8), 8), :] = what

    def send_parts(half):
        for copy in rim_copies(half):
            copy.wait()

        def send_block(far, carry):
            block, _ = whom(jnp.int32(GY) * far)
            finish_block(half, block)

            @pl.when(far > 0)
            def _():
                for turn in range(GY):
                    part_copy(half, GY * far - GY + turn).start()

            return carry

        lax.fori_loop(0, GX, send_block, 0)
        for turn in range(GY - 1):
            part_copy(half, OWNERS - GY + turn).start()
        mine = pl.ds(pl.multiple_of(16 * (GY * a + b), 16), 16)
        parts[half, mine, :] = total[half, mine, :]

    def blend_group(half, step, first):
        weigh_group(half, step)
        place_group(half, step, (0, 1), first)

    def blend_last(half, step):
        weigh_group(half, step)
        place_group(half, step, (1,), False)
        send_rims(half)
        place_group(half, step, (0,), False)

    blend_group(0, 0, True)
    blend_group(0, 1, False)
    blend_group(0, 3, False)
    blend_last(0, 2)
    blend_group(1, 0, True)
    send_parts(0)
    blend_group(1, 1, False)
    blend_group(1, 3, False)
    blend_last(1, 2)
    send_parts(1)

    for half in range(2):
        for step, turns in turns_of:
            for turn in turns:
                piece_copy(half, step, turn).wait_send()

        def await_part(index, carry, half=half):
            part_copy(half, index).wait()
            return carry

        lax.fori_loop(0, OWNERS - 1, await_part, 0)

    for x in range(BX):
        for h in range(2):
            for g in range(2):
                row = 8 * g * 16 + 8 * h + x
                norm = sums[4 * x + 2 * h + g]
                d1, d2 = [
                    (parts[half, pl.ds(row, 8, stride=16), :] + parts[half, pl.ds(row + 256, 8, stride=16), :]) / norm
                    for half in range(2)
                ]
                top = jnp.maximum(jnp.maximum(d1, d2), 0.0)
                e0, e1, e2 = jnp.exp(-top), jnp.exp(d1 - top), jnp.exp(d2 - top)
                scale = 1.0 / (e0 + e1 + e2)
                rows = slice(16 * h + 8 * g, 16 * h + 8 * g + 8)
                out_ref[x, 0, rows, :] = e0 * scale
                out_ref[x, 1, rows, :] = e1 * scale
                out_ref[x, 2, rows, :] = e2 * scale


def per_device(patch_logits, patch_start, patch_owner):
    tiles = patch_logits.reshape(GROUPS, 8, LAST + 1, 128)
    probs = pl.pallas_call(
        blend_kernel,
        out_shape=jax.ShapeDtypeStruct((BX, CLASSES, BY, BZ), F32),
        in_specs=[
            pl.BlockSpec(memory_space=pl.ANY),
            pl.BlockSpec(memory_space=pl.ANY),
            pl.BlockSpec(memory_space=pl.ANY),
        ],
        out_specs=pl.BlockSpec(memory_space=pltpu.VMEM),
        scratch_shapes=[
            pltpu.SMEM((GX, GY, GZ), jnp.int32),
            pltpu.SMEM((GX, 3, GY, GZ), jnp.int32),
            pltpu.VMEM((GROUPS, LAST + 1, 8, 128), BF16),
            pltpu.VMEM((16, TILES[0], 8, 128), BF16),
            pltpu.VMEM((16, TILES[1], 8, 128), BF16),
            pltpu.VMEM((16, TILES[0], 8, 128), BF16),
            pltpu.VMEM((16, TILES[1], 8, 128), BF16),
            pltpu.VMEM((3 * PX, 8, 128), F32),
            pltpu.VMEM((32, 8, 128), F32),
            pltpu.VMEM((16, VROWS, 2, GROUPS, 8, 128), F32),
            pltpu.VMEM((4, VROWS + 1, 2, SPAN, 8, 128), F32),
            pltpu.VMEM((2, 8, 2, 64, 128), F32),
            pltpu.VMEM((2, 2, 64, 128), F32),
            pltpu.VMEM((2, 2, 64, 128), F32),
            pltpu.VMEM((2, 16 * OWNERS, 128), F32),
            pltpu.VMEM((2, 16 * OWNERS, 128), F32),
            pltpu.SemaphoreType.DMA,
            pltpu.SemaphoreType.DMA,
            pltpu.SemaphoreType.DMA,
            pltpu.SemaphoreType.DMA((2, 16)),
            pltpu.SemaphoreType.DMA((2, 16)),
            pltpu.SemaphoreType.DMA((2, 2)),
            pltpu.SemaphoreType.DMA((2, 2)),
            pltpu.SemaphoreType.DMA((2, OWNERS)),
            pltpu.SemaphoreType.DMA((2, OWNERS)),
        ],
        compiler_params=pltpu.CompilerParams(collective_id=0, has_side_effects=True, vmem_limit_bytes=62000000),
    )(patch_owner, jnp.transpose(patch_start, (0, 3, 1, 2)), jnp.transpose(tiles, (0, 2, 1, 3)))
    return jnp.transpose(probs, (0, 2, 1, 3))


def solution(mesh):
    return jax.shard_map(
        per_device,
        mesh=mesh,
        in_specs=(P("gx", "gy", "gz", None, None), P(), P()),
        out_specs=P("gx", "gy", None, "gz"),
        check_vma=False,
    )
```

```python
import jax
import jax.numpy as jnp
from jax import lax
from jax.experimental import pallas as pl
from jax.experimental.pallas import tpu as pltpu
from jax.sharding import PartitionSpec as P

CLASSES = 3
BX, BY, BZ = 8, 32, 128
PX, PY, PZ = 24, 48, 144
GX, GY, GZ = 8, 4, 8
ROW = CLASSES * PZ
RES = 16
VROWS = PY // RES
GROUPS = PX // 8
TILES = (21, 11)
LAST = PY * ROW // 128 - 1
MARGIN = 5
SPAN = 13
OWNERS = GX * GY
F32 = jnp.float32
BF16 = jnp.bfloat16
MESH = pl.DeviceIdType.MESH
ORDER = (2, 1, 3, 0)


def profile(offsets, length):
    inside = (offsets >= 0) & (offsets < length)
    centre = (length - 1) / 2.0
    spread = length / 4.0
    values = jnp.exp(-((offsets.astype(F32) - centre) ** 2) / (2.0 * spread * spread))
    return jnp.where(inside, values, 0.0)


def iota(dim):
    return lax.broadcasted_iota(jnp.int32, (8, 128), dim)


def wrap(index, size):
    return index & (size - 1)


def halved(index, times):
    return lax.shift_right_logical(index, jnp.int32(times))


def hop_of(step, to_b):
    return (0, 1, 2 - 4 * (to_b & 1), -1)[step]


def blend_kernel(
    owner_hbm, start_hbm, x_ref, out_ref,
    owner_ref, start_ref, patch, send0, send1, recv0, recv1, table, sums, kept, value, acc, rim, rims, total, parts,
    in_sem, owner_sem, start_sem, send_sem, recv_sem, rim_send, rim_recv, part_send, part_recv,
):
    a, b, k = lax.axis_index("gx"), lax.axis_index("gy"), lax.axis_index("gz")
    above, below = wrap(k + 1, GZ), wrap(k - 1, GZ)
    send, recv = (send0, send1), (recv0, recv1)
    near = [
        (wrap(a + dz, GX), wrap(b + db, GY), k) for dz in (0, 1, -1, 2, -2) for db in range(GY) if dz or db
    ] + [(a, b, above), (a, b, below)]
    barrier = pltpu.get_barrier_semaphore()
    for to in near:
        pl.semaphore_signal(barrier, inc=1, device_id=to, device_id_type=MESH)
    load = pltpu.make_async_copy(x_ref, patch, in_sem)
    load.start()
    indices = [
        pltpu.make_async_copy(owner_hbm, owner_ref, owner_sem),
        pltpu.make_async_copy(start_hbm, start_ref, start_sem),
    ]
    for copy in indices:
        copy.start()

    lane, sub = iota(1), iota(0)
    zero = jnp.zeros((8, 128), F32)

    def start_of(code, at_k, dim):
        return start_ref[halved(code, 2), dim, code & (GY - 1), at_k]

    for copy in indices:
        copy.wait()
    my_sy = start_of(owner_ref[a, b, k], k, 1)
    load.wait()

    def cut(residue, store):
        rho = (residue - my_sy) & (RES - 1)
        tails = []
        for g in range(GROUPS):
            done = []
            for half, (skip, length) in enumerate(((0, 2 * PZ), (2 * PZ, PZ))):
                tiles = {}
                for v in range(VROWS):
                    into = length * v
                    delta = ROW * rho + (ROW * RES * v + skip - into)
                    first = halved(delta + 127, 7)
                    turn = first * 128 - delta
                    low, high = into // 128, (into + length - 1) // 128
                    turned = []
                    for t in range(low - 1, high + 1):
                        at = first + t
                        if t < 0:
                            at = jnp.maximum(at, 0)
                        if half == 1 and v == VROWS - 1 and t == high:
                            at = jnp.minimum(at, LAST)
                        turned.append(pltpu.roll(patch[g, at].astype(F32), turn, 1))
                    for t in range(low, high + 1):
                        tile = jnp.where(lane < turn, turned[t - low], turned[t - low + 1])
                        tiles[t] = jnp.where(lane < into % 128, tiles[t], tile) if t in tiles else tile
                done.append(tiles)
            for t in range(7):
                store(0, GROUPS * t + g, done[0][t].astype(BF16))
            for t in range(3):
                store(1, GROUPS * t + g, done[1][t].astype(BF16))
            tails.append(done[1][3])
        store(1, 9, jnp.where(lane < 48, tails[0], pltpu.roll(tails[1], 48, 1)).astype(BF16))
        store(1, 10, tails[2].astype(BF16))

    def piece_copy(half, step, turn):
        to_b = wrap(b + turn, GY)
        return pltpu.make_async_remote_copy(
            src_ref=send[half].at[4 * step + turn],
            dst_ref=recv[half].at[4 * step + b],
            send_sem=send_sem.at[half, 4 * step + turn],
            recv_sem=recv_sem.at[half, 4 * step + b],
            device_id=(wrap(a + hop_of(step, to_b), GX), to_b, k),
            device_id_type=MESH,
        )

    def piece_arrival(half, step, from_b):
        return pltpu.make_async_remote_copy(
            src_ref=send[half].at[4 * step],
            dst_ref=recv[half].at[4 * step + from_b],
            send_sem=send_sem.at[half, 4 * step],
            recv_sem=recv_sem.at[half, 4 * step + from_b],
            device_id=(a, b, above),
            device_id_type=MESH,
        )

    turns_of = [(step, [turn for turn in ORDER if step or turn]) for step in ORDER]
    for step, turns in turns_of:

        def cut_one(turn, carry, step=step):
            residue = 4 * wrap(a + step, 4) + wrap(b + turn, GY)

            def store(half, tile, what):
                send[half][4 * step + turn, tile] = what

            cut(residue, store)
            return carry

        lax.fori_loop(GY - len(turns), GY, cut_one, 0)
        if step == 2:
            pl.semaphore_wait(barrier, len(near))
        for turn in turns:
            piece_copy(0, step, turn).start()
    for step, turns in turns_of:
        for turn in turns:
            piece_copy(1, step, turn).start()

    def store_own(half, tile, what):
        recv[half][b, tile] = what

    cut(4 * wrap(a, 4) + b, store_own)

    for s in range(4):
        for t in range(2):
            for v in range(VROWS + 1):
                for at in range(SPAN):
                    if v == VROWS or not MARGIN <= at < MARGIN + GROUPS + 1:
                        value[s, v, t, at] = zero
    for offset in range(3 * PX):
        table[offset] = profile(jnp.full((8, 128), offset - PX, jnp.int32), PX)

    def add_weight(index, carry):
        i, j, at_k = a - 2 + lax.div(index, 9), b - 1 + lax.rem(lax.div(index, 3), 3), k - 1 + lax.rem(index, 3)
        valid = (i >= 0) & (i < GX) & (j >= 0) & (j < GY) & (at_k >= 0) & (at_k < GZ)
        i, j, at_k = jnp.clip(i, 0, GX - 1), jnp.clip(j, 0, GY - 1), jnp.clip(at_k, 0, GZ - 1)
        along_z = profile(BZ * k + lane - start_ref[i, 2, j, at_k], PZ)
        along_z = along_z * jnp.where(valid, 1.0, 0.0)
        y = BY * b + sub - start_ref[i, 1, j, at_k]
        planes = [profile(y + 8 * g, PY) * along_z for g in range(4)]
        base = jnp.clip(BX * a - start_ref[i, 0, j, at_k] + PX, 0, 2 * PX)
        new = []
        for x in range(BX):
            along_x = table[base + x]
            new += [carry[4 * x + g] + along_x * planes[g] for g in range(4)]
        return tuple(new)

    weights = lax.fori_loop(0, 45, add_weight, (zero,) * 32)
    for at in range(32):
        sums[at] = weights[at]

    residue = 4 * wrap(a, 4) + b
    along_x = [profile(sub + 8 * g, PX) for g in range(GROUPS)]
    columns = (lane, jnp.where(lane < 64, lane + 128, lane - 128))

    def corner(step, from_b):
        from_a = wrap(a - hop_of(step, b), GX)
        code = owner_ref[from_a, from_b, k]
        sy = start_of(code, k, 1)
        rho = (residue - sy) & (RES - 1)
        return start_of(code, k, 0), halved(sy + rho, 4), rho, start_of(code, k, 2) - BZ * k

    def aligned(first, second, shift, lead):
        turn = (shift - lead) & 255
        low = turn & 127
        swap = (jnp.where(lane < low, 1, 0) + halved(turn, 7)) == 1
        first, second = pltpu.roll(first.astype(F32), low, 1), pltpu.roll(second.astype(F32), low, 1)
        return jnp.where(swap, second, first), jnp.where(swap, first, second)

    def weigh_group(half, step):
        def weigh(from_b, carry):
            slot = 4 * step + from_b
            if step == 0:

                @pl.when(from_b != b)
                def _():
                    piece_arrival(half, step, from_b).wait_recv()

            else:
                piece_arrival(half, step, from_b).wait_recv()
            sx, _, rho, shift = corner(step, from_b)
            turn_x = sx & 7
            along_z = [profile(c - shift, PZ) for c in columns]
            held = {}
            for v in range(VROWS):
                for g in range(GROUPS):
                    if half == 0:
                        for m in (2 * v, 2 * v + 1):
                            held[m, g] = recv0[slot, GROUPS * m + g], recv0[slot, GROUPS * m + GROUPS + g]
                    else:
                        tail = 9 + g // 2 if v == VROWS - 1 else GROUPS * v + GROUPS + g
                        held[v, g] = recv1[slot, GROUPS * v + g], recv1[slot, tail]
                        held[v, g, 0] = [kept[slot, v, t, g] for t in range(2)]
            for v in range(VROWS):
                along_y = profile(jnp.full((8, 128), RES * v, jnp.int32) + rho, PY)
                turned = [[], []]
                for g in range(GROUPS):
                    if half == 0:
                        base, upper = [aligned(*held[m, g], shift, 16 * m) for m in (2 * v, 2 * v + 1)]
                        for t in range(2):
                            kept[slot, v, t, g] = base[t]
                    else:
                        first, second = held[v, g]
                        if v == VROWS - 1 and g == 1:
                            second = pltpu.roll(second.astype(F32), 80, 1)
                        upper = aligned(first, second, shift, 16 * v)
                        base = held[v, g, 0]
                    along_xy = along_x[g] * along_y
                    for t in range(2):
                        product = (upper[t] - base[t]) * (along_xy * along_z[t])
                        turned[t].append(pltpu.roll(product, turn_x, 0))
                for t in range(2):
                    ends = [zero] + turned[t] + [zero]
                    for g in range(GROUPS + 1):
                        value[from_b, v, t, MARGIN + g] = jnp.where(sub < turn_x, ends[g], ends[g + 1])
            return carry

        lax.fori_loop(0, GY, weigh, 0)

    def place_group(half, step, lane_tiles, first):
        corners = [corner(step, from_b) for from_b in range(GY)]

        def place(y, carry):
            places = []
            for sx, first_y, _, _ in corners:
                v = y - first_y
                places.append((jnp.where((v >= 0) & (v < VROWS), v, VROWS), MARGIN - halved(sx, 3)))
            loaded = [{t: value[s, v, t, pl.ds(at, GX)] for t in lane_tiles} for s, (v, at) in enumerate(places)]
            sums_of = {}
            for t in lane_tiles:
                for block in range(GX):
                    one, two, three, four = [tiles[t][block] for tiles in loaded]
                    got = (one + two) + (three + four)
                    if not first:
                        got = got + acc[half, y, t, 8 * block : 8 * block + 8, :]
                    sums_of[t, block] = got
            for (t, block), got in sums_of.items():
                acc[half, y, t, 8 * block : 8 * block + 8, :] = got
            return carry

        lax.fori_loop(0, 8, place, 0)

    def rim_copies(half):
        return [
            pltpu.make_async_remote_copy(
                src_ref=rim.at[half, side],
                dst_ref=rims.at[half, side],
                send_sem=rim_send.at[half, side],
                recv_sem=rim_recv.at[half, side],
                device_id=(a, b, to_k),
                device_id_type=MESH,
            )
            for side, to_k in ((0, above), (1, below))
        ]

    def send_rims(half):
        for block in range(GX):
            rows = slice(8 * block, 8 * block + 8)
            up, low = zero, zero
            for y in range(8):
                turned = acc[half, y, 1, rows, :]
                turned = pltpu.roll(turned, 16 * y, 1) if y else turned
                up = jnp.where(lane // 16 == y, turned, up)
                low = jnp.where(lane // 16 == (y + 7) % 8, turned, low)
            rim[half, 0, rows, :] = up
            rim[half, 1, rows, :] = low
        for copy in rim_copies(half):
            copy.start()

    def block_of(far):
        return wrap(a + 4 + halved(far + 1, 1) * (1 - 2 * (far & 1)), GX)

    def part_copy(half, far, turn):
        to_a, to_b = block_of(far), wrap(b + ORDER[turn], GY)
        return pltpu.make_async_remote_copy(
            src_ref=total.at[half, pl.ds(pl.multiple_of(16 * (GY * to_a + to_b), 16), 16)],
            dst_ref=parts.at[half, pl.ds(pl.multiple_of(16 * (GY * a + b), 16), 16)],
            send_sem=part_send.at[half, GY * far + turn],
            recv_sem=part_recv.at[half, GY * far + turn],
            device_id=(to_a, to_b, k),
            device_id_type=MESH,
        )

    def finish_block(half, block):
        rows = pl.ds(pl.multiple_of(8 * block, 8), 8)
        up, low = rims[half, 0, rows, :], rims[half, 1, rows, :]
        cells = []
        for y in range(8):
            back = (128 - 16 * y) % 128
            ends = (pltpu.roll(up, back, 1), pltpu.roll(low, back, 1)) if y else (up, low)
            more = jnp.where(lane < 16, ends[0], jnp.where(lane >= 112, ends[1], 0.0))
            cells.append(acc[half, y, 0, rows, :] + more)
        for y, what in enumerate(cells):
            total[half, pl.ds(pl.multiple_of(64 * block + 8 * y, 8), 8), :] = what

    def send_parts(half):
        for copy in rim_copies(half):
            copy.wait()

        def send_block(far, carry):
            finish_block(half, block_of(far))

            @pl.when(far > 0)
            def _():
                for turn in range(GY):
                    part_copy(half, far - 1, turn).start()

            return carry

        lax.fori_loop(0, GX, send_block, 0)
        for turn in range(GY - 1):
            part_copy(half, jnp.int32(GX - 1), turn).start()
        mine = pl.ds(pl.multiple_of(16 * (GY * a + b), 16), 16)
        parts[half, mine, :] = total[half, mine, :]

    def blend_group(half, step, first):
        weigh_group(half, step)
        place_group(half, step, (0, 1), first)

    def blend_last(half, step):
        weigh_group(half, step)
        place_group(half, step, (1,), False)
        send_rims(half)
        place_group(half, step, (0,), False)

    blend_group(0, 0, True)
    blend_group(0, 1, False)
    blend_group(0, 3, False)
    blend_last(0, 2)
    blend_group(1, 0, True)
    send_parts(0)
    blend_group(1, 1, False)
    blend_group(1, 3, False)
    blend_last(1, 2)
    send_parts(1)

    for half in range(2):
        for step, turns in turns_of:
            for turn in turns:
                piece_copy(half, step, turn).wait_send()

        def await_parts(far, carry, half=half):
            for turn in range(GY - 1):
                part_copy(half, far, turn).wait()

            @pl.when(far < GX - 1)
            def _():
                part_copy(half, far, GY - 1).wait()

            return carry

        lax.fori_loop(0, GX, await_parts, 0)

    for x in range(BX):
        for h in range(2):
            for g in range(2):
                row = 8 * g * 16 + 8 * h + x
                norm = sums[4 * x + 2 * h + g]
                d1, d2 = [
                    (parts[half, pl.ds(row, 8, stride=16), :] + parts[half, pl.ds(row + 256, 8, stride=16), :]) / norm
                    for half in range(2)
                ]
                top = jnp.maximum(jnp.maximum(d1, d2), 0.0)
                e0, e1, e2 = jnp.exp(-top), jnp.exp(d1 - top), jnp.exp(d2 - top)
                scale = 1.0 / (e0 + e1 + e2)
                rows = slice(16 * h + 8 * g, 16 * h + 8 * g + 8)
                out_ref[x, 0, rows, :] = e0 * scale
                out_ref[x, 1, rows, :] = e1 * scale
                out_ref[x, 2, rows, :] = e2 * scale


def per_device(patch_logits, patch_start, patch_owner):
    tiles = patch_logits.reshape(GROUPS, 8, LAST + 1, 128)
    probs = pl.pallas_call(
        blend_kernel,
        out_shape=jax.ShapeDtypeStruct((BX, CLASSES, BY, BZ), F32),
        in_specs=[
            pl.BlockSpec(memory_space=pl.ANY),
            pl.BlockSpec(memory_space=pl.ANY),
            pl.BlockSpec(memory_space=pl.ANY),
        ],
        out_specs=pl.BlockSpec(memory_space=pltpu.VMEM),
        scratch_shapes=[
            pltpu.SMEM((GX, GY, GZ), jnp.int32),
            pltpu.SMEM((GX, 3, GY, GZ), jnp.int32),
            pltpu.VMEM((GROUPS, LAST + 1, 8, 128), BF16),
            pltpu.VMEM((16, TILES[0], 8, 128), BF16),
            pltpu.VMEM((16, TILES[1], 8, 128), BF16),
            pltpu.VMEM((16, TILES[0], 8, 128), BF16),
            pltpu.VMEM((16, TILES[1], 8, 128), BF16),
            pltpu.VMEM((3 * PX, 8, 128), F32),
            pltpu.VMEM((32, 8, 128), F32),
            pltpu.VMEM((16, VROWS, 2, GROUPS, 8, 128), F32),
            pltpu.VMEM((4, VROWS + 1, 2, SPAN, 8, 128), F32),
            pltpu.VMEM((2, 8, 2, 64, 128), F32),
            pltpu.VMEM((2, 2, 64, 128), F32),
            pltpu.VMEM((2, 2, 64, 128), F32),
            pltpu.VMEM((2, 16 * OWNERS, 128), F32),
            pltpu.VMEM((2, 16 * OWNERS, 128), F32),
            pltpu.SemaphoreType.DMA,
            pltpu.SemaphoreType.DMA,
            pltpu.SemaphoreType.DMA,
            pltpu.SemaphoreType.DMA((2, 16)),
            pltpu.SemaphoreType.DMA((2, 16)),
            pltpu.SemaphoreType.DMA((2, 2)),
            pltpu.SemaphoreType.DMA((2, 2)),
            pltpu.SemaphoreType.DMA((2, OWNERS)),
            pltpu.SemaphoreType.DMA((2, OWNERS)),
        ],
        compiler_params=pltpu.CompilerParams(collective_id=0, has_side_effects=True, vmem_limit_bytes=62000000),
    )(patch_owner, jnp.transpose(patch_start, (0, 3, 1, 2)), jnp.transpose(tiles, (0, 2, 1, 3)))
    return jnp.transpose(probs, (0, 2, 1, 3))


def solution(mesh):
    return jax.shard_map(
        per_device,
        mesh=mesh,
        in_specs=(P("gx", "gy", "gz", None, None), P(), P()),
        out_specs=P("gx", "gy", None, "gz"),
        check_vma=False,
    )
```

```python
import jax
import jax.numpy as jnp
from jax import lax
from jax.experimental import pallas as pl
from jax.experimental.pallas import tpu as pltpu
from jax.sharding import PartitionSpec as P

CLASSES = 3
BX, BY, BZ = 8, 32, 128
PX, PY, PZ = 24, 48, 144
GX, GY, GZ = 8, 4, 8
ROW = CLASSES * PZ
RES = 16
VROWS = PY // RES
GROUPS = PX // 8
TILES = (21, 11)
LAST = PY * ROW // 128 - 1
MARGIN = 5
SPAN = 13
OWNERS = GX * GY
F32 = jnp.float32
BF16 = jnp.bfloat16
MESH = pl.DeviceIdType.MESH
ORDER = (2, 1, 3, 0)


def profile(offsets, length):
    inside = (offsets >= 0) & (offsets < length)
    centre = (length - 1) / 2.0
    spread = length / 4.0
    values = jnp.exp(-((offsets.astype(F32) - centre) ** 2) / (2.0 * spread * spread))
    return jnp.where(inside, values, 0.0)


def iota(dim):
    return lax.broadcasted_iota(jnp.int32, (8, 128), dim)


def wrap(index, size):
    return index & (size - 1)


def halved(index, times):
    return lax.shift_right_logical(index, jnp.int32(times))


def hop_of(step, to_b):
    return (0, 1, 2 - 4 * (to_b & 1), -1)[step]


def blend_kernel(
    owner_hbm, start_hbm, x_ref, out_ref,
    owner_ref, start_ref, patch, send0, send1, recv0, recv1, table, sums, kept, value, acc, rim, rims, total, parts,
    in_sem, owner_sem, start_sem, send_sem, recv_sem, rim_send, rim_recv, part_send, part_recv,
):
    a, b, k = lax.axis_index("gx"), lax.axis_index("gy"), lax.axis_index("gz")
    above, below = wrap(k + 1, GZ), wrap(k - 1, GZ)
    send, recv = (send0, send1), (recv0, recv1)
    near = [
        (wrap(a + dz, GX), wrap(b + db, GY), k) for dz in (0, 1, -1, 2, -2) for db in range(GY) if dz or db
    ] + [(a, b, above), (a, b, below)]
    barrier = pltpu.get_barrier_semaphore()
    for to in near:
        pl.semaphore_signal(barrier, inc=1, device_id=to, device_id_type=MESH)
    load = pltpu.make_async_copy(x_ref, patch, in_sem)
    load.start()
    indices = [
        pltpu.make_async_copy(owner_hbm, owner_ref, owner_sem),
        pltpu.make_async_copy(start_hbm, start_ref, start_sem),
    ]
    for copy in indices:
        copy.start()

    lane, sub = iota(1), iota(0)
    zero = jnp.zeros((8, 128), F32)

    def start_of(code, at_k, dim):
        return start_ref[halved(code, 2), dim, code & (GY - 1), at_k]

    for copy in indices:
        copy.wait()
    my_sy = start_of(owner_ref[a, b, k], k, 1)
    load.wait()

    def cut(residue, store):
        rho = (residue - my_sy) & (RES - 1)
        tails = []
        for g in range(GROUPS):
            done = []
            for half, (skip, length) in enumerate(((0, 2 * PZ), (2 * PZ, PZ))):
                tiles = {}
                for v in range(VROWS):
                    into = length * v
                    delta = ROW * rho + (ROW * RES * v + skip - into)
                    first = halved(delta + 127, 7)
                    turn = first * 128 - delta
                    low, high = into // 128, (into + length - 1) // 128
                    turned = []
                    for t in range(low - 1, high + 1):
                        at = first + t
                        if t < 0:
                            at = jnp.maximum(at, 0)
                        if half == 1 and v == VROWS - 1 and t == high:
                            at = jnp.minimum(at, LAST)
                        turned.append(pltpu.roll(patch[g, at].astype(F32), turn, 1))
                    for t in range(low, high + 1):
                        tile = jnp.where(lane < turn, turned[t - low], turned[t - low + 1])
                        tiles[t] = jnp.where(lane < into % 128, tiles[t], tile) if t in tiles else tile
                done.append(tiles)
            for t in range(7):
                store(0, GROUPS * t + g, done[0][t].astype(BF16))
            for t in range(3):
                store(1, GROUPS * t + g, done[1][t].astype(BF16))
            tails.append(done[1][3])
        store(1, 9, jnp.where(lane < 48, tails[0], pltpu.roll(tails[1], 48, 1)).astype(BF16))
        store(1, 10, tails[2].astype(BF16))

    def piece_copy(half, step, turn):
        to_b = wrap(b + turn, GY)
        return pltpu.make_async_remote_copy(
            src_ref=send[half].at[4 * step + turn],
            dst_ref=recv[half].at[4 * step + b],
            send_sem=send_sem.at[half, 4 * step + turn],
            recv_sem=recv_sem.at[half, 4 * step + b],
            device_id=(wrap(a + hop_of(step, to_b), GX), to_b, k),
            device_id_type=MESH,
        )

    def piece_arrival(half, step, from_b):
        return pltpu.make_async_remote_copy(
            src_ref=send[half].at[4 * step],
            dst_ref=recv[half].at[4 * step + from_b],
            send_sem=send_sem.at[half, 4 * step],
            recv_sem=recv_sem.at[half, 4 * step + from_b],
            device_id=(a, b, above),
            device_id_type=MESH,
        )

    turns_of = [(step, [turn for turn in ORDER if step or turn]) for step in ORDER]
    for step, turns in turns_of:

        def cut_one(turn, carry, step=step):
            residue = 4 * wrap(a + step, 4) + wrap(b + turn, GY)

            def store(half, tile, what):
                send[half][4 * step + turn, tile] = what

            cut(residue, store)
            return carry

        lax.fori_loop(GY - len(turns), GY, cut_one, 0)
        if step == 2:
            pl.semaphore_wait(barrier, len(near))
        for turn in turns:
            piece_copy(0, step, turn).start()
    def store_own(half, tile, what):
        recv[half][b, tile] = what

    cut(4 * wrap(a, 4) + b, store_own)

    for s in range(4):
        for t in range(2):
            for v in range(VROWS + 1):
                for at in range(SPAN):
                    if v == VROWS or not MARGIN <= at < MARGIN + GROUPS + 1:
                        value[s, v, t, at] = zero
    for offset in range(3 * PX):
        table[offset] = profile(jnp.full((8, 128), offset - PX, jnp.int32), PX)

    def add_weight(index, carry):
        i, j, at_k = a - 2 + lax.div(index, 9), b - 1 + lax.rem(lax.div(index, 3), 3), k - 1 + lax.rem(index, 3)
        valid = (i >= 0) & (i < GX) & (j >= 0) & (j < GY) & (at_k >= 0) & (at_k < GZ)
        i, j, at_k = jnp.clip(i, 0, GX - 1), jnp.clip(j, 0, GY - 1), jnp.clip(at_k, 0, GZ - 1)
        along_z = profile(BZ * k + lane - start_ref[i, 2, j, at_k], PZ)
        along_z = along_z * jnp.where(valid, 1.0, 0.0)
        y = BY * b + sub - start_ref[i, 1, j, at_k]
        planes = [profile(y + 8 * g, PY) * along_z for g in range(4)]
        base = jnp.clip(BX * a - start_ref[i, 0, j, at_k] + PX, 0, 2 * PX)
        new = []
        for x in range(BX):
            along_x = table[base + x]
            new += [carry[4 * x + g] + along_x * planes[g] for g in range(4)]
        return tuple(new)

    weights = lax.fori_loop(0, 45, add_weight, (zero,) * 32)
    for at in range(32):
        sums[at] = weights[at]

    residue = 4 * wrap(a, 4) + b
    along_x = [profile(sub + 8 * g, PX) for g in range(GROUPS)]
    columns = (lane, jnp.where(lane < 64, lane + 128, lane - 128))

    def corner(step, from_b):
        from_a = wrap(a - hop_of(step, b), GX)
        code = owner_ref[from_a, from_b, k]
        sy = start_of(code, k, 1)
        rho = (residue - sy) & (RES - 1)
        return start_of(code, k, 0), halved(sy + rho, 4), rho, start_of(code, k, 2) - BZ * k

    def aligned(first, second, shift, lead):
        turn = (shift - lead) & 255
        low = turn & 127
        swap = (jnp.where(lane < low, 1, 0) + halved(turn, 7)) == 1
        first, second = pltpu.roll(first.astype(F32), low, 1), pltpu.roll(second.astype(F32), low, 1)
        return jnp.where(swap, second, first), jnp.where(swap, first, second)

    def weigh_group(half, step):
        def weigh(from_b, carry):
            slot = 4 * step + from_b
            if step == 0:

                @pl.when(from_b != b)
                def _():
                    piece_arrival(half, step, from_b).wait_recv()

            else:
                piece_arrival(half, step, from_b).wait_recv()
            sx, _, rho, shift = corner(step, from_b)
            turn_x = sx & 7
            along_z = [profile(c - shift, PZ) for c in columns]
            held = {}
            for v in range(VROWS):
                for g in range(GROUPS):
                    if half == 0:
                        for m in (2 * v, 2 * v + 1):
                            held[m, g] = recv0[slot, GROUPS * m + g], recv0[slot, GROUPS * m + GROUPS + g]
                    else:
                        tail = 9 + g // 2 if v == VROWS - 1 else GROUPS * v + GROUPS + g
                        held[v, g] = recv1[slot, GROUPS * v + g], recv1[slot, tail]
                        held[v, g, 0] = [kept[slot, v, t, g] for t in range(2)]
            for v in range(VROWS):
                along_y = profile(jnp.full((8, 128), RES * v, jnp.int32) + rho, PY)
                turned = [[], []]
                for g in range(GROUPS):
                    if half == 0:
                        base, upper = [aligned(*held[m, g], shift, 16 * m) for m in (2 * v, 2 * v + 1)]
                        for t in range(2):
                            kept[slot, v, t, g] = base[t]
                    else:
                        first, second = held[v, g]
                        if v == VROWS - 1 and g == 1:
                            second = pltpu.roll(second.astype(F32), 80, 1)
                        upper = aligned(first, second, shift, 16 * v)
                        base = held[v, g, 0]
                    along_xy = along_x[g] * along_y
                    for t in range(2):
                        product = (upper[t] - base[t]) * (along_xy * along_z[t])
                        turned[t].append(pltpu.roll(product, turn_x, 0))
                for t in range(2):
                    ends = [zero] + turned[t] + [zero]
                    for g in range(GROUPS + 1):
                        value[from_b, v, t, MARGIN + g] = jnp.where(sub < turn_x, ends[g], ends[g + 1])
            return carry

        lax.fori_loop(0, GY, weigh, 0)

    def place_group(half, step, lane_tiles, first):
        corners = [corner(step, from_b) for from_b in range(GY)]

        def place(y, carry):
            places = []
            for sx, first_y, _, _ in corners:
                v = y - first_y
                places.append((jnp.where((v >= 0) & (v < VROWS), v, VROWS), MARGIN - halved(sx, 3)))
            loaded = [{t: value[s, v, t, pl.ds(at, GX)] for t in lane_tiles} for s, (v, at) in enumerate(places)]
            sums_of = {}
            for t in lane_tiles:
                for block in range(GX):
                    one, two, three, four = [tiles[t][block] for tiles in loaded]
                    got = (one + two) + (three + four)
                    if not first:
                        got = got + acc[half, y, t, 8 * block : 8 * block + 8, :]
                    sums_of[t, block] = got
            for (t, block), got in sums_of.items():
                acc[half, y, t, 8 * block : 8 * block + 8, :] = got
            return carry

        lax.fori_loop(0, 8, place, 0)

    def rim_copies(half):
        return [
            pltpu.make_async_remote_copy(
                src_ref=rim.at[half, side],
                dst_ref=rims.at[half, side],
                send_sem=rim_send.at[half, side],
                recv_sem=rim_recv.at[half, side],
                device_id=(a, b, to_k),
                device_id_type=MESH,
            )
            for side, to_k in ((0, above), (1, below))
        ]

    def send_rims(half):
        for block in range(GX):
            rows = slice(8 * block, 8 * block + 8)
            up, low = zero, zero
            for y in range(8):
                turned = acc[half, y, 1, rows, :]
                turned = pltpu.roll(turned, 16 * y, 1) if y else turned
                up = jnp.where(lane // 16 == y, turned, up)
                low = jnp.where(lane // 16 == (y + 7) % 8, turned, low)
            rim[half, 0, rows, :] = up
            rim[half, 1, rows, :] = low
        for copy in rim_copies(half):
            copy.start()

    def block_of(far):
        return wrap(a + 4 + halved(far + 1, 1) * (1 - 2 * (far & 1)), GX)

    def part_copy(half, far, turn):
        to_a, to_b = block_of(far), wrap(b + ORDER[turn], GY)
        return pltpu.make_async_remote_copy(
            src_ref=total.at[half, pl.ds(pl.multiple_of(16 * (GY * to_a + to_b), 16), 16)],
            dst_ref=parts.at[half, pl.ds(pl.multiple_of(16 * (GY * a + b), 16), 16)],
            send_sem=part_send.at[half, GY * far + turn],
            recv_sem=part_recv.at[half, GY * far + turn],
            device_id=(to_a, to_b, k),
            device_id_type=MESH,
        )

    def finish_block(half, block):
        rows = pl.ds(pl.multiple_of(8 * block, 8), 8)
        up, low = rims[half, 0, rows, :], rims[half, 1, rows, :]
        cells = []
        for y in range(8):
            back = (128 - 16 * y) % 128
            ends = (pltpu.roll(up, back, 1), pltpu.roll(low, back, 1)) if y else (up, low)
            more = jnp.where(lane < 16, ends[0], jnp.where(lane >= 112, ends[1], 0.0))
            cells.append(acc[half, y, 0, rows, :] + more)
        for y, what in enumerate(cells):
            total[half, pl.ds(pl.multiple_of(64 * block + 8 * y, 8), 8), :] = what

    def send_parts(half):
        for copy in rim_copies(half):
            copy.wait()

        def send_block(far, carry):
            finish_block(half, block_of(far))

            @pl.when(far > 0)
            def _():
                for turn in range(GY):
                    part_copy(half, far - 1, turn).start()

            return carry

        lax.fori_loop(0, GX, send_block, 0)
        for turn in range(GY - 1):
            part_copy(half, jnp.int32(GX - 1), turn).start()
        mine = pl.ds(pl.multiple_of(16 * (GY * a + b), 16), 16)
        parts[half, mine, :] = total[half, mine, :]

    def blend_group(half, step, first):
        weigh_group(half, step)
        place_group(half, step, (0, 1), first)

    def blend_last(half, step):
        weigh_group(half, step)
        place_group(half, step, (1,), False)
        send_rims(half)
        place_group(half, step, (0,), False)

    def send_rest(*steps):
        for step, turns in turns_of:
            for turn in turns if step in steps else ():
                piece_copy(0, step, turn).wait_send()
                piece_copy(1, step, turn).start()

    blend_group(0, 2, True)
    send_rest(2)
    blend_group(0, 1, False)
    send_rest(1)
    blend_group(0, 3, False)
    send_rest(3, 0)
    blend_last(0, 0)
    blend_group(1, 2, True)
    send_parts(0)
    blend_group(1, 1, False)
    blend_group(1, 3, False)
    blend_last(1, 0)
    send_parts(1)

    for step, turns in turns_of:
        for turn in turns:
            piece_copy(1, step, turn).wait_send()
    for half in range(2):

        def await_parts(far, carry, half=half):
            for turn in range(GY - 1):
                part_copy(half, far, turn).wait()

            @pl.when(far < GX - 1)
            def _():
                part_copy(half, far, GY - 1).wait()

            return carry

        lax.fori_loop(0, GX, await_parts, 0)

    for x in range(BX):
        for h in range(2):
            for g in range(2):
                row = 8 * g * 16 + 8 * h + x
                norm = sums[4 * x + 2 * h + g]
                d1, d2 = [
                    (parts[half, pl.ds(row, 8, stride=16), :] + parts[half, pl.ds(row + 256, 8, stride=16), :]) / norm
                    for half in range(2)
                ]
                top = jnp.maximum(jnp.maximum(d1, d2), 0.0)
                e0, e1, e2 = jnp.exp(-top), jnp.exp(d1 - top), jnp.exp(d2 - top)
                scale = 1.0 / (e0 + e1 + e2)
                rows = slice(16 * h + 8 * g, 16 * h + 8 * g + 8)
                out_ref[x, 0, rows, :] = e0 * scale
                out_ref[x, 1, rows, :] = e1 * scale
                out_ref[x, 2, rows, :] = e2 * scale


def per_device(patch_logits, patch_start, patch_owner):
    tiles = patch_logits.reshape(GROUPS, 8, LAST + 1, 128)
    probs = pl.pallas_call(
        blend_kernel,
        out_shape=jax.ShapeDtypeStruct((BX, CLASSES, BY, BZ), F32),
        in_specs=[
            pl.BlockSpec(memory_space=pl.ANY),
            pl.BlockSpec(memory_space=pl.ANY),
            pl.BlockSpec(memory_space=pl.ANY),
        ],
        out_specs=pl.BlockSpec(memory_space=pltpu.VMEM),
        scratch_shapes=[
            pltpu.SMEM((GX, GY, GZ), jnp.int32),
            pltpu.SMEM((GX, 3, GY, GZ), jnp.int32),
            pltpu.VMEM((GROUPS, LAST + 1, 8, 128), BF16),
            pltpu.VMEM((16, TILES[0], 8, 128), BF16),
            pltpu.VMEM((16, TILES[1], 8, 128), BF16),
            pltpu.VMEM((16, TILES[0], 8, 128), BF16),
            pltpu.VMEM((16, TILES[1], 8, 128), BF16),
            pltpu.VMEM((3 * PX, 8, 128), F32),
            pltpu.VMEM((32, 8, 128), F32),
            pltpu.VMEM((16, VROWS, 2, GROUPS, 8, 128), F32),
            pltpu.VMEM((4, VROWS + 1, 2, SPAN, 8, 128), F32),
            pltpu.VMEM((2, 8, 2, 64, 128), F32),
            pltpu.VMEM((2, 2, 64, 128), F32),
            pltpu.VMEM((2, 2, 64, 128), F32),
            pltpu.VMEM((2, 16 * OWNERS, 128), F32),
            pltpu.VMEM((2, 16 * OWNERS, 128), F32),
            pltpu.SemaphoreType.DMA,
            pltpu.SemaphoreType.DMA,
            pltpu.SemaphoreType.DMA,
            pltpu.SemaphoreType.DMA((2, 16)),
            pltpu.SemaphoreType.DMA((2, 16)),
            pltpu.SemaphoreType.DMA((2, 2)),
            pltpu.SemaphoreType.DMA((2, 2)),
            pltpu.SemaphoreType.DMA((2, OWNERS)),
            pltpu.SemaphoreType.DMA((2, OWNERS)),
        ],
        compiler_params=pltpu.CompilerParams(collective_id=0, has_side_effects=True, vmem_limit_bytes=62000000),
    )(patch_owner, jnp.transpose(patch_start, (0, 3, 1, 2)), jnp.transpose(tiles, (0, 2, 1, 3)))
    return jnp.transpose(probs, (0, 2, 1, 3))


def solution(mesh):
    return jax.shard_map(
        per_device,
        mesh=mesh,
        in_specs=(P("gx", "gy", "gz", None, None), P(), P()),
        out_specs=P("gx", "gy", None, "gz"),
        check_vma=False,
    )
```

```python
import jax
import jax.numpy as jnp
from jax import lax
from jax.experimental import pallas as pl
from jax.experimental.pallas import tpu as pltpu
from jax.sharding import PartitionSpec as P

CLASSES = 3
BX, BY, BZ = 8, 32, 128
PX, PY, PZ = 24, 48, 144
GX, GY, GZ = 8, 4, 8
ROW = CLASSES * PZ
RES = 16
VROWS = PY // RES
SLOTS = 16
GROUPS = PX // 8
TILES = (21, 11)
LAST = PY * ROW // 128 - 1
MARGIN = 5
SPAN = 13
OWNERS = GX * GY
F32 = jnp.float32
BF16 = jnp.bfloat16
MESH = pl.DeviceIdType.MESH
ORDER = (2, 1, 3, 0)


def profile(offsets, length):
    inside = (offsets >= 0) & (offsets < length)
    centre = (length - 1) / 2.0
    spread = length / 4.0
    values = jnp.exp(-((offsets.astype(F32) - centre) ** 2) / (2.0 * spread * spread))
    return jnp.where(inside, values, 0.0)


def iota(dim):
    return lax.broadcasted_iota(jnp.int32, (8, 128), dim)


def wrap(index, size):
    return index & (size - 1)


def halved(index, times):
    return lax.shift_right_logical(index, jnp.int32(times))


def hop_of(step, to_b):
    return (0, 1, 2 - 4 * (to_b & 1), -1)[step]


def blend_kernel(
    owner_hbm, start_hbm, x_ref, out_ref,
    owner_ref, start_ref, patch, send0, send1, recv0, recv1, table, sums, kept, value, acc, rim, rims, total, parts,
    in_sem, owner_sem, start_sem, send_sem, recv_sem, rim_send, rim_recv, part_send, part_recv,
):
    a, b, k = lax.axis_index("gx"), lax.axis_index("gy"), lax.axis_index("gz")
    above, below = wrap(k + 1, GZ), wrap(k - 1, GZ)
    send, recv = (send0, send1), (recv0, recv1)
    near = [
        (wrap(a + dz, GX), wrap(b + db, GY), k) for dz in (0, 1, -1, 2, -2) for db in range(GY) if dz or db
    ] + [(a, b, above), (a, b, below)]
    barrier = pltpu.get_barrier_semaphore()
    for to in near:
        pl.semaphore_signal(barrier, inc=1, device_id=to, device_id_type=MESH)
    load = pltpu.make_async_copy(x_ref, patch, in_sem)
    load.start()
    indices = [
        pltpu.make_async_copy(owner_hbm, owner_ref, owner_sem),
        pltpu.make_async_copy(start_hbm, start_ref, start_sem),
    ]
    for copy in indices:
        copy.start()

    lane, sub = iota(1), iota(0)
    zero = jnp.zeros((8, 128), F32)

    def start_of(code, at_k, dim):
        return start_ref[halved(code, 2), dim, code & (GY - 1), at_k]

    for copy in indices:
        copy.wait()
    my_sy = start_of(owner_ref[a, b, k], k, 1)
    load.wait()

    def cut(half, residue, store):
        rho = (residue - my_sy) & (RES - 1)
        skip, length = ((0, 2 * PZ), (2 * PZ, PZ))[half]
        tails = []
        for g in range(GROUPS):
            tiles = {}
            for v in range(VROWS):
                into = length * v
                delta = ROW * rho + (ROW * RES * v + skip - into)
                first = halved(delta + 127, 7)
                turn = first * 128 - delta
                low, high = into // 128, (into + length - 1) // 128
                turned = []
                for t in range(low - 1, high + 1):
                    at = first + t
                    if t < 0:
                        at = jnp.maximum(at, 0)
                    if half == 1 and v == VROWS - 1 and t == high:
                        at = jnp.minimum(at, LAST)
                    turned.append(pltpu.roll(patch[g, at].astype(F32), turn, 1))
                for t in range(low, high + 1):
                    tile = jnp.where(lane < turn, turned[t - low], turned[t - low + 1])
                    tiles[t] = jnp.where(lane < into % 128, tiles[t], tile) if t in tiles else tile
            for t in range(7 if half == 0 else 3):
                store(GROUPS * t + g, tiles[t].astype(BF16))
            if half == 1:
                tails.append(tiles[3])
        if half == 1:
            store(9, jnp.where(lane < 48, tails[0], pltpu.roll(tails[1], 48, 1)).astype(BF16))
            store(10, tails[2].astype(BF16))

    def piece_copy(half, step, turn):
        to_b = wrap(b + turn, GY)
        return pltpu.make_async_remote_copy(
            src_ref=send[half].at[4 * step + turn],
            dst_ref=recv[half].at[4 * step + b],
            send_sem=send_sem.at[half, 4 * step + turn],
            recv_sem=recv_sem.at[half, 4 * step + b],
            device_id=(wrap(a + hop_of(step, to_b), GX), to_b, k),
            device_id_type=MESH,
        )

    def piece_arrival(half, step, from_b):
        return pltpu.make_async_remote_copy(
            src_ref=send[half].at[4 * step],
            dst_ref=recv[half].at[4 * step + from_b],
            send_sem=send_sem.at[half, 4 * step],
            recv_sem=recv_sem.at[half, 4 * step + from_b],
            device_id=(a, b, above),
            device_id_type=MESH,
        )

    turns_of = [(step, [turn for turn in ORDER if step or turn]) for step in ORDER]
    def cut_step(half, step):
        def cut_one(turn, carry):
            def store(tile, what):
                send[half][4 * step + turn, tile] = what

            cut(half, 4 * wrap(a + step, 4) + wrap(b + turn, GY), store)
            return carry

        lax.fori_loop(0 if step else 1, GY, cut_one, 0)

    def cut_own(half):
        def store(tile, what):
            recv[half][b, tile] = what

        cut(half, 4 * wrap(a, 4) + b, store)

    for step, turns in turns_of:
        cut_step(0, step)
        if step == 2:
            pl.semaphore_wait(barrier, len(near))
        for turn in turns:
            piece_copy(0, step, turn).start()
    cut_own(0)
    for step, _ in turns_of:
        cut_step(1, step)
    cut_own(1)

    for t in range(2):
        for at in range(SPAN):
            value[SLOTS * VROWS, t, at] = zero

    def clear(at, carry):
        for t in range(2):
            for margin in (*range(MARGIN), *range(MARGIN + GROUPS + 1, SPAN)):
                value[at, t, margin] = zero
        return carry

    lax.fori_loop(0, SLOTS * VROWS, clear, 0)

    residue = 4 * wrap(a, 4) + b
    along_x = [profile(sub + 8 * g, PX) for g in range(GROUPS)]
    columns = (lane, jnp.where(lane < 64, lane + 128, lane - 128))

    def corner(step, from_b):
        from_a = wrap(a - hop_of(step, b), GX)
        code = owner_ref[from_a, from_b, k]
        sy = start_of(code, k, 1)
        rho = (residue - sy) & (RES - 1)
        return start_of(code, k, 0), halved(sy + rho, 4), rho, start_of(code, k, 2) - BZ * k

    def aligned(first, second, shift, lead):
        turn = (shift - lead) & 255
        low = turn & 127
        swap = (jnp.where(lane < low, 1, 0) + halved(turn, 7)) == 1
        first, second = pltpu.roll(first.astype(F32), low, 1), pltpu.roll(second.astype(F32), low, 1)
        return jnp.where(swap, second, first), jnp.where(swap, first, second)

    def weigh_group(half, step):
        def weigh(from_b, carry):
            slot = 4 * step + from_b
            if step == 0:

                @pl.when(from_b != b)
                def _():
                    piece_arrival(half, step, from_b).wait_recv()

            else:
                piece_arrival(half, step, from_b).wait_recv()
            sx, _, rho, shift = corner(step, from_b)
            turn_x = sx & 7
            along_z = [profile(c - shift, PZ) for c in columns]
            held = {}
            for v in range(VROWS):
                for g in range(GROUPS):
                    if half == 0:
                        for m in (2 * v, 2 * v + 1):
                            held[m, g] = recv0[slot, GROUPS * m + g], recv0[slot, GROUPS * m + GROUPS + g]
                    else:
                        tail = 9 + g // 2 if v == VROWS - 1 else GROUPS * v + GROUPS + g
                        held[v, g] = recv1[slot, GROUPS * v + g], recv1[slot, tail]
                        held[v, g, 0] = [kept[slot, v, t, g] for t in range(2)]
            for v in range(VROWS):
                along_y = profile(jnp.full((8, 128), RES * v, jnp.int32) + rho, PY)
                turned = [[], []]
                for g in range(GROUPS):
                    if half == 0:
                        base, upper = [aligned(*held[m, g], shift, 16 * m) for m in (2 * v, 2 * v + 1)]
                        for t in range(2):
                            kept[slot, v, t, g] = base[t]
                    else:
                        first, second = held[v, g]
                        if v == VROWS - 1 and g == 1:
                            second = pltpu.roll(second.astype(F32), 80, 1)
                        upper = aligned(first, second, shift, 16 * v)
                        base = held[v, g, 0]
                    along_xy = along_x[g] * along_y
                    for t in range(2):
                        product = (upper[t] - base[t]) * (along_xy * along_z[t])
                        turned[t].append(pltpu.roll(product, turn_x, 0))
                for t in range(2):
                    ends = [zero] + turned[t] + [zero]
                    for g in range(GROUPS + 1):
                        value[VROWS * slot + v, t, MARGIN + g] = jnp.where(sub < turn_x, ends[g], ends[g + 1])
            return carry

        lax.fori_loop(0, GY, weigh, 0)

    def place_all(half, t):
        corners = [(4 * step + from_b, corner(step, from_b)) for step in range(4) for from_b in range(GY)]
        bases = [(VROWS * slot - first_y, first_y, MARGIN - halved(sx, 3)) for slot, (sx, first_y, _, _) in corners]

        def place(y, carry):
            places = []
            for base, first_y, at in bases:
                valid = (y >= first_y) & (y < first_y + VROWS)
                places.append((jnp.where(valid, base + y, SLOTS * VROWS), at))
            got = [value[v, t, pl.ds(at, GX)] for v, at in places]
            while len(got) > 1:
                got = [one + two for one, two in zip(got[::2], got[1::2])]
            acc[half, y, t] = got[0]
            return carry

        lax.fori_loop(0, 8, place, 0)

    def rim_copies(half):
        return [
            pltpu.make_async_remote_copy(
                src_ref=rim.at[half, side],
                dst_ref=rims.at[half, side],
                send_sem=rim_send.at[half, side],
                recv_sem=rim_recv.at[half, side],
                device_id=(a, b, to_k),
                device_id_type=MESH,
            )
            for side, to_k in ((0, above), (1, below))
        ]

    def send_rims(half):
        for block in range(GX):
            rows = slice(8 * block, 8 * block + 8)
            up, low = zero, zero
            for y in range(8):
                turned = acc[half, y, 1, block]
                turned = pltpu.roll(turned, 16 * y, 1) if y else turned
                up = jnp.where(lane // 16 == y, turned, up)
                low = jnp.where(lane // 16 == (y + 7) % 8, turned, low)
            rim[half, 0, rows, :] = up
            rim[half, 1, rows, :] = low
        for copy in rim_copies(half):
            copy.start()

    def block_of(far):
        return wrap(a + 4 + halved(far + 1, 1) * (1 - 2 * (far & 1)), GX)

    def part_copy(half, far, turn):
        to_a, to_b = block_of(far), wrap(b + ORDER[turn], GY)
        return pltpu.make_async_remote_copy(
            src_ref=total.at[half, pl.ds(pl.multiple_of(16 * (GY * to_a + to_b), 16), 16)],
            dst_ref=parts.at[half, pl.ds(pl.multiple_of(16 * (GY * a + b), 16), 16)],
            send_sem=part_send.at[half, GY * far + turn],
            recv_sem=part_recv.at[half, GY * far + turn],
            device_id=(to_a, to_b, k),
            device_id_type=MESH,
        )

    def finish_block(half, block):
        rows = pl.ds(pl.multiple_of(8 * block, 8), 8)
        up, low = rims[half, 0, rows, :], rims[half, 1, rows, :]
        cells = []
        for y in range(8):
            back = (128 - 16 * y) % 128
            ends = (pltpu.roll(up, back, 1), pltpu.roll(low, back, 1)) if y else (up, low)
            more = jnp.where(lane < 16, ends[0], jnp.where(lane >= 112, ends[1], 0.0))
            cells.append(acc[half, y, 0, block] + more)
        for y, what in enumerate(cells):
            total[half, pl.ds(pl.multiple_of(64 * block + 8 * y, 8), 8), :] = what

    def send_parts(half):
        for copy in rim_copies(half):
            copy.wait()

        def send_block(far, carry):
            finish_block(half, block_of(far))

            @pl.when(far > 0)
            def _():
                for turn in range(GY):
                    part_copy(half, far - 1, turn).start()

            return carry

        lax.fori_loop(0, GX, send_block, 0)
        for turn in range(GY - 1):
            part_copy(half, jnp.int32(GX - 1), turn).start()
        mine = pl.ds(pl.multiple_of(16 * (GY * a + b), 16), 16)
        parts[half, mine, :] = total[half, mine, :]

    def place_and_send_rims(half):
        place_all(half, 1)
        send_rims(half)
        place_all(half, 0)

    def send_rest(*steps):
        for step, turns in turns_of:
            for turn in turns if step in steps else ():
                piece_copy(0, step, turn).wait_send()
                piece_copy(1, step, turn).start()

    weigh_group(0, 2)
    send_rest(2)
    weigh_group(0, 1)
    send_rest(1)
    weigh_group(0, 3)
    send_rest(3, 0)
    weigh_group(0, 0)
    place_and_send_rims(0)
    weigh_group(1, 2)
    send_parts(0)
    weigh_group(1, 1)
    weigh_group(1, 3)
    weigh_group(1, 0)
    place_and_send_rims(1)
    send_parts(1)

    for offset in range(3 * PX):
        table[offset] = profile(jnp.full((8, 128), offset - PX, jnp.int32), PX)

    def add_weight(index, carry):
        i, j, at_k = a - 2 + lax.div(index, 9), b - 1 + lax.rem(lax.div(index, 3), 3), k - 1 + lax.rem(index, 3)
        valid = (i >= 0) & (i < GX) & (j >= 0) & (j < GY) & (at_k >= 0) & (at_k < GZ)
        i, j, at_k = jnp.clip(i, 0, GX - 1), jnp.clip(j, 0, GY - 1), jnp.clip(at_k, 0, GZ - 1)
        along_z = profile(BZ * k + lane - start_ref[i, 2, j, at_k], PZ)
        along_z = along_z * jnp.where(valid, 1.0, 0.0)
        y = BY * b + sub - start_ref[i, 1, j, at_k]
        planes = [profile(y + 8 * g, PY) * along_z for g in range(4)]
        base = jnp.clip(BX * a - start_ref[i, 0, j, at_k] + PX, 0, 2 * PX)
        new = []
        for x in range(BX):
            along_x = table[base + x]
            new += [carry[4 * x + g] + along_x * planes[g] for g in range(4)]
        return tuple(new)

    weights = lax.fori_loop(0, 45, add_weight, (zero,) * 32)
    for at in range(32):
        sums[at] = weights[at]

    for step, turns in turns_of:
        for turn in turns:
            piece_copy(1, step, turn).wait_send()
    for half in range(2):

        def await_parts(far, carry, half=half):
            for turn in range(GY - 1):
                part_copy(half, far, turn).wait()

            @pl.when(far < GX - 1)
            def _():
                part_copy(half, far, GY - 1).wait()

            return carry

        lax.fori_loop(0, GX, await_parts, 0)

    for x in range(BX):
        for h in range(2):
            for g in range(2):
                row = 8 * g * 16 + 8 * h + x
                norm = sums[4 * x + 2 * h + g]
                d1, d2 = [
                    (parts[half, pl.ds(row, 8, stride=16), :] + parts[half, pl.ds(row + 256, 8, stride=16), :]) / norm
                    for half in range(2)
                ]
                top = jnp.maximum(jnp.maximum(d1, d2), 0.0)
                e0, e1, e2 = jnp.exp(-top), jnp.exp(d1 - top), jnp.exp(d2 - top)
                scale = 1.0 / (e0 + e1 + e2)
                rows = slice(16 * h + 8 * g, 16 * h + 8 * g + 8)
                out_ref[x, 0, rows, :] = e0 * scale
                out_ref[x, 1, rows, :] = e1 * scale
                out_ref[x, 2, rows, :] = e2 * scale


def per_device(patch_logits, patch_start, patch_owner):
    tiles = patch_logits.reshape(GROUPS, 8, LAST + 1, 128)
    probs = pl.pallas_call(
        blend_kernel,
        out_shape=jax.ShapeDtypeStruct((BX, CLASSES, BY, BZ), F32),
        in_specs=[
            pl.BlockSpec(memory_space=pl.ANY),
            pl.BlockSpec(memory_space=pl.ANY),
            pl.BlockSpec(memory_space=pl.ANY),
        ],
        out_specs=pl.BlockSpec(memory_space=pltpu.VMEM),
        scratch_shapes=[
            pltpu.SMEM((GX, GY, GZ), jnp.int32),
            pltpu.SMEM((GX, 3, GY, GZ), jnp.int32),
            pltpu.VMEM((GROUPS, LAST + 1, 8, 128), BF16),
            pltpu.VMEM((16, TILES[0], 8, 128), BF16),
            pltpu.VMEM((16, TILES[1], 8, 128), BF16),
            pltpu.VMEM((16, TILES[0], 8, 128), BF16),
            pltpu.VMEM((16, TILES[1], 8, 128), BF16),
            pltpu.VMEM((3 * PX, 8, 128), F32),
            pltpu.VMEM((32, 8, 128), F32),
            pltpu.VMEM((16, VROWS, 2, GROUPS, 8, 128), F32),
            pltpu.VMEM((SLOTS * VROWS + 1, 2, SPAN, 8, 128), F32),
            pltpu.VMEM((2, 8, 2, GX, 8, 128), F32),
            pltpu.VMEM((2, 2, 64, 128), F32),
            pltpu.VMEM((2, 2, 64, 128), F32),
            pltpu.VMEM((2, 16 * OWNERS, 128), F32),
            pltpu.VMEM((2, 16 * OWNERS, 128), F32),
            pltpu.SemaphoreType.DMA,
            pltpu.SemaphoreType.DMA,
            pltpu.SemaphoreType.DMA,
            pltpu.SemaphoreType.DMA((2, 16)),
            pltpu.SemaphoreType.DMA((2, 16)),
            pltpu.SemaphoreType.DMA((2, 2)),
            pltpu.SemaphoreType.DMA((2, 2)),
            pltpu.SemaphoreType.DMA((2, OWNERS)),
            pltpu.SemaphoreType.DMA((2, OWNERS)),
        ],
        compiler_params=pltpu.CompilerParams(collective_id=0, has_side_effects=True, vmem_limit_bytes=62000000),
    )(patch_owner, jnp.transpose(patch_start, (0, 3, 1, 2)), jnp.transpose(tiles, (0, 2, 1, 3)))
    return jnp.transpose(probs, (0, 2, 1, 3))


def solution(mesh):
    return jax.shard_map(
        per_device,
        mesh=mesh,
        in_specs=(P("gx", "gy", "gz", None, None), P(), P()),
        out_specs=P("gx", "gy", None, "gz"),
        check_vma=False,
    )
```

```python
import jax
import jax.numpy as jnp
from jax import lax
from jax.experimental import pallas as pl
from jax.experimental.pallas import tpu as pltpu
from jax.sharding import PartitionSpec as P

CLASSES = 3
BX, BY, BZ = 8, 32, 128
PX, PY, PZ = 24, 48, 144
GX, GY, GZ = 8, 4, 8
ROW = CLASSES * PZ
RES = 16
VROWS = PY // RES
SLOTS = 16
GROUPS = PX // 8
TILES = (21, 11)
LAST = PY * ROW // 128 - 1
MARGIN = 5
SPAN = 13
OWNERS = GX * GY
F32 = jnp.float32
BF16 = jnp.bfloat16
MESH = pl.DeviceIdType.MESH
ORDER = (2, 1, 3, 0)


def profile(offsets, length):
    inside = (offsets >= 0) & (offsets < length)
    centre = (length - 1) / 2.0
    spread = length / 4.0
    values = jnp.exp(-((offsets.astype(F32) - centre) ** 2) / (2.0 * spread * spread))
    return jnp.where(inside, values, 0.0)


def iota(dim):
    return lax.broadcasted_iota(jnp.int32, (8, 128), dim)


def wrap(index, size):
    return index & (size - 1)


def halved(index, times):
    return lax.shift_right_logical(index, jnp.int32(times))


def hop_of(step, to_b):
    return (0, 1, 2 - 4 * (to_b & 1), -1)[step]


def blend_kernel(
    owner_hbm, start_hbm, x_ref, out_ref,
    owner_ref, start_ref, patch, send0, send1, recv0, recv1, table, sums, kept, value, acc, rim, rims, total, parts,
    in_sem, owner_sem, start_sem, send_sem, recv_sem, rim_send, rim_recv, part_send, part_recv,
):
    a, b, k = lax.axis_index("gx"), lax.axis_index("gy"), lax.axis_index("gz")
    above, below = wrap(k + 1, GZ), wrap(k - 1, GZ)
    send, recv = (send0, send1), (recv0, recv1)
    near = [
        (wrap(a + dz, GX), wrap(b + db, GY), k) for dz in (0, 1, -1, 2, -2) for db in range(GY) if dz or db
    ] + [(a, b, above), (a, b, below)]
    barrier = pltpu.get_barrier_semaphore()
    for to in near:
        pl.semaphore_signal(barrier, inc=1, device_id=to, device_id_type=MESH)
    load = pltpu.make_async_copy(x_ref, patch, in_sem)
    load.start()
    indices = [
        pltpu.make_async_copy(owner_hbm, owner_ref, owner_sem),
        pltpu.make_async_copy(start_hbm, start_ref, start_sem),
    ]
    for copy in indices:
        copy.start()

    lane, sub = iota(1), iota(0)
    zero = jnp.zeros((8, 128), F32)

    def start_of(code, at_k, dim):
        return start_ref[halved(code, 2), dim, code & (GY - 1), at_k]

    for copy in indices:
        copy.wait()
    my_sy = start_of(owner_ref[a, b, k], k, 1)
    load.wait()

    def cut(half, residue, store):
        rho = (residue - my_sy) & (RES - 1)
        skip, length = ((0, 2 * PZ), (2 * PZ, PZ))[half]
        tails = []
        for g in range(GROUPS):
            tiles = {}
            for v in range(VROWS):
                into = length * v
                delta = ROW * rho + (ROW * RES * v + skip - into)
                first = halved(delta + 127, 7)
                turn = first * 128 - delta
                low, high = into // 128, (into + length - 1) // 128
                turned = []
                for t in range(low - 1, high + 1):
                    at = first + t
                    if t < 0:
                        at = jnp.maximum(at, 0)
                    if half == 1 and v == VROWS - 1 and t == high:
                        at = jnp.minimum(at, LAST)
                    turned.append(pltpu.roll(patch[g, at].astype(F32), turn, 1))
                for t in range(low, high + 1):
                    tile = jnp.where(lane < turn, turned[t - low], turned[t - low + 1])
                    tiles[t] = jnp.where(lane < into % 128, tiles[t], tile) if t in tiles else tile
            for t in range(7 if half == 0 else 3):
                store(GROUPS * t + g, tiles[t].astype(BF16))
            if half == 1:
                tails.append(tiles[3])
        if half == 1:
            store(9, jnp.where(lane < 48, tails[0], pltpu.roll(tails[1], 48, 1)).astype(BF16))
            store(10, tails[2].astype(BF16))

    def piece_copy(half, step, turn):
        to_b = wrap(b + turn, GY)
        return pltpu.make_async_remote_copy(
            src_ref=send[half].at[4 * step + turn],
            dst_ref=recv[half].at[4 * step + b],
            send_sem=send_sem.at[half, 4 * step + turn],
            recv_sem=recv_sem.at[half, 4 * step + b],
            device_id=(wrap(a + hop_of(step, to_b), GX), to_b, k),
            device_id_type=MESH,
        )

    def piece_arrival(half, step, from_b):
        return pltpu.make_async_remote_copy(
            src_ref=send[half].at[4 * step],
            dst_ref=recv[half].at[4 * step + from_b],
            send_sem=send_sem.at[half, 4 * step],
            recv_sem=recv_sem.at[half, 4 * step + from_b],
            device_id=(a, b, above),
            device_id_type=MESH,
        )

    turns_of = [(step, [turn for turn in ORDER if step or turn]) for step in ORDER]
    def cut_step(half, step):
        def cut_one(turn, carry):
            def store(tile, what):
                send[half][4 * step + turn, tile] = what

            cut(half, 4 * wrap(a + step, 4) + wrap(b + turn, GY), store)
            return carry

        lax.fori_loop(0 if step else 1, GY, cut_one, 0)

    def cut_own(half):
        def store(tile, what):
            recv[half][b, tile] = what

        cut(half, 4 * wrap(a, 4) + b, store)

    for step, turns in turns_of:
        cut_step(0, step)
        if step == 2:
            pl.semaphore_wait(barrier, len(near))
        for turn in turns:
            piece_copy(0, step, turn).start()
    cut_own(0)
    for step, _ in turns_of:
        cut_step(1, step)
    cut_own(1)

    for t in range(2):
        for at in range(SPAN):
            value[SLOTS * VROWS, t, at] = zero

    def clear(at, carry):
        for t in range(2):
            for margin in (*range(MARGIN), *range(MARGIN + GROUPS + 1, SPAN)):
                value[at, t, margin] = zero
        return carry

    lax.fori_loop(0, SLOTS * VROWS, clear, 0)

    residue = 4 * wrap(a, 4) + b
    along_x = [profile(sub + 8 * g, PX) for g in range(GROUPS)]
    columns = (lane, jnp.where(lane < 64, lane + 128, lane - 128))

    def corner(step, from_b):
        from_a = wrap(a - hop_of(step, b), GX)
        code = owner_ref[from_a, from_b, k]
        sy = start_of(code, k, 1)
        rho = (residue - sy) & (RES - 1)
        return start_of(code, k, 0), halved(sy + rho, 4), rho, start_of(code, k, 2) - BZ * k

    def aligned(first, second, shift, lead):
        turn = (shift - lead) & 255
        low = turn & 127
        swap = (jnp.where(lane < low, 1, 0) + halved(turn, 7)) == 1
        first, second = pltpu.roll(first.astype(F32), low, 1), pltpu.roll(second.astype(F32), low, 1)
        return jnp.where(swap, second, first), jnp.where(swap, first, second)

    def weigh_group(half, step):
        def weigh(from_b, carry):
            slot = 4 * step + from_b
            if step == 0:

                @pl.when(from_b != b)
                def _():
                    piece_arrival(half, step, from_b).wait_recv()

            else:
                piece_arrival(half, step, from_b).wait_recv()
            sx, _, rho, shift = corner(step, from_b)
            turn_x = sx & 7
            along_z = [profile(c - shift, PZ) for c in columns]
            held = {}
            for v in range(VROWS):
                for g in range(GROUPS):
                    if half == 0:
                        for m in (2 * v, 2 * v + 1):
                            held[m, g] = recv0[slot, GROUPS * m + g], recv0[slot, GROUPS * m + GROUPS + g]
                    else:
                        tail = 9 + g // 2 if v == VROWS - 1 else GROUPS * v + GROUPS + g
                        held[v, g] = recv1[slot, GROUPS * v + g], recv1[slot, tail]
                        held[v, g, 0] = [kept[slot, v, t, g] for t in range(2)]
            for v in range(VROWS):
                along_y = profile(jnp.full((8, 128), RES * v, jnp.int32) + rho, PY)
                turned = [[], []]
                for g in range(GROUPS):
                    if half == 0:
                        base, upper = [aligned(*held[m, g], shift, 16 * m) for m in (2 * v, 2 * v + 1)]
                        for t in range(2):
                            kept[slot, v, t, g] = base[t]
                    else:
                        first, second = held[v, g]
                        if v == VROWS - 1 and g == 1:
                            second = pltpu.roll(second.astype(F32), 80, 1)
                        upper = aligned(first, second, shift, 16 * v)
                        base = held[v, g, 0]
                    along_xy = along_x[g] * along_y
                    for t in range(2):
                        product = (upper[t] - base[t]) * (along_xy * along_z[t])
                        turned[t].append(pltpu.roll(product, turn_x, 0))
                for t in range(2):
                    ends = [zero] + turned[t] + [zero]
                    for g in range(GROUPS + 1):
                        value[VROWS * slot + v, t, MARGIN + g] = jnp.where(sub < turn_x, ends[g], ends[g + 1])
            return carry

        lax.fori_loop(0, GY, weigh, 0)

    def place_all(half, t):
        corners = [(4 * step + from_b, corner(step, from_b)) for step in range(4) for from_b in range(GY)]
        bases = [(VROWS * slot - first_y, first_y, MARGIN - halved(sx, 3)) for slot, (sx, first_y, _, _) in corners]

        def place(y, carry):
            places = []
            for base, first_y, at in bases:
                valid = (y >= first_y) & (y < first_y + VROWS)
                places.append((jnp.where(valid, base + y, SLOTS * VROWS), at))
            got = [value[v, t, pl.ds(at, GX)] for v, at in places]
            while len(got) > 1:
                got = [one + two for one, two in zip(got[::2], got[1::2])]
            acc[half, y, t] = got[0]
            return carry

        lax.fori_loop(0, 8, place, 0)

    def rim_copies(half):
        return [
            pltpu.make_async_remote_copy(
                src_ref=rim.at[half, side],
                dst_ref=rims.at[half, side],
                send_sem=rim_send.at[half, side],
                recv_sem=rim_recv.at[half, side],
                device_id=(a, b, to_k),
                device_id_type=MESH,
            )
            for side, to_k in ((0, above), (1, below))
        ]

    def send_rims(half):
        for block in range(GX):
            rows = slice(8 * block, 8 * block + 8)
            up, low = zero, zero
            for y in range(8):
                turned = acc[half, y, 1, block]
                turned = pltpu.roll(turned, 16 * y, 1) if y else turned
                up = jnp.where(lane // 16 == y, turned, up)
                low = jnp.where(lane // 16 == (y + 7) % 8, turned, low)
            rim[half, 0, rows, :] = up
            rim[half, 1, rows, :] = low
        for copy in rim_copies(half):
            copy.start()

    def block_of(far):
        return wrap(a + 4 + halved(far + 1, 1) * (1 - 2 * (far & 1)), GX)

    def part_copy(half, far, turn):
        to_a, to_b = block_of(far), wrap(b + ORDER[turn], GY)
        return pltpu.make_async_remote_copy(
            src_ref=total.at[half, pl.ds(pl.multiple_of(16 * (GY * to_a + to_b), 16), 16)],
            dst_ref=parts.at[half, pl.ds(pl.multiple_of(16 * (GY * a + b), 16), 16)],
            send_sem=part_send.at[half, GY * far + turn],
            recv_sem=part_recv.at[half, GY * far + turn],
            device_id=(to_a, to_b, k),
            device_id_type=MESH,
        )

    def finish_block(half, block):
        rows = pl.ds(pl.multiple_of(8 * block, 8), 8)
        up, low = rims[half, 0, rows, :], rims[half, 1, rows, :]
        cells = []
        for y in range(8):
            back = (128 - 16 * y) % 128
            ends = (pltpu.roll(up, back, 1), pltpu.roll(low, back, 1)) if y else (up, low)
            more = jnp.where(lane < 16, ends[0], jnp.where(lane >= 112, ends[1], 0.0))
            cells.append(acc[half, y, 0, block] + more)
        for y, what in enumerate(cells):
            total[half, pl.ds(pl.multiple_of(64 * block + 8 * y, 8), 8), :] = what

    def send_parts(half):
        for copy in rim_copies(half):
            copy.wait()

        def send_block(far, carry):
            finish_block(half, block_of(far))

            @pl.when(far > 0)
            def _():
                for turn in range(GY):
                    part_copy(half, far - 1, turn).start()

            return carry

        lax.fori_loop(0, GX, send_block, 0)
        for turn in range(GY - 1):
            part_copy(half, jnp.int32(GX - 1), turn).start()
        mine = pl.ds(pl.multiple_of(16 * (GY * a + b), 16), 16)
        parts[half, mine, :] = total[half, mine, :]

    def place_and_send_rims(half):
        place_all(half, 1)
        send_rims(half)
        place_all(half, 0)

    def send_rest(*steps):
        for step, turns in turns_of:
            for turn in turns if step in steps else ():
                piece_copy(0, step, turn).wait_send()
                piece_copy(1, step, turn).start()

    weigh_group(0, 2)
    send_rest(2)
    weigh_group(0, 1)
    send_rest(1)
    weigh_group(0, 3)
    send_rest(3, 0)
    weigh_group(0, 0)
    place_and_send_rims(0)
    weigh_group(1, 2)
    send_parts(0)
    weigh_group(1, 1)
    weigh_group(1, 3)
    weigh_group(1, 0)
    place_and_send_rims(1)
    send_parts(1)

    for offset in range(3 * PX):
        table[offset] = profile(jnp.full((8, 128), offset - PX, jnp.int32), PX)

    def add_weight(index, carry):
        i, j, at_k = a - 2 + lax.div(index, 9), b - 1 + lax.rem(lax.div(index, 3), 3), k - 1 + lax.rem(index, 3)
        valid = (i >= 0) & (i < GX) & (j >= 0) & (j < GY) & (at_k >= 0) & (at_k < GZ)
        i, j, at_k = jnp.clip(i, 0, GX - 1), jnp.clip(j, 0, GY - 1), jnp.clip(at_k, 0, GZ - 1)
        along_z = profile(BZ * k + lane - start_ref[i, 2, j, at_k], PZ)
        along_z = along_z * jnp.where(valid, 1.0, 0.0)
        y = BY * b + sub - start_ref[i, 1, j, at_k]
        planes = [profile(y + 8 * g, PY) * along_z for g in range(4)]
        base = jnp.clip(BX * a - start_ref[i, 0, j, at_k] + PX, 0, 2 * PX)
        new = []
        for x in range(BX):
            along_x = table[base + x]
            new += [carry[4 * x + g] + along_x * planes[g] for g in range(4)]
        return tuple(new)

    weights = lax.fori_loop(0, 45, add_weight, (zero,) * 32)
    for at in range(32):
        sums[at] = weights[at]

    for step, turns in turns_of:
        for turn in turns:
            piece_copy(1, step, turn).wait_send()
    for half in range(2):

        def await_parts(far, carry, half=half):
            for turn in range(GY - 1):
                part_copy(half, far, turn).wait()

            @pl.when(far < GX - 1)
            def _():
                part_copy(half, far, GY - 1).wait()

            return carry

        lax.fori_loop(0, GX, await_parts, 0)

    for x in range(BX):
        for h in range(2):
            for g in range(2):
                row = 8 * g * 16 + 8 * h + x
                norm = sums[4 * x + 2 * h + g]
                d1, d2 = [
                    (parts[half, pl.ds(row, 8, stride=16), :] + parts[half, pl.ds(row + 256, 8, stride=16), :]) / norm
                    for half in range(2)
                ]
                top = jnp.maximum(jnp.maximum(d1, d2), 0.0)
                e0, e1, e2 = jnp.exp(-top), jnp.exp(d1 - top), jnp.exp(d2 - top)
                scale = 1.0 / (e0 + e1 + e2)
                rows = slice(16 * h + 8 * g, 16 * h + 8 * g + 8)
                out_ref[x, 0, rows, :] = e0 * scale
                out_ref[x, 1, rows, :] = e1 * scale
                out_ref[x, 2, rows, :] = e2 * scale


def per_device(patch_logits, patch_start, patch_owner):
    tiles = patch_logits.reshape(GROUPS, 8, LAST + 1, 128)
    probs = pl.pallas_call(
        blend_kernel,
        out_shape=jax.ShapeDtypeStruct((BX, CLASSES, BY, BZ), F32),
        in_specs=[
            pl.BlockSpec(memory_space=pl.ANY),
            pl.BlockSpec(memory_space=pl.ANY),
            pl.BlockSpec(memory_space=pl.ANY),
        ],
        out_specs=pl.BlockSpec(memory_space=pltpu.VMEM),
        scratch_shapes=[
            pltpu.SMEM((GX, GY, GZ), jnp.int32),
            pltpu.SMEM((GX, 3, GY, GZ), jnp.int32),
            pltpu.VMEM((GROUPS, LAST + 1, 8, 128), BF16),
            pltpu.VMEM((16, TILES[0], 8, 128), BF16),
            pltpu.VMEM((16, TILES[1], 8, 128), BF16),
            pltpu.VMEM((16, TILES[0], 8, 128), BF16),
            pltpu.VMEM((16, TILES[1], 8, 128), BF16),
            pltpu.VMEM((3 * PX, 8, 128), F32),
            pltpu.VMEM((32, 8, 128), F32),
            pltpu.VMEM((16, VROWS, 2, GROUPS, 8, 128), F32),
            pltpu.VMEM((SLOTS * VROWS + 1, 2, SPAN, 8, 128), F32),
            pltpu.VMEM((2, 8, 2, GX, 8, 128), F32),
            pltpu.VMEM((2, 2, 64, 128), F32),
            pltpu.VMEM((2, 2, 64, 128), F32),
            pltpu.VMEM((2, 16 * OWNERS, 128), F32),
            pltpu.VMEM((2, 16 * OWNERS, 128), F32),
            pltpu.SemaphoreType.DMA,
            pltpu.SemaphoreType.DMA,
            pltpu.SemaphoreType.DMA,
            pltpu.SemaphoreType.DMA((2, 16)),
            pltpu.SemaphoreType.DMA((2, 16)),
            pltpu.SemaphoreType.DMA((2, 2)),
            pltpu.SemaphoreType.DMA((2, 2)),
            pltpu.SemaphoreType.DMA((2, OWNERS)),
            pltpu.SemaphoreType.DMA((2, OWNERS)),
        ],
        compiler_params=pltpu.CompilerParams(collective_id=0, has_side_effects=True, vmem_limit_bytes=56000000),
    )(patch_owner, jnp.transpose(patch_start, (0, 3, 1, 2)), jnp.transpose(tiles, (0, 2, 1, 3)))
    return jnp.transpose(probs, (0, 2, 1, 3))


def solution(mesh):
    return jax.shard_map(
        per_device,
        mesh=mesh,
        in_specs=(P("gx", "gy", "gz", None, None), P(), P()),
        out_specs=P("gx", "gy", None, "gz"),
        check_vma=False,
    )
```

```python
import jax
import jax.numpy as jnp
from jax import lax
from jax.experimental import pallas as pl
from jax.experimental.pallas import tpu as pltpu
from jax.sharding import PartitionSpec as P

CLASSES = 3
BX, BY, BZ = 8, 32, 128
PX, PY, PZ = 24, 48, 144
GX, GY, GZ = 8, 4, 8
ROW = CLASSES * PZ
RES = 16
VROWS = PY // RES
SLOTS = 16
GROUPS = PX // 8
TILES = (21, 11)
LAST = PY * ROW // 128 - 1
MARGIN = 5
SPAN = 13
OWNERS = GX * GY
F32 = jnp.float32
BF16 = jnp.bfloat16
MESH = pl.DeviceIdType.MESH
ORDER = (2, 1, 3, 0)


def profile(offsets, length):
    inside = (offsets >= 0) & (offsets < length)
    centre = (length - 1) / 2.0
    spread = length / 4.0
    values = jnp.exp(-((offsets.astype(F32) - centre) ** 2) / (2.0 * spread * spread))
    return jnp.where(inside, values, 0.0)


def iota(dim):
    return lax.broadcasted_iota(jnp.int32, (8, 128), dim)


def wrap(index, size):
    return index & (size - 1)


def halved(index, times):
    return lax.shift_right_logical(index, jnp.int32(times))


def hop_of(step, to_b):
    return (0, 1, 2 - 4 * (to_b & 1), -1)[step]


def blend_kernel(
    owner_hbm, start_hbm, x_ref, out_ref,
    owner_ref, start_ref, patch, send0, send1, recv0, recv1, table, sums, kept, value, acc, rim, rims, total, parts,
    in_sem, owner_sem, start_sem, send_sem, recv_sem, rim_send, rim_recv, part_send, part_recv,
):
    a, b, k = lax.axis_index("gx"), lax.axis_index("gy"), lax.axis_index("gz")
    above, below = wrap(k + 1, GZ), wrap(k - 1, GZ)
    send, recv = (send0, send1), (recv0, recv1)
    near = [
        (wrap(a + dz, GX), wrap(b + db, GY), k) for dz in (0, 1, -1, 2, -2) for db in range(GY) if dz or db
    ] + [(a, b, above), (a, b, below)]
    barrier = pltpu.get_barrier_semaphore()
    for to in near:
        pl.semaphore_signal(barrier, inc=1, device_id=to, device_id_type=MESH)
    load = pltpu.make_async_copy(x_ref, patch, in_sem)
    load.start()
    indices = [
        pltpu.make_async_copy(owner_hbm, owner_ref, owner_sem),
        pltpu.make_async_copy(start_hbm, start_ref, start_sem),
    ]
    for copy in indices:
        copy.start()

    lane, sub = iota(1), iota(0)
    zero = jnp.zeros((8, 128), F32)

    def start_of(code, at_k, dim):
        return start_ref[halved(code, 2), dim, code & (GY - 1), at_k]

    for copy in indices:
        copy.wait()
    my_sy = start_of(owner_ref[a, b, k], k, 1)
    load.wait()

    def cut(half, residue, store):
        rho = (residue - my_sy) & (RES - 1)
        skip, length = ((0, 2 * PZ), (2 * PZ, PZ))[half]
        tails = []
        for g in range(GROUPS):
            tiles = {}
            for v in range(VROWS):
                into = length * v
                delta = ROW * rho + (ROW * RES * v + skip - into)
                first = halved(delta + 127, 7)
                turn = first * 128 - delta
                low, high = into // 128, (into + length - 1) // 128
                turned = []
                for t in range(low - 1, high + 1):
                    at = first + t
                    if t < 0:
                        at = jnp.maximum(at, 0)
                    if half == 1 and v == VROWS - 1 and t == high:
                        at = jnp.minimum(at, LAST)
                    turned.append(pltpu.roll(patch[g, at].astype(F32), turn, 1))
                for t in range(low, high + 1):
                    tile = jnp.where(lane < turn, turned[t - low], turned[t - low + 1])
                    tiles[t] = jnp.where(lane < into % 128, tiles[t], tile) if t in tiles else tile
            for t in range(7 if half == 0 else 3):
                store(GROUPS * t + g, tiles[t].astype(BF16))
            if half == 1:
                tails.append(tiles[3])
        if half == 1:
            store(9, jnp.where(lane < 48, tails[0], pltpu.roll(tails[1], 48, 1)).astype(BF16))
            store(10, tails[2].astype(BF16))

    def piece_copy(half, step, turn):
        to_b = wrap(b + turn, GY)
        return pltpu.make_async_remote_copy(
            src_ref=send[half].at[4 * step + turn],
            dst_ref=recv[half].at[4 * step + b],
            send_sem=send_sem.at[half, 4 * step + turn],
            recv_sem=recv_sem.at[half, 4 * step + b],
            device_id=(wrap(a + hop_of(step, to_b), GX), to_b, k),
            device_id_type=MESH,
        )

    def piece_arrival(half, step, from_b):
        return pltpu.make_async_remote_copy(
            src_ref=send[half].at[4 * step],
            dst_ref=recv[half].at[4 * step + from_b],
            send_sem=send_sem.at[half, 4 * step],
            recv_sem=recv_sem.at[half, 4 * step + from_b],
            device_id=(a, b, above),
            device_id_type=MESH,
        )

    turns_of = [(step, [turn for turn in ORDER if step or turn]) for step in ORDER]
    def cut_step(half, step):
        def cut_one(turn, carry):
            def store(tile, what):
                send[half][4 * step + turn, tile] = what

            cut(half, 4 * wrap(a + step, 4) + wrap(b + turn, GY), store)
            return carry

        lax.fori_loop(0 if step else 1, GY, cut_one, 0)

    def cut_own(half):
        def store(tile, what):
            recv[half][b, tile] = what

        cut(half, 4 * wrap(a, 4) + b, store)

    for step, turns in turns_of:
        cut_step(0, step)
        if step == 2:
            pl.semaphore_wait(barrier, len(near))
        for turn in turns:
            piece_copy(0, step, turn).start()
    cut_own(0)
    for step, _ in turns_of:
        cut_step(1, step)
    cut_own(1)

    for t in range(2):
        for at in range(SPAN):
            value[SLOTS * VROWS, t, at] = zero

    def clear(at, carry):
        for t in range(2):
            for margin in (*range(MARGIN), *range(MARGIN + GROUPS + 1, SPAN)):
                value[at, t, margin] = zero
        return carry

    lax.fori_loop(0, SLOTS * VROWS, clear, 0)

    residue = 4 * wrap(a, 4) + b
    along_x = [profile(sub + 8 * g, PX) for g in range(GROUPS)]
    columns = (lane, jnp.where(lane < 64, lane + 128, lane - 128))

    def corner(step, from_b):
        from_a = wrap(a - hop_of(step, b), GX)
        code = owner_ref[from_a, from_b, k]
        sy = start_of(code, k, 1)
        rho = (residue - sy) & (RES - 1)
        return start_of(code, k, 0), halved(sy + rho, 4), rho, start_of(code, k, 2) - BZ * k

    def aligned(first, second, shift, lead):
        turn = (shift - lead) & 255
        low = turn & 127
        swap = (jnp.where(lane < low, 1, 0) + halved(turn, 7)) == 1
        first, second = pltpu.roll(first.astype(F32), low, 1), pltpu.roll(second.astype(F32), low, 1)
        return jnp.where(swap, second, first), jnp.where(swap, first, second)

    def weigh_group(half, step):
        def weigh(from_b, carry):
            slot = 4 * step + from_b
            if step == 0:

                @pl.when(from_b != b)
                def _():
                    piece_arrival(half, step, from_b).wait_recv()

            else:
                piece_arrival(half, step, from_b).wait_recv()
            sx, _, rho, shift = corner(step, from_b)
            turn_x = sx & 7
            along_z = [profile(c - shift, PZ) for c in columns]
            held = {}
            for v in range(VROWS):
                for g in range(GROUPS):
                    if half == 0:
                        for m in (2 * v, 2 * v + 1):
                            held[m, g] = recv0[slot, GROUPS * m + g], recv0[slot, GROUPS * m + GROUPS + g]
                    else:
                        tail = 9 + g // 2 if v == VROWS - 1 else GROUPS * v + GROUPS + g
                        held[v, g] = recv1[slot, GROUPS * v + g], recv1[slot, tail]
                        held[v, g, 0] = [kept[slot, v, t, g] for t in range(2)]
            for v in range(VROWS):
                along_y = profile(jnp.full((8, 128), RES * v, jnp.int32) + rho, PY)
                turned = [[], []]
                for g in range(GROUPS):
                    if half == 0:
                        base, upper = [aligned(*held[m, g], shift, 16 * m) for m in (2 * v, 2 * v + 1)]
                        for t in range(2):
                            kept[slot, v, t, g] = base[t]
                    else:
                        first, second = held[v, g]
                        if v == VROWS - 1 and g == 1:
                            second = pltpu.roll(second.astype(F32), 80, 1)
                        upper = aligned(first, second, shift, 16 * v)
                        base = held[v, g, 0]
                    along_xy = along_x[g] * along_y
                    for t in range(2):
                        product = (upper[t] - base[t]) * (along_xy * along_z[t])
                        turned[t].append(pltpu.roll(product, turn_x, 0))
                for t in range(2):
                    ends = [zero] + turned[t] + [zero]
                    for g in range(GROUPS + 1):
                        value[VROWS * slot + v, t, MARGIN + g] = jnp.where(sub < turn_x, ends[g], ends[g + 1])
            return carry

        lax.fori_loop(0, GY, weigh, 0)

    def place_all(half, t):
        corners = [(4 * step + from_b, corner(step, from_b)) for step in range(4) for from_b in range(GY)]
        bases = [(VROWS * slot - first_y, first_y, MARGIN - halved(sx, 3)) for slot, (sx, first_y, _, _) in corners]

        def place(y, carry):
            places = []
            for base, first_y, at in bases:
                valid = (y >= first_y) & (y < first_y + VROWS)
                places.append((jnp.where(valid, base + y, SLOTS * VROWS), at))
            got = [value[v, t, pl.ds(at, GX)] for v, at in places]
            while len(got) > 1:
                got = [one + two for one, two in zip(got[::2], got[1::2])]
            acc[half, y, t] = got[0]
            return carry

        lax.fori_loop(0, 8, place, 0)

    def rim_copies(half):
        return [
            pltpu.make_async_remote_copy(
                src_ref=rim.at[half, side],
                dst_ref=rims.at[half, side],
                send_sem=rim_send.at[half, side],
                recv_sem=rim_recv.at[half, side],
                device_id=(a, b, to_k),
                device_id_type=MESH,
            )
            for side, to_k in ((0, above), (1, below))
        ]

    def send_rims(half):
        for block in range(GX):
            rows = slice(8 * block, 8 * block + 8)
            up, low = zero, zero
            for y in range(8):
                turned = acc[half, y, 1, block]
                turned = pltpu.roll(turned, 16 * y, 1) if y else turned
                up = jnp.where(lane // 16 == y, turned, up)
                low = jnp.where(lane // 16 == (y + 7) % 8, turned, low)
            rim[half, 0, rows, :] = up
            rim[half, 1, rows, :] = low
        for copy in rim_copies(half):
            copy.start()

    def block_of(far):
        return wrap(a + 4 + halved(far + 1, 1) * (1 - 2 * (far & 1)), GX)

    def part_copy(half, far, turn):
        to_a, to_b = block_of(far), wrap(b + ORDER[turn], GY)
        return pltpu.make_async_remote_copy(
            src_ref=total.at[half, pl.ds(pl.multiple_of(16 * (GY * to_a + to_b), 16), 16)],
            dst_ref=parts.at[half, pl.ds(pl.multiple_of(16 * (GY * a + b), 16), 16)],
            send_sem=part_send.at[half, GY * far + turn],
            recv_sem=part_recv.at[half, GY * far + turn],
            device_id=(to_a, to_b, k),
            device_id_type=MESH,
        )

    def finish_block(half, block):
        rows = pl.ds(pl.multiple_of(8 * block, 8), 8)
        up, low = rims[half, 0, rows, :], rims[half, 1, rows, :]
        cells = []
        for y in range(8):
            back = (128 - 16 * y) % 128
            ends = (pltpu.roll(up, back, 1), pltpu.roll(low, back, 1)) if y else (up, low)
            more = jnp.where(lane < 16, ends[0], jnp.where(lane >= 112, ends[1], 0.0))
            cells.append(acc[half, y, 0, block] + more)
        for y, what in enumerate(cells):
            total[half, pl.ds(pl.multiple_of(64 * block + 8 * y, 8), 8), :] = what

    def send_parts(half):
        for copy in rim_copies(half):
            copy.wait()

        def send_block(far, carry):
            finish_block(half, block_of(far))

            @pl.when(far > 0)
            def _():
                for turn in range(GY):
                    part_copy(half, far - 1, turn).start()

            return carry

        lax.fori_loop(0, GX, send_block, 0)
        for turn in range(GY - 1):
            part_copy(half, jnp.int32(GX - 1), turn).start()
        mine = pl.ds(pl.multiple_of(16 * (GY * a + b), 16), 16)
        parts[half, mine, :] = total[half, mine, :]

    def place_and_send_rims(half):
        place_all(half, 1)
        send_rims(half)
        place_all(half, 0)

    def send_rest(*steps):
        for step, turns in turns_of:
            for turn in turns if step in steps else ():
                piece_copy(0, step, turn).wait_send()
                piece_copy(1, step, turn).start()

    weigh_group(0, 2)
    send_rest(2)
    weigh_group(0, 1)
    send_rest(1)
    weigh_group(0, 3)
    send_rest(3, 0)
    weigh_group(0, 0)
    place_and_send_rims(0)
    weigh_group(1, 2)
    send_parts(0)
    weigh_group(1, 1)
    weigh_group(1, 3)
    weigh_group(1, 0)
    place_and_send_rims(1)
    send_parts(1)

    for offset in range(3 * PX):
        table[offset] = profile(jnp.full((8, 128), offset - PX, jnp.int32), PX)

    def add_weight(index, carry):
        i, j, at_k = a - 2 + lax.div(index, 9), b - 1 + lax.rem(lax.div(index, 3), 3), k - 1 + lax.rem(index, 3)
        valid = (i >= 0) & (i < GX) & (j >= 0) & (j < GY) & (at_k >= 0) & (at_k < GZ)
        i, j, at_k = jnp.clip(i, 0, GX - 1), jnp.clip(j, 0, GY - 1), jnp.clip(at_k, 0, GZ - 1)
        along_z = profile(BZ * k + lane - start_ref[i, 2, j, at_k], PZ)
        along_z = along_z * jnp.where(valid, 1.0, 0.0)
        y = BY * b + sub - start_ref[i, 1, j, at_k]
        planes = [profile(y + 8 * g, PY) * along_z for g in range(4)]
        base = jnp.clip(BX * a - start_ref[i, 0, j, at_k] + PX, 0, 2 * PX)
        new = []
        for x in range(BX):
            along_x = table[base + x]
            new += [carry[4 * x + g] + along_x * planes[g] for g in range(4)]
        return tuple(new)

    weights = lax.fori_loop(0, 45, add_weight, (zero,) * 32)
    for at in range(32):
        sums[at] = weights[at]

    for step, turns in turns_of:
        for turn in turns:
            piece_copy(1, step, turn).wait_send()
    for half in range(2):

        def await_parts(far, carry, half=half):
            for turn in range(GY - 1):
                part_copy(half, far, turn).wait()

            @pl.when(far < GX - 1)
            def _():
                part_copy(half, far, GY - 1).wait()

            return carry

        lax.fori_loop(0, GX, await_parts, 0)

    for x in range(BX):
        for h in range(2):
            for g in range(2):
                row = 8 * g * 16 + 8 * h + x
                norm = sums[4 * x + 2 * h + g]
                d1, d2 = [
                    (parts[half, pl.ds(row, 8, stride=16), :] + parts[half, pl.ds(row + 256, 8, stride=16), :]) / norm
                    for half in range(2)
                ]
                top = jnp.maximum(jnp.maximum(d1, d2), 0.0)
                e0, e1, e2 = jnp.exp(-top), jnp.exp(d1 - top), jnp.exp(d2 - top)
                scale = 1.0 / (e0 + e1 + e2)
                rows = slice(16 * h + 8 * g, 16 * h + 8 * g + 8)
                out_ref[x, 0, rows, :] = e0 * scale
                out_ref[x, 1, rows, :] = e1 * scale
                out_ref[x, 2, rows, :] = e2 * scale


def per_device(patch_logits, patch_start, patch_owner):
    tiles = patch_logits.reshape(GROUPS, 8, LAST + 1, 128)
    probs = pl.pallas_call(
        blend_kernel,
        out_shape=jax.ShapeDtypeStruct((BX, CLASSES, BY, BZ), F32),
        in_specs=[
            pl.BlockSpec(memory_space=pl.ANY),
            pl.BlockSpec(memory_space=pl.ANY),
            pl.BlockSpec(memory_space=pl.ANY),
        ],
        out_specs=pl.BlockSpec(memory_space=pltpu.VMEM),
        scratch_shapes=[
            pltpu.SMEM((GX, GY, GZ), jnp.int32),
            pltpu.SMEM((GX, 3, GY, GZ), jnp.int32),
            pltpu.VMEM((GROUPS, LAST + 1, 8, 128), BF16),
            pltpu.VMEM((16, TILES[0], 8, 128), BF16),
            pltpu.VMEM((16, TILES[1], 8, 128), BF16),
            pltpu.VMEM((16, TILES[0], 8, 128), BF16),
            pltpu.VMEM((16, TILES[1], 8, 128), BF16),
            pltpu.VMEM((3 * PX, 8, 128), F32),
            pltpu.VMEM((32, 8, 128), F32),
            pltpu.VMEM((16, VROWS, 2, GROUPS, 8, 128), F32),
            pltpu.VMEM((SLOTS * VROWS + 1, 2, SPAN, 8, 128), F32),
            pltpu.VMEM((2, 8, 2, GX, 8, 128), F32),
            pltpu.VMEM((2, 2, 64, 128), F32),
            pltpu.VMEM((2, 2, 64, 128), F32),
            pltpu.VMEM((2, 16 * OWNERS, 128), F32),
            pltpu.VMEM((2, 16 * OWNERS, 128), F32),
            pltpu.SemaphoreType.DMA,
            pltpu.SemaphoreType.DMA,
            pltpu.SemaphoreType.DMA,
            pltpu.SemaphoreType.DMA((2, 16)),
            pltpu.SemaphoreType.DMA((2, 16)),
            pltpu.SemaphoreType.DMA((2, 2)),
            pltpu.SemaphoreType.DMA((2, 2)),
            pltpu.SemaphoreType.DMA((2, OWNERS)),
            pltpu.SemaphoreType.DMA((2, OWNERS)),
        ],
        compiler_params=pltpu.CompilerParams(collective_id=0, has_side_effects=True, vmem_limit_bytes=56000000),
    )(
        pltpu.with_memory_space_constraint(patch_owner, pltpu.HBM),
        pltpu.with_memory_space_constraint(jnp.transpose(patch_start, (0, 3, 1, 2)), pltpu.HBM),
        jnp.transpose(tiles, (0, 2, 1, 3)),
    )
    return jnp.transpose(probs, (0, 2, 1, 3))


def solution(mesh):
    return jax.shard_map(
        per_device,
        mesh=mesh,
        in_specs=(P("gx", "gy", "gz", None, None), P(), P()),
        out_specs=P("gx", "gy", None, "gz"),
        check_vma=False,
    )
```

```python
import jax
import jax.numpy as jnp
from jax import lax
from jax.experimental import pallas as pl
from jax.experimental.pallas import tpu as pltpu
from jax.sharding import PartitionSpec as P

CLASSES = 3
BX, BY, BZ = 8, 32, 128
PX, PY, PZ = 24, 48, 144
GX, GY, GZ = 8, 4, 8
ROW = CLASSES * PZ
RES = 16
VROWS = PY // RES
SLOTS = 16
GROUPS = PX // 8
TILES = (21, 11)
LAST = PY * ROW // 128 - 1
MARGIN = 5
SPAN = 13
OWNERS = GX * GY
F32 = jnp.float32
BF16 = jnp.bfloat16
MESH = pl.DeviceIdType.MESH
ORDER = (2, 1, 3, 0)


def profile(offsets, length):
    inside = (offsets >= 0) & (offsets < length)
    centre = (length - 1) / 2.0
    spread = length / 4.0
    values = jnp.exp(-((offsets.astype(F32) - centre) ** 2) / (2.0 * spread * spread))
    return jnp.where(inside, values, 0.0)


def iota(dim):
    return lax.broadcasted_iota(jnp.int32, (8, 128), dim)


def wrap(index, size):
    return index & (size - 1)


def halved(index, times):
    return lax.shift_right_logical(index, jnp.int32(times))


def hop_of(step, to_b):
    return (0, 1, 2 - 4 * (to_b & 1), -1)[step]


def blend_kernel(
    owner_hbm, start_hbm, x_ref, out_ref,
    owner_ref, start_ref, patch, send0, send1, recv0, recv1, table, sums, kept, value, acc, rim, rims, total, parts,
    in_sem, owner_sem, start_sem, send_sem, recv_sem, rim_send, rim_recv, part_send, part_recv,
):
    a, b, k = lax.axis_index("gx"), lax.axis_index("gy"), lax.axis_index("gz")
    above, below = wrap(k + 1, GZ), wrap(k - 1, GZ)
    send, recv = (send0, send1), (recv0, recv1)
    near = [
        (wrap(a + dz, GX), wrap(b + db, GY), k) for dz in (0, 1, -1, 2, -2) for db in range(GY) if dz or db
    ] + [(a, b, above), (a, b, below)]
    barrier = pltpu.get_barrier_semaphore()
    for to in near:
        pl.semaphore_signal(barrier, inc=1, device_id=to, device_id_type=MESH)
    load = pltpu.make_async_copy(x_ref, patch, in_sem)
    load.start()
    indices = [
        pltpu.make_async_copy(owner_hbm, owner_ref, owner_sem),
        pltpu.make_async_copy(start_hbm, start_ref, start_sem),
    ]
    for copy in indices:
        copy.start()

    lane, sub = iota(1), iota(0)
    zero = jnp.zeros((8, 128), F32)

    def start_of(code, at_k, dim):
        return start_ref[halved(code, 2), dim, code & (GY - 1), at_k]

    for copy in indices:
        copy.wait()
    my_sy = start_of(owner_ref[a, b, k], k, 1)
    load.wait()

    def cut(half, residue, store):
        rho = (residue - my_sy) & (RES - 1)
        skip, length = ((0, 2 * PZ), (2 * PZ, PZ))[half]
        tails = []
        for g in range(GROUPS):
            tiles = {}
            for v in range(VROWS):
                into = length * v
                delta = ROW * rho + (ROW * RES * v + skip - into)
                first = halved(delta + 127, 7)
                turn = first * 128 - delta
                low, high = into // 128, (into + length - 1) // 128
                turned = []
                for t in range(low - 1, high + 1):
                    at = first + t
                    if t < 0:
                        at = jnp.maximum(at, 0)
                    if half == 1 and v == VROWS - 1 and t == high:
                        at = jnp.minimum(at, LAST)
                    turned.append(pltpu.roll(patch[g, at].astype(F32), turn, 1))
                for t in range(low, high + 1):
                    tile = jnp.where(lane < turn, turned[t - low], turned[t - low + 1])
                    tiles[t] = jnp.where(lane < into % 128, tiles[t], tile) if t in tiles else tile
            for t in range(7 if half == 0 else 3):
                store(GROUPS * t + g, tiles[t].astype(BF16))
            if half == 1:
                tails.append(tiles[3])
        if half == 1:
            store(9, jnp.where(lane < 48, tails[0], pltpu.roll(tails[1], 48, 1)).astype(BF16))
            store(10, tails[2].astype(BF16))

    def piece_copy(half, step, turn):
        to_b = wrap(b + turn, GY)
        return pltpu.make_async_remote_copy(
            src_ref=send[half].at[4 * step + turn],
            dst_ref=recv[half].at[4 * step + b],
            send_sem=send_sem.at[half, 4 * step + turn],
            recv_sem=recv_sem.at[half, 4 * step + b],
            device_id=(wrap(a + hop_of(step, to_b), GX), to_b, k),
            device_id_type=MESH,
        )

    def piece_arrival(half, step, from_b):
        return pltpu.make_async_remote_copy(
            src_ref=send[half].at[4 * step],
            dst_ref=recv[half].at[4 * step + from_b],
            send_sem=send_sem.at[half, 4 * step],
            recv_sem=recv_sem.at[half, 4 * step + from_b],
            device_id=(a, b, above),
            device_id_type=MESH,
        )

    turns_of = [(step, [turn for turn in ORDER if step or turn]) for step in ORDER]
    def cut_step(half, step):
        def cut_one(turn, carry):
            def store(tile, what):
                send[half][4 * step + turn, tile] = what

            cut(half, 4 * wrap(a + step, 4) + wrap(b + turn, GY), store)
            return carry

        if half == 0 and step == 2:
            for at, turn in enumerate(ORDER):
                cut_one(turn, 0)
                if at == 1:
                    pl.semaphore_wait(barrier, len(near))
                if at:
                    piece_copy(0, step, ORDER[at - 1]).start()
        else:
            lax.fori_loop(0 if step else 1, GY, cut_one, 0)

    def cut_own(half):
        def store(tile, what):
            recv[half][b, tile] = what

        cut(half, 4 * wrap(a, 4) + b, store)

    for step, turns in turns_of:
        cut_step(0, step)
        for turn in turns[3:] if step == 2 else turns:
            piece_copy(0, step, turn).start()
    cut_own(0)
    for step, _ in turns_of:
        cut_step(1, step)
    cut_own(1)

    for t in range(2):
        for at in range(SPAN):
            value[SLOTS * VROWS, t, at] = zero

    def clear(at, carry):
        for t in range(2):
            for margin in (*range(MARGIN), *range(MARGIN + GROUPS + 1, SPAN)):
                value[at, t, margin] = zero
        return carry

    lax.fori_loop(0, SLOTS * VROWS, clear, 0)

    residue = 4 * wrap(a, 4) + b
    along_x = [profile(sub + 8 * g, PX) for g in range(GROUPS)]
    columns = (lane, jnp.where(lane < 64, lane + 128, lane - 128))

    def corner(step, from_b):
        from_a = wrap(a - hop_of(step, b), GX)
        code = owner_ref[from_a, from_b, k]
        sy = start_of(code, k, 1)
        rho = (residue - sy) & (RES - 1)
        return start_of(code, k, 0), halved(sy + rho, 4), rho, start_of(code, k, 2) - BZ * k

    def aligned(first, second, shift, lead):
        turn = (shift - lead) & 255
        low = turn & 127
        swap = (jnp.where(lane < low, 1, 0) + halved(turn, 7)) == 1
        first, second = pltpu.roll(first.astype(F32), low, 1), pltpu.roll(second.astype(F32), low, 1)
        return jnp.where(swap, second, first), jnp.where(swap, first, second)

    def weigh_group(half, step):
        def weigh(from_b, carry):
            slot = 4 * step + from_b
            if step == 0:

                @pl.when(from_b != b)
                def _():
                    piece_arrival(half, step, from_b).wait_recv()

            else:
                piece_arrival(half, step, from_b).wait_recv()
            sx, _, rho, shift = corner(step, from_b)
            turn_x = sx & 7
            along_z = [profile(c - shift, PZ) for c in columns]
            held = {}
            for v in range(VROWS):
                for g in range(GROUPS):
                    if half == 0:
                        for m in (2 * v, 2 * v + 1):
                            held[m, g] = recv0[slot, GROUPS * m + g], recv0[slot, GROUPS * m + GROUPS + g]
                    else:
                        tail = 9 + g // 2 if v == VROWS - 1 else GROUPS * v + GROUPS + g
                        held[v, g] = recv1[slot, GROUPS * v + g], recv1[slot, tail]
                        held[v, g, 0] = [kept[slot, v, t, g] for t in range(2)]
            for v in range(VROWS):
                along_y = profile(jnp.full((8, 128), RES * v, jnp.int32) + rho, PY)
                turned = [[], []]
                for g in range(GROUPS):
                    if half == 0:
                        base, upper = [aligned(*held[m, g], shift, 16 * m) for m in (2 * v, 2 * v + 1)]
                        for t in range(2):
                            kept[slot, v, t, g] = base[t]
                    else:
                        first, second = held[v, g]
                        if v == VROWS - 1 and g == 1:
                            second = pltpu.roll(second.astype(F32), 80, 1)
                        upper = aligned(first, second, shift, 16 * v)
                        base = held[v, g, 0]
                    along_xy = along_x[g] * along_y
                    for t in range(2):
                        product = (upper[t] - base[t]) * (along_xy * along_z[t])
                        turned[t].append(pltpu.roll(product, turn_x, 0))
                for t in range(2):
                    ends = [zero] + turned[t] + [zero]
                    for g in range(GROUPS + 1):
                        value[VROWS * slot + v, t, MARGIN + g] = jnp.where(sub < turn_x, ends[g], ends[g + 1])
            return carry

        lax.fori_loop(0, GY, weigh, 0)

    def place_all(half, t):
        corners = [(4 * step + from_b, corner(step, from_b)) for step in range(4) for from_b in range(GY)]
        bases = [(VROWS * slot - first_y, first_y, MARGIN - halved(sx, 3)) for slot, (sx, first_y, _, _) in corners]

        def place(y, carry):
            places = []
            for base, first_y, at in bases:
                valid = (y >= first_y) & (y < first_y + VROWS)
                places.append((jnp.where(valid, base + y, SLOTS * VROWS), at))
            got = [value[v, t, pl.ds(at, GX)] for v, at in places]
            while len(got) > 1:
                got = [one + two for one, two in zip(got[::2], got[1::2])]
            acc[half, y, t] = got[0]
            return carry

        lax.fori_loop(0, 8, place, 0)

    def rim_copies(half):
        return [
            pltpu.make_async_remote_copy(
                src_ref=rim.at[half, side],
                dst_ref=rims.at[half, side],
                send_sem=rim_send.at[half, side],
                recv_sem=rim_recv.at[half, side],
                device_id=(a, b, to_k),
                device_id_type=MESH,
            )
            for side, to_k in ((0, above), (1, below))
        ]

    def send_rims(half):
        for block in range(GX):
            rows = slice(8 * block, 8 * block + 8)
            up, low = zero, zero
            for y in range(8):
                turned = acc[half, y, 1, block]
                turned = pltpu.roll(turned, 16 * y, 1) if y else turned
                up = jnp.where(lane // 16 == y, turned, up)
                low = jnp.where(lane // 16 == (y + 7) % 8, turned, low)
            rim[half, 0, rows, :] = up
            rim[half, 1, rows, :] = low
        for copy in rim_copies(half):
            copy.start()

    def block_of(far):
        return wrap(a + 4 + halved(far + 1, 1) * (1 - 2 * (far & 1)), GX)

    def part_copy(half, far, turn):
        to_a, to_b = block_of(far), wrap(b + ORDER[turn], GY)
        return pltpu.make_async_remote_copy(
            src_ref=total.at[half, pl.ds(pl.multiple_of(16 * (GY * to_a + to_b), 16), 16)],
            dst_ref=parts.at[half, pl.ds(pl.multiple_of(16 * (GY * a + b), 16), 16)],
            send_sem=part_send.at[half, GY * far + turn],
            recv_sem=part_recv.at[half, GY * far + turn],
            device_id=(to_a, to_b, k),
            device_id_type=MESH,
        )

    def finish_block(half, block):
        rows = pl.ds(pl.multiple_of(8 * block, 8), 8)
        up, low = rims[half, 0, rows, :], rims[half, 1, rows, :]
        cells = []
        for y in range(8):
            back = (128 - 16 * y) % 128
            ends = (pltpu.roll(up, back, 1), pltpu.roll(low, back, 1)) if y else (up, low)
            more = jnp.where(lane < 16, ends[0], jnp.where(lane >= 112, ends[1], 0.0))
            cells.append(acc[half, y, 0, block] + more)
        for y, what in enumerate(cells):
            total[half, pl.ds(pl.multiple_of(64 * block + 8 * y, 8), 8), :] = what

    def send_parts(half):
        for copy in rim_copies(half):
            copy.wait()

        def send_block(far, carry):
            finish_block(half, block_of(far))

            @pl.when(far > 0)
            def _():
                for turn in range(GY):
                    part_copy(half, far - 1, turn).start()

            return carry

        lax.fori_loop(0, GX, send_block, 0)
        for turn in range(GY - 1):
            part_copy(half, jnp.int32(GX - 1), turn).start()
        mine = pl.ds(pl.multiple_of(16 * (GY * a + b), 16), 16)
        parts[half, mine, :] = total[half, mine, :]

    def place_and_send_rims(half):
        place_all(half, 1)
        send_rims(half)
        place_all(half, 0)

    def send_rest(*steps):
        for step, turns in turns_of:
            for turn in turns if step in steps else ():
                piece_copy(0, step, turn).wait_send()
                piece_copy(1, step, turn).start()

    weigh_group(0, 2)
    send_rest(2)
    weigh_group(0, 1)
    send_rest(1)
    weigh_group(0, 3)
    send_rest(3, 0)
    weigh_group(0, 0)
    place_and_send_rims(0)
    weigh_group(1, 2)
    send_parts(0)
    weigh_group(1, 1)
    weigh_group(1, 3)
    weigh_group(1, 0)
    place_and_send_rims(1)
    send_parts(1)

    for offset in range(3 * PX):
        table[offset] = profile(jnp.full((8, 128), offset - PX, jnp.int32), PX)

    def add_weight(index, carry):
        i, j, at_k = a - 2 + lax.div(index, 9), b - 1 + lax.rem(lax.div(index, 3), 3), k - 1 + lax.rem(index, 3)
        valid = (i >= 0) & (i < GX) & (j >= 0) & (j < GY) & (at_k >= 0) & (at_k < GZ)
        i, j, at_k = jnp.clip(i, 0, GX - 1), jnp.clip(j, 0, GY - 1), jnp.clip(at_k, 0, GZ - 1)
        along_z = profile(BZ * k + lane - start_ref[i, 2, j, at_k], PZ)
        along_z = along_z * jnp.where(valid, 1.0, 0.0)
        y = BY * b + sub - start_ref[i, 1, j, at_k]
        planes = [profile(y + 8 * g, PY) * along_z for g in range(4)]
        base = jnp.clip(BX * a - start_ref[i, 0, j, at_k] + PX, 0, 2 * PX)
        new = []
        for x in range(BX):
            along_x = table[base + x]
            new += [carry[4 * x + g] + along_x * planes[g] for g in range(4)]
        return tuple(new)

    weights = lax.fori_loop(0, 45, add_weight, (zero,) * 32)
    for at in range(32):
        sums[at] = weights[at]

    for step, turns in turns_of:
        for turn in turns:
            piece_copy(1, step, turn).wait_send()

    def await_parts(half):
        def await_block(far, carry):
            for turn in range(GY - 1):
                part_copy(half, far, turn).wait()

            @pl.when(far < GX - 1)
            def _():
                part_copy(half, far, GY - 1).wait()

            return carry

        lax.fori_loop(0, GX, await_block, 0)

    def score(half, x, quarter):
        row = 8 * 16 * (quarter % 2) + 8 * (quarter // 2) + x
        one, two = [parts[half, pl.ds(row + more, 8, stride=16), :] for more in (0, 256)]
        return (one + two) / sums[4 * x + quarter]

    await_parts(0)
    for x in range(BX):
        scores = [score(0, x, quarter) for quarter in range(4)]
        for quarter in range(4):
            acc[0, x, 0, quarter] = scores[quarter]
    await_parts(1)
    for x in range(BX):
        for quarter in range(4):
            d1, d2 = acc[0, x, 0, quarter], score(1, x, quarter)
            top = jnp.maximum(jnp.maximum(d1, d2), 0.0)
            e0, e1, e2 = jnp.exp(-top), jnp.exp(d1 - top), jnp.exp(d2 - top)
            scale = 1.0 / (e0 + e1 + e2)
            rows = slice(8 * quarter, 8 * quarter + 8)
            out_ref[x, 0, rows, :] = e0 * scale
            out_ref[x, 1, rows, :] = e1 * scale
            out_ref[x, 2, rows, :] = e2 * scale


def per_device(patch_logits, patch_start, patch_owner):
    tiles = patch_logits.reshape(GROUPS, 8, LAST + 1, 128)
    probs = pl.pallas_call(
        blend_kernel,
        out_shape=jax.ShapeDtypeStruct((BX, CLASSES, BY, BZ), F32),
        in_specs=[
            pl.BlockSpec(memory_space=pl.ANY),
            pl.BlockSpec(memory_space=pl.ANY),
            pl.BlockSpec(memory_space=pl.ANY),
        ],
        out_specs=pl.BlockSpec(memory_space=pltpu.VMEM),
        scratch_shapes=[
            pltpu.SMEM((GX, GY, GZ), jnp.int32),
            pltpu.SMEM((GX, 3, GY, GZ), jnp.int32),
            pltpu.VMEM((GROUPS, LAST + 1, 8, 128), BF16),
            pltpu.VMEM((16, TILES[0], 8, 128), BF16),
            pltpu.VMEM((16, TILES[1], 8, 128), BF16),
            pltpu.VMEM((16, TILES[0], 8, 128), BF16),
            pltpu.VMEM((16, TILES[1], 8, 128), BF16),
            pltpu.VMEM((3 * PX, 8, 128), F32),
            pltpu.VMEM((32, 8, 128), F32),
            pltpu.VMEM((16, VROWS, 2, GROUPS, 8, 128), F32),
            pltpu.VMEM((SLOTS * VROWS + 1, 2, SPAN, 8, 128), F32),
            pltpu.VMEM((2, 8, 2, GX, 8, 128), F32),
            pltpu.VMEM((2, 2, 64, 128), F32),
            pltpu.VMEM((2, 2, 64, 128), F32),
            pltpu.VMEM((2, 16 * OWNERS, 128), F32),
            pltpu.VMEM((2, 16 * OWNERS, 128), F32),
            pltpu.SemaphoreType.DMA,
            pltpu.SemaphoreType.DMA,
            pltpu.SemaphoreType.DMA,
            pltpu.SemaphoreType.DMA((2, 16)),
            pltpu.SemaphoreType.DMA((2, 16)),
            pltpu.SemaphoreType.DMA((2, 2)),
            pltpu.SemaphoreType.DMA((2, 2)),
            pltpu.SemaphoreType.DMA((2, OWNERS)),
            pltpu.SemaphoreType.DMA((2, OWNERS)),
        ],
        compiler_params=pltpu.CompilerParams(collective_id=0, has_side_effects=True, vmem_limit_bytes=56000000),
    )(
        pltpu.with_memory_space_constraint(patch_owner, pltpu.HBM),
        pltpu.with_memory_space_constraint(jnp.transpose(patch_start, (0, 3, 1, 2)), pltpu.HBM),
        jnp.transpose(tiles, (0, 2, 1, 3)),
    )
    return jnp.transpose(probs, (0, 2, 1, 3))


def solution(mesh):
    return jax.shard_map(
        per_device,
        mesh=mesh,
        in_specs=(P("gx", "gy", "gz", None, None), P(), P()),
        out_specs=P("gx", "gy", None, "gz"),
        check_vma=False,
    )
```

```python
import jax
import jax.numpy as jnp
from jax import lax
from jax.experimental import pallas as pl
from jax.experimental.pallas import tpu as pltpu
from jax.sharding import PartitionSpec as P

CLASSES = 3
BX, BY, BZ = 8, 32, 128
PX, PY, PZ = 24, 48, 144
GX, GY, GZ = 8, 4, 8
ROW = CLASSES * PZ
RES = 16
VROWS = PY // RES
SLOTS = 16
GROUPS = PX // 8
TILES = (21, 11)
LAST = PY * ROW // 128 - 1
MARGIN = 5
SPAN = 13
OWNERS = GX * GY
F32 = jnp.float32
BF16 = jnp.bfloat16
MESH = pl.DeviceIdType.MESH
ORDER = (2, 1, 3, 0)


def profile(offsets, length):
    inside = (offsets >= 0) & (offsets < length)
    centre = (length - 1) / 2.0
    spread = length / 4.0
    values = jnp.exp(-((offsets.astype(F32) - centre) ** 2) / (2.0 * spread * spread))
    return jnp.where(inside, values, 0.0)


def iota(dim):
    return lax.broadcasted_iota(jnp.int32, (8, 128), dim)


def wrap(index, size):
    return index & (size - 1)


def halved(index, times):
    return lax.shift_right_logical(index, jnp.int32(times))


def hop_of(step, to_b):
    return (0, 1, 2 - 4 * (to_b & 1), -1)[step]


def blend_kernel(
    owner_hbm, start_hbm, x_ref, out_ref,
    owner_ref, start_ref, patch, send0, send1, recv0, recv1, table, sums, kept, value, acc, rim, rims, total, parts,
    in_sem, owner_sem, start_sem, send_sem, recv_sem, rim_send, rim_recv, part_send, part_recv,
):
    a, b, k = lax.axis_index("gx"), lax.axis_index("gy"), lax.axis_index("gz")
    above, below = wrap(k + 1, GZ), wrap(k - 1, GZ)
    send, recv = (send0, send1), (recv0, recv1)
    near = [
        (wrap(a + dz, GX), wrap(b + db, GY), k) for dz in (0, 1, -1, 2, -2) for db in range(GY) if dz or db
    ] + [(a, b, above), (a, b, below)]
    load = pltpu.make_async_copy(x_ref, patch, in_sem)
    load.start()
    indices = [
        pltpu.make_async_copy(owner_hbm, owner_ref, owner_sem),
        pltpu.make_async_copy(start_hbm, start_ref, start_sem),
    ]
    for copy in indices:
        copy.start()
    barrier = pltpu.get_barrier_semaphore()
    for to in near:
        pl.semaphore_signal(barrier, inc=1, device_id=to, device_id_type=MESH)

    lane, sub = iota(1), iota(0)
    zero = jnp.zeros((8, 128), F32)

    def start_of(code, at_k, dim):
        return start_ref[halved(code, 2), dim, code & (GY - 1), at_k]

    for copy in indices:
        copy.wait()
    my_sy = start_of(owner_ref[a, b, k], k, 1)
    load.wait()

    def cut(half, residue, store):
        rho = (residue - my_sy) & (RES - 1)
        skip, length = ((0, 2 * PZ), (2 * PZ, PZ))[half]
        tails = []
        for g in range(GROUPS):
            tiles = {}
            for v in range(VROWS):
                into = length * v
                delta = ROW * rho + (ROW * RES * v + skip - into)
                first = halved(delta + 127, 7)
                turn = first * 128 - delta
                low, high = into // 128, (into + length - 1) // 128
                turned = []
                for t in range(low - 1, high + 1):
                    at = first + t
                    if t < 0:
                        at = jnp.maximum(at, 0)
                    if half == 1 and v == VROWS - 1 and t == high:
                        at = jnp.minimum(at, LAST)
                    turned.append(pltpu.roll(patch[g, at].astype(F32), turn, 1))
                for t in range(low, high + 1):
                    tile = jnp.where(lane < turn, turned[t - low], turned[t - low + 1])
                    tiles[t] = jnp.where(lane < into % 128, tiles[t], tile) if t in tiles else tile
            for t in range(7 if half == 0 else 3):
                store(GROUPS * t + g, tiles[t].astype(BF16))
            if half == 1:
                tails.append(tiles[3])
        if half == 1:
            store(9, jnp.where(lane < 48, tails[0], pltpu.roll(tails[1], 48, 1)).astype(BF16))
            store(10, tails[2].astype(BF16))

    def piece_copy(half, step, turn):
        to_b = wrap(b + turn, GY)
        return pltpu.make_async_remote_copy(
            src_ref=send[half].at[4 * step + turn],
            dst_ref=recv[half].at[4 * step + b],
            send_sem=send_sem.at[half, 4 * step + turn],
            recv_sem=recv_sem.at[half, 4 * step + b],
            device_id=(wrap(a + hop_of(step, to_b), GX), to_b, k),
            device_id_type=MESH,
        )

    def piece_arrival(half, step, from_b):
        return pltpu.make_async_remote_copy(
            src_ref=send[half].at[4 * step],
            dst_ref=recv[half].at[4 * step + from_b],
            send_sem=send_sem.at[half, 4 * step],
            recv_sem=recv_sem.at[half, 4 * step + from_b],
            device_id=(a, b, above),
            device_id_type=MESH,
        )

    turns_of = [(step, [turn for turn in ORDER if step or turn]) for step in ORDER]
    def cut_step(half, step):
        def cut_one(turn, carry):
            def store(tile, what):
                send[half][4 * step + turn, tile] = what

            cut(half, 4 * wrap(a + step, 4) + wrap(b + turn, GY), store)
            return carry

        if half == 0 and step == 2:
            for at, turn in enumerate(ORDER):
                cut_one(turn, 0)
                if at == 1:
                    pl.semaphore_wait(barrier, len(near))
                if at:
                    piece_copy(0, step, ORDER[at - 1]).start()
        else:
            lax.fori_loop(0 if step else 1, GY, cut_one, 0)

    def cut_own(half):
        def store(tile, what):
            recv[half][b, tile] = what

        cut(half, 4 * wrap(a, 4) + b, store)

    for step, turns in turns_of:
        cut_step(0, step)
        for turn in turns[3:] if step == 2 else turns:
            piece_copy(0, step, turn).start()
    cut_own(0)
    for step, _ in turns_of:
        cut_step(1, step)
    cut_own(1)

    for t in range(2):
        for at in range(SPAN):
            value[SLOTS * VROWS, t, at] = zero

    def clear(at, carry):
        for t in range(2):
            for margin in (*range(MARGIN), *range(MARGIN + GROUPS + 1, SPAN)):
                value[at, t, margin] = zero
        return carry

    lax.fori_loop(0, SLOTS * VROWS, clear, 0)

    residue = 4 * wrap(a, 4) + b
    along_x = [profile(sub + 8 * g, PX) for g in range(GROUPS)]
    columns = (lane, jnp.where(lane < 64, lane + 128, lane - 128))

    def corner(step, from_b):
        from_a = wrap(a - hop_of(step, b), GX)
        code = owner_ref[from_a, from_b, k]
        sy = start_of(code, k, 1)
        rho = (residue - sy) & (RES - 1)
        return start_of(code, k, 0), halved(sy + rho, 4), rho, start_of(code, k, 2) - BZ * k

    def aligned(first, second, shift, lead):
        turn = (shift - lead) & 255
        low = turn & 127
        swap = (jnp.where(lane < low, 1, 0) + halved(turn, 7)) == 1
        first, second = pltpu.roll(first.astype(F32), low, 1), pltpu.roll(second.astype(F32), low, 1)
        return jnp.where(swap, second, first), jnp.where(swap, first, second)

    def weigh_group(half, step):
        def weigh(from_b, carry):
            slot = 4 * step + from_b
            if step == 0:

                @pl.when(from_b != b)
                def _():
                    piece_arrival(half, step, from_b).wait_recv()

            else:
                piece_arrival(half, step, from_b).wait_recv()
            sx, _, rho, shift = corner(step, from_b)
            turn_x = sx & 7
            along_z = [profile(c - shift, PZ) for c in columns]
            held = {}
            for v in range(VROWS):
                for g in range(GROUPS):
                    if half == 0:
                        for m in (2 * v, 2 * v + 1):
                            held[m, g] = recv0[slot, GROUPS * m + g], recv0[slot, GROUPS * m + GROUPS + g]
                    else:
                        tail = 9 + g // 2 if v == VROWS - 1 else GROUPS * v + GROUPS + g
                        held[v, g] = recv1[slot, GROUPS * v + g], recv1[slot, tail]
                        held[v, g, 0] = [kept[slot, v, t, g] for t in range(2)]
            for v in range(VROWS):
                along_y = profile(jnp.full((8, 128), RES * v, jnp.int32) + rho, PY)
                turned = [[], []]
                for g in range(GROUPS):
                    if half == 0:
                        base, upper = [aligned(*held[m, g], shift, 16 * m) for m in (2 * v, 2 * v + 1)]
                        for t in range(2):
                            kept[slot, v, t, g] = base[t]
                    else:
                        first, second = held[v, g]
                        if v == VROWS - 1 and g == 1:
                            second = pltpu.roll(second.astype(F32), 80, 1)
                        upper = aligned(first, second, shift, 16 * v)
                        base = held[v, g, 0]
                    along_xy = along_x[g] * along_y
                    for t in range(2):
                        product = (upper[t] - base[t]) * (along_xy * along_z[t])
                        turned[t].append(pltpu.roll(product, turn_x, 0))
                for t in range(2):
                    ends = [zero] + turned[t] + [zero]
                    for g in range(GROUPS + 1):
                        value[VROWS * slot + v, t, MARGIN + g] = jnp.where(sub < turn_x, ends[g], ends[g + 1])
            return carry

        lax.fori_loop(0, GY, weigh, 0)

    def place_all(half, t):
        corners = [(4 * step + from_b, corner(step, from_b)) for step in range(4) for from_b in range(GY)]
        bases = [(VROWS * slot - first_y, first_y, MARGIN - halved(sx, 3)) for slot, (sx, first_y, _, _) in corners]

        def place(y, carry):
            places = []
            for base, first_y, at in bases:
                valid = (y >= first_y) & (y < first_y + VROWS)
                places.append((jnp.where(valid, base + y, SLOTS * VROWS), at))
            got = [value[v, t, pl.ds(at, GX)] for v, at in places]
            while len(got) > 1:
                got = [one + two for one, two in zip(got[::2], got[1::2])]
            acc[half, y, t] = got[0]
            return carry

        lax.fori_loop(0, 8, place, 0)

    def rim_copies(half):
        return [
            pltpu.make_async_remote_copy(
                src_ref=rim.at[half, side],
                dst_ref=rims.at[half, side],
                send_sem=rim_send.at[half, side],
                recv_sem=rim_recv.at[half, side],
                device_id=(a, b, to_k),
                device_id_type=MESH,
            )
            for side, to_k in ((0, above), (1, below))
        ]

    def send_rims(half):
        for block in range(GX):
            rows = slice(8 * block, 8 * block + 8)
            up, low = zero, zero
            for y in range(8):
                turned = acc[half, y, 1, block]
                turned = pltpu.roll(turned, 16 * y, 1) if y else turned
                up = jnp.where(lane // 16 == y, turned, up)
                low = jnp.where(lane // 16 == (y + 7) % 8, turned, low)
            rim[half, 0, rows, :] = up
            rim[half, 1, rows, :] = low
        for copy in rim_copies(half):
            copy.start()

    def block_of(far):
        return wrap(a + 4 + halved(far + 1, 1) * (1 - 2 * (far & 1)), GX)

    def part_copy(half, far, turn):
        to_a, to_b = block_of(far), wrap(b + ORDER[turn], GY)
        return pltpu.make_async_remote_copy(
            src_ref=total.at[half, pl.ds(pl.multiple_of(16 * (GY * to_a + to_b), 16), 16)],
            dst_ref=parts.at[half, pl.ds(pl.multiple_of(16 * (GY * a + b), 16), 16)],
            send_sem=part_send.at[half, GY * far + turn],
            recv_sem=part_recv.at[half, GY * far + turn],
            device_id=(to_a, to_b, k),
            device_id_type=MESH,
        )

    def finish_block(half, block):
        rows = pl.ds(pl.multiple_of(8 * block, 8), 8)
        up, low = rims[half, 0, rows, :], rims[half, 1, rows, :]
        cells = []
        for y in range(8):
            back = (128 - 16 * y) % 128
            ends = (pltpu.roll(up, back, 1), pltpu.roll(low, back, 1)) if y else (up, low)
            more = jnp.where(lane < 16, ends[0], jnp.where(lane >= 112, ends[1], 0.0))
            cells.append(acc[half, y, 0, block] + more)
        for y, what in enumerate(cells):
            total[half, pl.ds(pl.multiple_of(64 * block + 8 * y, 8), 8), :] = what

    def send_parts(half):
        for copy in rim_copies(half):
            copy.wait()

        def send_block(far, carry):
            finish_block(half, block_of(far))

            @pl.when(far > 0)
            def _():
                for turn in range(GY):
                    part_copy(half, far - 1, turn).start()

            return carry

        lax.fori_loop(0, GX, send_block, 0)
        for turn in range(GY - 1):
            part_copy(half, jnp.int32(GX - 1), turn).start()
        mine = pl.ds(pl.multiple_of(16 * (GY * a + b), 16), 16)
        parts[half, mine, :] = total[half, mine, :]

    def place_and_send_rims(half):
        place_all(half, 1)
        send_rims(half)
        place_all(half, 0)

    def send_rest(*steps):
        for step, turns in turns_of:
            for turn in turns if step in steps else ():
                piece_copy(0, step, turn).wait_send()
                piece_copy(1, step, turn).start()

    weigh_group(0, 2)
    send_rest(2)
    weigh_group(0, 1)
    send_rest(1)
    weigh_group(0, 3)
    send_rest(3, 0)
    weigh_group(0, 0)
    place_and_send_rims(0)
    weigh_group(1, 2)
    send_parts(0)
    weigh_group(1, 1)
    weigh_group(1, 3)
    weigh_group(1, 0)
    place_and_send_rims(1)
    send_parts(1)

    for offset in range(3 * PX):
        table[offset] = profile(jnp.full((8, 128), offset - PX, jnp.int32), PX)

    def add_weight(index, carry):
        i, j, at_k = a - 2 + lax.div(index, 9), b - 1 + lax.rem(lax.div(index, 3), 3), k - 1 + lax.rem(index, 3)
        valid = (i >= 0) & (i < GX) & (j >= 0) & (j < GY) & (at_k >= 0) & (at_k < GZ)
        i, j, at_k = jnp.clip(i, 0, GX - 1), jnp.clip(j, 0, GY - 1), jnp.clip(at_k, 0, GZ - 1)
        along_z = profile(BZ * k + lane - start_ref[i, 2, j, at_k], PZ)
        along_z = along_z * jnp.where(valid, 1.0, 0.0)
        y = BY * b + sub - start_ref[i, 1, j, at_k]
        planes = [profile(y + 8 * g, PY) * along_z for g in range(4)]
        base = jnp.clip(BX * a - start_ref[i, 0, j, at_k] + PX, 0, 2 * PX)
        new = []
        for x in range(BX):
            along_x = table[base + x]
            new += [carry[4 * x + g] + along_x * planes[g] for g in range(4)]
        return tuple(new)

    weights = lax.fori_loop(0, 45, add_weight, (zero,) * 32)
    for at in range(32):
        sums[at] = weights[at]

    for step, turns in turns_of:
        for turn in turns:
            piece_copy(1, step, turn).wait_send()

    def await_parts(half):
        def await_block(far, carry):
            for turn in range(GY - 1):
                part_copy(half, far, turn).wait()

            @pl.when(far < GX - 1)
            def _():
                part_copy(half, far, GY - 1).wait()

            return carry

        lax.fori_loop(0, GX, await_block, 0)

    def score(half, x, quarter):
        row = 8 * 16 * (quarter % 2) + 8 * (quarter // 2) + x
        one, two = [parts[half, pl.ds(row + more, 8, stride=16), :] for more in (0, 256)]
        return (one + two) / sums[4 * x + quarter]

    await_parts(0)
    for x in range(BX):
        scores = [score(0, x, quarter) for quarter in range(4)]
        for quarter in range(4):
            acc[0, x, 0, quarter] = scores[quarter]
    await_parts(1)
    for x in range(BX):
        for quarter in range(4):
            d1, d2 = acc[0, x, 0, quarter], score(1, x, quarter)
            top = jnp.maximum(jnp.maximum(d1, d2), 0.0)
            e0, e1, e2 = jnp.exp(-top), jnp.exp(d1 - top), jnp.exp(d2 - top)
            scale = 1.0 / (e0 + e1 + e2)
            rows = slice(8 * quarter, 8 * quarter + 8)
            out_ref[x, 0, rows, :] = e0 * scale
            out_ref[x, 1, rows, :] = e1 * scale
            out_ref[x, 2, rows, :] = e2 * scale


def per_device(patch_logits, patch_start, patch_owner):
    tiles = patch_logits.reshape(GROUPS, 8, LAST + 1, 128)
    probs = pl.pallas_call(
        blend_kernel,
        out_shape=jax.ShapeDtypeStruct((BX, CLASSES, BY, BZ), F32),
        in_specs=[
            pl.BlockSpec(memory_space=pl.ANY),
            pl.BlockSpec(memory_space=pl.ANY),
            pl.BlockSpec(memory_space=pl.ANY),
        ],
        out_specs=pl.BlockSpec(memory_space=pltpu.VMEM),
        scratch_shapes=[
            pltpu.SMEM((GX, GY, GZ), jnp.int32),
            pltpu.SMEM((GX, 3, GY, GZ), jnp.int32),
            pltpu.VMEM((GROUPS, LAST + 1, 8, 128), BF16),
            pltpu.VMEM((16, TILES[0], 8, 128), BF16),
            pltpu.VMEM((16, TILES[1], 8, 128), BF16),
            pltpu.VMEM((16, TILES[0], 8, 128), BF16),
            pltpu.VMEM((16, TILES[1], 8, 128), BF16),
            pltpu.VMEM((3 * PX, 8, 128), F32),
            pltpu.VMEM((32, 8, 128), F32),
            pltpu.VMEM((16, VROWS, 2, GROUPS, 8, 128), F32),
            pltpu.VMEM((SLOTS * VROWS + 1, 2, SPAN, 8, 128), F32),
            pltpu.VMEM((2, 8, 2, GX, 8, 128), F32),
            pltpu.VMEM((2, 2, 64, 128), F32),
            pltpu.VMEM((2, 2, 64, 128), F32),
            pltpu.VMEM((2, 16 * OWNERS, 128), F32),
            pltpu.VMEM((2, 16 * OWNERS, 128), F32),
            pltpu.SemaphoreType.DMA,
            pltpu.SemaphoreType.DMA,
            pltpu.SemaphoreType.DMA,
            pltpu.SemaphoreType.DMA((2, 16)),
            pltpu.SemaphoreType.DMA((2, 16)),
            pltpu.SemaphoreType.DMA((2, 2)),
            pltpu.SemaphoreType.DMA((2, 2)),
            pltpu.SemaphoreType.DMA((2, OWNERS)),
            pltpu.SemaphoreType.DMA((2, OWNERS)),
        ],
        compiler_params=pltpu.CompilerParams(collective_id=0, has_side_effects=True, vmem_limit_bytes=56000000),
    )(
        pltpu.with_memory_space_constraint(patch_owner, pltpu.HBM),
        pltpu.with_memory_space_constraint(jnp.transpose(patch_start, (0, 3, 1, 2)), pltpu.HBM),
        jnp.transpose(tiles, (0, 2, 1, 3)),
    )
    return jnp.transpose(probs, (0, 2, 1, 3))


def solution(mesh):
    return jax.shard_map(
        per_device,
        mesh=mesh,
        in_specs=(P("gx", "gy", "gz", None, None), P(), P()),
        out_specs=P("gx", "gy", None, "gz"),
        check_vma=False,
    )
```
